128 devices in a mesh: seq: 32 (over x, y, core), head: 4 (over z).
Axes of the slice: x: 4, y: 4, z: 4, core: 2. Of those that a mesh axis runs over, the one named last changes fastest.
Arguments:
- values: bfloat16 [65536, 5120], P('seq', 'head'), may hold values from -6 to 6
- gates: bfloat16 [65536, 5120], P('seq', 'head'), may hold values from -6 to 6
- b_proj: bfloat16 [65536, 128], P('seq'), may hold values from -2 to 2
- c_proj: bfloat16 [65536, 128], P('seq'), may hold values from -2 to 2
- step_size: float32 [80, 65536], P('head', 'seq'), may hold values from 0.006 to 0.06
- decay_rate: float32 [80, 65536], P('head', 'seq'), may hold values from 0 to 1.2, as said below
- skip_gain: float32 [80], P('head'), may hold values from 0.5 to 2
- norm_gain: float32 [5120], P('head'), may hold values from 0.25 to 1.75
- readout_matrix: bfloat16 [5120, 2560], P('head'), may hold values from -0.078125 to 0.078125
- span_counts: int32 [32], P('seq'), may hold values from 1 to 8, as said below
- remaining_count: int32 [32], P('seq'), may hold values from 1 to 256
Outputs:
- mixer_response: bfloat16 [65536, 2560], P(('seq', 'head'))
The draws below stay inside these ranges and needn't reach their ends.
Inputs may be any that keep to these rules, and one draw needn't show every extreme that they name: `span_counts`: some shard uses all 8 span slots in every draw. `decay_rate`: Positive.
All inputs are finite; a program needn't handle non-finite values.
Results may differ from the reference program's by a relative error of at most 0.02.
Values may be sent and summed in bfloat16 or wider, within the bound.
No kernel may reach another device: no remote copies, remote signals or barrier semaphores. Data moves between devices by JAX's collectives and lax.ppermute only.
A program may use at most 192 MiB of HBM per device.

```python
import math
import jax
import jax.numpy as jnp
from jax import lax

D = 2560
HEADS = 80
P_SIZE = 64
N = 128
SPAN = 256
CH_DEV = 8
TOK_DEV = 2048
SHARDS = 32
ENTRY_CAPACITY = 65536
N_HEAD = 4


def draw_decay_rate(key, part):
    keys = jax.random.split(key, 6)
    share = 0.5
    quick_heads = jax.random.uniform(keys[0], (HEADS,)) < share
    quick = jnp.exp(jax.random.uniform(keys[1], (HEADS,), jnp.float32, math.log(1.0 / 50.0), math.log(1.0 / 30.0)))
    slow = 0.2 * math.log(10.0) / ENTRY_CAPACITY * jnp.exp(jax.random.uniform(keys[2], (HEADS,), jnp.float32, -0.5, 0.5))
    base = jnp.where(quick_heads, quick, slow)
    blockwise = jnp.exp(jax.random.uniform(keys[3], (HEADS, ENTRY_CAPACITY // SPAN, 1), jnp.float32, -0.7, 0.7))
    rough = jax.random.uniform(keys[4], (HEADS, ENTRY_CAPACITY // SPAN, SPAN), jnp.float32, 0.5, 2.0)
    forgetting_factor = (base[:, None, None] * blockwise * rough).reshape(HEADS, ENTRY_CAPACITY)
    entry_indices = jax.random.randint(keys[5], (3,), 0, ENTRY_CAPACITY)
    element_cluster = jnp.zeros((ENTRY_CAPACITY,), jnp.float32).at[entry_indices].add(0.3)
    return (forgetting_factor + element_cluster[None, :]).astype(jnp.float32)


def draw_span_counts(key, part):
    first_key, second_key = jax.random.split(key)
    first = jax.random.randint(first_key, (SHARDS,), 0, CH_DEV)
    second = jax.random.randint(second_key, (SHARDS,), 0, CH_DEV)
    counts = 1 + first * second // (CH_DEV - 1)
    chosen = jax.random.randint(jax.random.fold_in(key, 7), (), 0, SHARDS)
    return counts.at[chosen].set(CH_DEV).astype(jnp.int32)


def place_ends(values, key, least, high):
    shape = values.shape
    place = [jax.random.randint(jax.random.fold_in(key, axis), (), 0, shape[axis]) for axis in range(len(shape))]
    values = values.at[tuple(place)].set(least)
    longest = shape.index(max(shape))
    place[longest] = (place[longest] + 1) % shape[longest]
    return values.at[tuple(place)].set(high)


def level_of(own_key, extent, pieces, low, high):
    loudness, own = 1.0, jax.random.fold_in(own_key, 6)
    for position, shards_of in pieces:
        heights = jnp.exp(jax.random.uniform(jax.random.fold_in(own, position), (shards_of,), jnp.float32, low / len(pieces), high / len(pieces)))
        loudness = loudness * jnp.repeat(heights, extent[position] // shards_of).reshape([-1 if axis == position else 1 for axis in range(len(extent))])
    return loudness


def gaussian(key, dims, scale, reach, pieces=(), kind=jnp.bfloat16):
    values = jax.random.normal(key, dims, jnp.float32) * scale
    if len(pieces) > 0:
        values = level_of(key, dims, pieces, -0.22, 0.18) * values
    return jnp.clip(values, min=-reach, max=reach).astype(kind)


def setup_inputs(seed: int = 0) -> dict:
    seeds = jax.random.split(jax.random.key(seed), 12)
    values = gaussian(seeds[0], (ENTRY_CAPACITY, HEADS * P_SIZE), 1.0, 6.0, ((0, 32), (1, 4)))
    gates = gaussian(seeds[1], (ENTRY_CAPACITY, HEADS * P_SIZE), 1.0, 6.0, ((0, 32), (1, 4)))
    b_proj = gaussian(seeds[2], (ENTRY_CAPACITY, N), 0.3, 2.0, ((0, 32),))
    c_proj = gaussian(seeds[3], (ENTRY_CAPACITY, N), 0.3, 2.0, ((0, 32),))
    step_size = jnp.clip(jnp.exp(math.log(0.06) - 2.3025851 * jax.random.uniform(seeds[4], (HEADS, ENTRY_CAPACITY), jnp.float32) ** level_of(seeds[4], (HEADS, ENTRY_CAPACITY), ((0, 4), (1, 32)), -0.2, 0.2)), 0.006, 0.06)
    decay_rate = draw_decay_rate(jax.random.fold_in(seeds[11], 71), 0)
    skip_gain = jnp.clip(0.5 + 1.5 * jax.random.uniform(seeds[6], (HEADS,), jnp.float32) ** level_of(seeds[6], (HEADS,), ((0, 4),), -0.2, 0.2), 0.5, 2.0)
    norm_gain = jnp.clip(1.0 + 0.15 * jax.random.normal(seeds[7], (HEADS * P_SIZE,), jnp.float32), 0.25, 1.75)
    readout_matrix = gaussian(seeds[8], (HEADS * P_SIZE, D), (HEADS * P_SIZE) ** -0.5, 0.078125, ((0, 4),))
    span_counts = draw_span_counts(jax.random.fold_in(seeds[11], 71), 0)
    remaining_count = place_ends(jax.random.randint(seeds[10], (SHARDS,), 1, SPAN + 1), jax.random.fold_in(seeds[10], 1), 1, SPAN).astype(jnp.int32)
    return {"values": values, "gates": gates, "b_proj": b_proj, "c_proj": c_proj, "step_size": step_size, "decay_rate": decay_rate, "skip_gain": skip_gain, "norm_gain": norm_gain, "readout_matrix": readout_matrix, "span_counts": span_counts, "remaining_count": remaining_count}


def reference(values, gates, b_proj, c_proj, step_size, decay_rate, skip_gain, norm_gain, readout_matrix, span_counts, remaining_count):
    f32 = jnp.float32
    bf16 = jnp.bfloat16
    valid = (span_counts - 1) * SPAN + remaining_count
    limit = jnp.repeat(valid, TOK_DEV)
    positioned_entries = jnp.arange(ENTRY_CAPACITY, dtype=jnp.int32) % TOK_DEV
    live = (positioned_entries < limit).astype(f32)
    blocks = ENTRY_CAPACITY // SPAN

    def spanned(array):
        return array.reshape((blocks, SPAN) + array.shape[1:])

    def per_head(array):
        return array.reshape(HEADS, blocks, SPAN).transpose(1, 0, 2)
    items = (spanned(values), spanned(gates), spanned(b_proj), spanned(c_proj), per_head(step_size), per_head(decay_rate), spanned(live))
    lower = jnp.arange(SPAN)[:, None] >= jnp.arange(SPAN)[None, :]
    group_width = HEADS * P_SIZE // N_HEAD

    def advance(state, item):
        x_span, z_span, b_span, c_span, dt_span, rate_span, live_span = item
        logdec = -rate_span * live_span[None, :]
        running = jnp.cumsum(logdec, axis=1)
        weight = dt_span * live_span[None, :]
        gram = jnp.einsum('in,jn->ij', c_span.astype(f32), b_span.astype(f32))
        spread = jnp.where(lower[None], running[:, :, None] - running[:, None, :], -1e+30)
        mixing = lax.optimization_barrier((gram[None] * jnp.exp(spread) * weight[:, None, :]).astype(bf16))
        heads_x = x_span.reshape(SPAN, HEADS, P_SIZE).astype(f32)
        inner = jnp.einsum('hij,jhp->ihp', mixing.astype(f32), heads_x)
        held = lax.optimization_barrier(state.astype(bf16))
        carried = jnp.einsum('in,hpn->ihp', c_span.astype(f32), held.astype(f32)) * jnp.exp(running).T[:, :, None]
        mixed = (inner + carried + skip_gain[None, :, None] * heads_x) * live_span[:, None, None]
        tail = jnp.exp(running[:, -1:] - running) * weight
        weighted = lax.optimization_barrier((heads_x * tail.T[:, :, None]).astype(bf16))
        fresh = jnp.einsum('jhp,jn->hpn', weighted.astype(f32), b_span.astype(f32))
        state = jnp.exp(running[:, -1])[:, None, None] * state + fresh
        gated = mixed.reshape(SPAN, HEADS * P_SIZE) * jax.nn.silu(z_span.astype(f32))
        meansq = lax.optimization_barrier(jnp.mean(gated * gated, axis=1, keepdims=True))
        normed = (gated * lax.rsqrt(meansq + 1e-05) * norm_gain[None, :]).astype(bf16)
        summed = jnp.zeros((SPAN, D), f32)
        for group in range(N_HEAD):
            lo_col = group * group_width
            partial_term = jnp.dot(normed[:, lo_col:lo_col + group_width], readout_matrix[lo_col:lo_col + group_width], preferred_element_type=f32).astype(bf16)
            summed = summed + lax.optimization_barrier(partial_term).astype(f32)
        return (state, summed.astype(bf16))
    start_state = jnp.zeros((HEADS, P_SIZE, N), f32)
    _, produced = lax.scan(advance, start_state, items)
    return produced.reshape(ENTRY_CAPACITY, D)
```

```python
import jax
import jax.numpy as jnp
from jax import lax
from jax.experimental import pallas as pl
from jax.experimental.pallas import tpu as pltpu
from jax.sharding import Mesh
from jax.sharding import PartitionSpec as P

HEADS = 80
P_SIZE = 64
SPAN = 256
PART = 128
SEQ = ("seq_0", "seq_1", "seq_2")
SEQ_HEAD = ("seq_0", "seq_1", "seq_2", "head")
LOG2E = 1.4426950408889634
HIGHEST = lax.Precision.HIGHEST
f32 = jnp.float32
bf16 = jnp.bfloat16


def iota(shape, dim):
    return lax.broadcasted_iota(jnp.int32, shape, dim)


def pair(columns, first):
    rows = columns.shape[0]
    return jnp.where(
        iota((rows, 128), 1) < 64,
        columns[:, first : first + 1],
        columns[:, first + 1 : first + 2],
    )


def states_kernel(
    scalars, x_ref, b_ref, rate_ref, dt_ref,
    before_ref, meta_ref, row_ref, mine_ref, other_ref,
    state, raw, lead, weighted,
):
    step = pl.program_id(0)
    heads = rate_ref.shape[0]
    pairs = heads // 2
    width = x_ref.shape[1]
    half = width // 2

    @pl.when(step == 0)
    def _():
        state[...] = jnp.zeros_like(state)
        raw[...] = jnp.zeros_like(raw)
        lead[...] = jnp.zeros_like(lead)

    upper = (iota((PART, PART), 0) <= iota((PART, PART), 1)).astype(f32)
    for k in range(x_ref.shape[0] // PART):
        at = slice(k * PART, (k + 1) * PART)
        token = (step * (x_ref.shape[0] // PART) + k) * PART + iota((1, PART), 1)
        live = (token < scalars[0]).astype(f32)
        raw[0:heads, :] = rate_ref[:, at] * (live * -LOG2E)
        raw[32 : 32 + heads, :] = dt_ref[:, at] * live
        weight = raw[32:64, :]
        running = jnp.dot(raw[0:32, :], upper, precision=HIGHEST, preferred_element_type=f32)
        tail = jnp.exp2(running[:, PART - 1 : PART] - running) * weight
        total = lead[...] + running
        lead[...] = jnp.broadcast_to(total[:, PART - 1 : PART], (32, PART))
        row_ref[:, at] = running - jnp.where(weight > 0, jnp.log(weight) * LOG2E, -1e30)
        meta = jnp.concatenate([running, tail, total, total], axis=0).T
        meta_ref[at, :] = meta
        before_ref[k] = state[...].astype(bf16)
        for q in range(pairs):
            cols = slice(q * 128, (q + 1) * 128)
            weighted[:, cols] = (x_ref[at, cols].astype(f32) * pair(meta, 32 + 2 * q)).astype(bf16)
        turned = b_ref[at, :].astype(f32).T.astype(bf16)
        fresh = jnp.dot(turned, weighted[...], preferred_element_type=f32)
        ends = jnp.exp2(meta[PART - 8 : PART, :])
        for q in range(pairs):
            cols = slice(q * 128, (q + 1) * 128)
            state[:, cols] = state[:, cols] * pair(ends, 2 * q)[7:8, :] + fresh[:, cols]

    @pl.when(step == pl.num_programs(0) - 1)
    def _():
        ends = meta_ref[meta_ref.shape[0] - 16 : meta_ref.shape[0], :]
        wide = jnp.concatenate([pair(ends, 64 + 2 * q)[15:16, :] for q in range(pairs)], axis=1)
        high = wide.astype(bf16).astype(f32)
        line = iota((16, width), 0)
        decay = jnp.where(line == 0, high, jnp.where(line == 1, wide - high, 0.0)).astype(bf16)
        core = scalars[1]
        for place, ref in ((0, mine_ref), (1, other_ref)):
            low = (core == place)
            ref[0:128, :] = jnp.where(low, state[:, :half], state[:, half:]).astype(bf16)
            ref[128:144, :] = jnp.where(
                low, decay[:, :half].astype(f32), decay[:, half:].astype(f32)
            ).astype(bf16)


def states(scalars, x, b, rate, dt):
    length, width = x.shape
    heads = rate.shape[0]
    steps = 4
    rows = length // steps
    parts = rows // PART
    return pl.pallas_call(
        states_kernel,
        grid_spec=pltpu.PrefetchScalarGridSpec(
            num_scalar_prefetch=1,
            grid=(steps,),
            in_specs=[
                pl.BlockSpec((rows, width), lambda i, s: (i, 0)),
                pl.BlockSpec((rows, 128), lambda i, s: (i, 0)),
                pl.BlockSpec((heads, rows), lambda i, s: (0, i)),
                pl.BlockSpec((heads, rows), lambda i, s: (0, i)),
            ],
            out_specs=[
                pl.BlockSpec((parts, 128, width), lambda i, s: (i, 0, 0)),
                pl.BlockSpec((rows, 128), lambda i, s: (i, 0)),
                pl.BlockSpec((32, rows), lambda i, s: (0, i)),
                pl.BlockSpec((144, width // 2), lambda i, s: (0, 0)),
                pl.BlockSpec((144, width // 2), lambda i, s: (0, 0)),
            ],
            scratch_shapes=[
                pltpu.VMEM((128, width), f32),
                pltpu.VMEM((64, PART), f32),
                pltpu.VMEM((32, PART), f32),
                pltpu.VMEM((PART, width), bf16),
            ],
        ),
        out_shape=[
            jax.ShapeDtypeStruct((length // PART, 128, width), bf16),
            jax.ShapeDtypeStruct((length, 128), f32),
            jax.ShapeDtypeStruct((32, length), f32),
            jax.ShapeDtypeStruct((144, width // 2), bf16),
            jax.ShapeDtypeStruct((144, width // 2), bf16),
        ],
        compiler_params=pltpu.CompilerParams(dimension_semantics=("arbitrary",)),
        name="states",
    )(scalars, x, b, rate, dt)


def local_kernel(scalars, x_ref, b_ref, c_ref, meta_ref, row_ref, before_ref, skip_ref, y_ref):
    pairs = x_ref.shape[1] // 128
    lower = iota((PART, PART), 0) >= iota((PART, PART), 1)
    left = iota((PART, 128), 1) < 64
    for k in range(x_ref.shape[0] // PART):
        at = slice(k * PART, (k + 1) * PART)
        gram = lax.dot_general(
            c_ref[at, :], b_ref[at, :], (((1,), (1,)), ((), ())), preferred_element_type=f32
        )
        gram = jnp.where(lower, gram, 0.0)
        meta = meta_ref[at, :]
        grown = jnp.exp2(meta)
        for q in range(pairs):
            cols = slice(q * 128, (q + 1) * 128)
            both = []
            for h in (2 * q, 2 * q + 1):
                power = jnp.minimum(meta[:, h : h + 1] - row_ref[h : h + 1, at], 100.0)
                both.append((gram * jnp.exp2(power)).astype(bf16))
            x = x_ref[at, cols]
            wide = x.astype(f32)
            stack = jnp.concatenate(
                [jnp.where(left, wide, 0.0).astype(bf16), jnp.where(left, 0.0, wide).astype(bf16)],
                axis=0,
            )
            inner = jnp.dot(jnp.concatenate(both, axis=1), stack, preferred_element_type=f32)
            held = jnp.dot(c_ref[at, :], before_ref[k, :, cols], preferred_element_type=f32)
            y = inner + pair(grown, 2 * q) * held + skip_ref[0:1, cols] * wide
            y_ref[at, cols] = y.astype(bf16)


def local(scalars, x, b, c, meta, row, before, skip, block, rows):
    width = x.shape[1]
    tile = 256
    steps = rows // tile
    parts = tile // PART

    def at(i, s):
        return s[2 + block] * steps + i

    return pl.pallas_call(
        local_kernel,
        grid_spec=pltpu.PrefetchScalarGridSpec(
            num_scalar_prefetch=1,
            grid=(steps,),
            in_specs=[
                pl.BlockSpec((tile, width), lambda i, s: (at(i, s), 0)),
                pl.BlockSpec((tile, 128), lambda i, s: (at(i, s), 0)),
                pl.BlockSpec((tile, 128), lambda i, s: (at(i, s), 0)),
                pl.BlockSpec((tile, 128), lambda i, s: (at(i, s), 0)),
                pl.BlockSpec((32, tile), lambda i, s: (0, at(i, s))),
                pl.BlockSpec((parts, 128, width), lambda i, s: (at(i, s), 0, 0)),
                pl.BlockSpec((1, width), lambda i, s: (0, 0)),
            ],
            out_specs=pl.BlockSpec((tile, width), lambda i, s: (i, 0)),
        ),
        out_shape=jax.ShapeDtypeStruct((rows, width), bf16),
        compiler_params=pltpu.CompilerParams(dimension_semantics=("arbitrary",)),
        name="local",
    )(scalars, x, b, c, meta, row, before, skip)


def gate_kernel(scalars, block, y_ref, g_ref, c_ref, meta_ref, mine_ref, other_ref, out_ref):
    rows, width = y_ref.shape
    half = width // 2
    low = scalars[1] == 0
    grown = jnp.exp2(meta_ref[...])
    first = block * pl.num_programs(0) + pl.program_id(0)
    live = (first * rows + iota((rows, 1), 0) < scalars[0]).astype(f32)
    for place in (0, 1):
        held = jnp.where(
            low == (place == 0), mine_ref[...].astype(f32), other_ref[...].astype(f32)
        ).astype(bf16)
        wide = jnp.dot(c_ref[...], held, preferred_element_type=f32)
        for k in range(half // 128):
            cols = slice(place * half + k * 128, place * half + (k + 1) * 128)
            q = place * (half // 128) + k
            y = y_ref[:, cols].astype(f32) + pair(grown, 64 + 2 * q) * wide[:, k * 128 : (k + 1) * 128]
            g = g_ref[:, cols].astype(f32)
            out_ref[:, cols] = (y * live * (g / (1.0 + jnp.exp2(g * -LOG2E)))).astype(bf16)


def gate(scalars, y, g, c, meta, mine, other, block):
    rows, width = y.shape
    tile = 256
    steps = rows // tile

    def at(i, s):
        return s[2 + block] * steps + i

    def body(s, *refs):
        gate_kernel(s, s[2 + block], *refs)

    return pl.pallas_call(
        body,
        grid_spec=pltpu.PrefetchScalarGridSpec(
            num_scalar_prefetch=1,
            grid=(steps,),
            in_specs=[
                pl.BlockSpec((tile, width), lambda i, s: (i, 0)),
                pl.BlockSpec((tile, width), lambda i, s: (at(i, s), 0)),
                pl.BlockSpec((tile, 128), lambda i, s: (at(i, s), 0)),
                pl.BlockSpec((tile, 128), lambda i, s: (at(i, s), 0)),
                pl.BlockSpec((128, width // 2), lambda i, s: (0, 0)),
                pl.BlockSpec((128, width // 2), lambda i, s: (0, 0)),
            ],
            out_specs=pl.BlockSpec((tile, width), lambda i, s: (i, 0)),
        ),
        out_shape=jax.ShapeDtypeStruct((rows, width), bf16),
        compiler_params=pltpu.CompilerParams(dimension_semantics=("arbitrary",)),
        name="gate",
    )(scalars, y, g, c, meta, mine, other)


def unpack(message):
    decay = message[128].astype(f32) + message[129].astype(f32)
    return message[:128].astype(f32), decay


def pack(state, decay):
    high = decay.astype(bf16)
    low = (decay - high.astype(f32)).astype(bf16)
    rest = jnp.zeros((14, decay.shape[0]), bf16)
    return jnp.concatenate([state.astype(bf16), high[None], low[None], rest], axis=0)


def join(earlier, later):
    return (
        jnp.exp2(later[1])[None, :] * earlier[0] + later[0],
        earlier[1] + later[1],
    )


def shift(value, axis, by):
    count = lax.axis_size(axis)
    return lax.ppermute(value, axis, [(i, (i + by) % count) for i in range(count)])


def gather_ring(value, axis):
    count, place = lax.axis_size(axis), lax.axis_index(axis)
    got = [value] + [shift(value, axis, by) for by in range(1, count)]
    return [
        lax.select_n((place - k) % count, *got) for k in range(count)
    ]


def before_in(pieces, place):
    zero = (jnp.zeros((128, pieces[0].shape[1]), f32), jnp.zeros((pieces[0].shape[1],), f32))
    inside, running = zero, zero
    for k, piece in enumerate(pieces):
        running = join(running, unpack(piece)) if k else unpack(piece)
        passed = k < place
        inside = jax.tree.map(lambda new, old: jnp.where(passed, new, old), running, inside)
    return inside, running


def incoming(mine, other, core):
    theirs = shift(other, "seq_2", 1)
    first = lax.select_n(core, mine, theirs)
    second = lax.select_n(core, theirs, mine)
    lone = unpack(first)
    chip = join(lone, unpack(second))
    inside_y, row = before_in(gather_ring(pack(*chip), "seq_1"), lax.axis_index("seq_1"))
    inside_x, _ = before_in(gather_ring(pack(*row), "seq_0"), lax.axis_index("seq_0"))
    start = join(inside_x, inside_y)
    middle = join(start, lone)
    own = lax.select_n(core, start[0], middle[0]).astype(bf16)
    away = lax.select_n(core, middle[0], start[0]).astype(bf16)
    return own, shift(away, "seq_2", 1)


def body(
    values,
    gates,
    b_proj,
    c_proj,
    step_size,
    decay_rate,
    skip_gain,
    norm_gain,
    readout_matrix,
    span_counts,
    remaining_count,
):
    length, width = values.shape
    valid = (span_counts[0] - 1) * SPAN + remaining_count[0]
    core = lax.axis_index("seq_2")
    place = lax.axis_index("head")
    order = jnp.arange(4, dtype=jnp.int32)
    scalars = jnp.concatenate([jnp.stack([valid, core]).astype(jnp.int32), order])
    skip = jnp.repeat(skip_gain, P_SIZE)[None, :]
    before, meta, row, mine, other = states(scalars, values, b_proj, decay_rate, step_size)
    own, theirs = incoming(mine, other, core)
    rows = length // 4
    gated = []
    for block in range(4):
        y = local(scalars, values, b_proj, c_proj, meta, row, before, skip, block, rows)
        gated.append(gate(scalars, y, gates, c_proj, meta, own, theirs, block))
    gated = jnp.concatenate(gated, axis=0)
    wide = gated.astype(f32)
    ss = jnp.sum(wide * wide, axis=1)
    squares = lax.psum_scatter(ss, "head", scatter_dimension=0, tiled=True)
    scaled = (readout_matrix.astype(f32) * norm_gain[:, None]).astype(bf16)
    summed = lax.psum_scatter(
        jnp.dot(gated, scaled, preferred_element_type=f32).astype(bf16),
        "head",
        scatter_dimension=0,
        tiled=True,
    ).astype(f32)
    return (summed * lax.rsqrt(squares / (HEADS * P_SIZE) + 1e-05)[:, None]).astype(bf16)


def solution(mesh):
    finer = Mesh(
        mesh.devices.reshape(4, 4, 2, mesh.shape["head"]), ("seq_0", "seq_1", "seq_2", "head")
    )
    return jax.shard_map(
        body,
        mesh=finer,
        in_specs=(
            P(SEQ, "head"),
            P(SEQ, "head"),
            P(SEQ, None),
            P(SEQ, None),
            P("head", SEQ),
            P("head", SEQ),
            P("head"),
            P("head"),
            P("head", None),
            P(SEQ),
            P(SEQ),
        ),
        out_specs=P(SEQ_HEAD, None),
        check_vma=False,
    )
```

```python
import jax
import jax.numpy as jnp
from jax import lax
from jax.experimental import pallas as pl
from jax.experimental.pallas import tpu as pltpu
from jax.sharding import Mesh
from jax.sharding import PartitionSpec as P

HEADS = 80
P_SIZE = 64
SPAN = 256
PART = 128
SEQ = ("seq_0", "seq_1", "seq_2")
SEQ_HEAD = ("seq_0", "seq_1", "seq_2", "head")
LOG2E = 1.4426950408889634
HIGHEST = lax.Precision.HIGHEST
f32 = jnp.float32
bf16 = jnp.bfloat16


def iota(shape, dim):
    return lax.broadcasted_iota(jnp.int32, shape, dim)


def selector(width):
    rows, cols = iota((256, width), 0), iota((256, width), 1)
    return ((rows % 32) == cols // P_SIZE).astype(f32).astype(bf16)


def spread(columns, group, chosen):
    lane = iota(columns.shape, 1)
    columns = jnp.where((lane >= 32 * group) & (lane < 32 * group + 32), columns, 0.0)
    high = columns.astype(bf16)
    low = (columns - high.astype(f32)).astype(bf16)
    return jnp.dot(
        jnp.concatenate([high, low], axis=1), chosen, preferred_element_type=f32
    )


def states_kernel(
    scalars, x_ref, b_ref, rate_ref, dt_ref,
    meta_ref, row_ref, turned_ref, chosen_ref, mine_ref, other_ref,
    state, raw, weighted,
):
    step = pl.program_id(0)
    heads, length = rate_ref.shape
    parts = length // PART
    rows, width = x_ref.shape
    half = width // 2

    @pl.when(step == 0)
    def _():
        state[...] = jnp.zeros_like(state)
        raw[...] = jnp.zeros_like(raw)
        chosen_ref[...] = selector(width)
        for k in range(parts):
            at = slice(k * PART, (k + 1) * PART)
            live = (k * PART + iota((1, PART), 1) < scalars[0]).astype(f32)
            raw[0, 32 * k : 32 * k + heads, :] = rate_ref[:, at] * (live * -LOG2E)
            raw[1, 32 * k : 32 * k + heads, :] = dt_ref[:, at] * live
        upper = (iota((PART, PART), 0) <= iota((PART, PART), 1)).astype(f32)
        running = jnp.dot(raw[0], upper, precision=HIGHEST, preferred_element_type=f32)
        ends = jnp.broadcast_to(running[:, PART - 1 : PART], running.shape)
        leads = [jnp.zeros((32, PART), f32)]
        for k in range(parts):
            leads.append(leads[-1] + ends[32 * k : 32 * k + 32])
        for k in range(parts):
            at = slice(k * PART, (k + 1) * PART)
            run = running[32 * k : 32 * k + 32]
            weight = raw[1, 32 * k : 32 * k + 32, :]
            total = leads[k] + run
            row_ref[:, at] = run - jnp.where(weight > 0, jnp.log(weight) * LOG2E, -1e30)
            tail = jnp.exp2(ends[32 * k : 32 * k + 32] - run) * weight
            last = jnp.exp2(leads[parts] - total) * weight
            meta_ref[at, :] = jnp.concatenate([run, tail, total, last], axis=0).T

    here = pl.ds(pl.multiple_of(step * rows, rows), rows)
    wide = spread(meta_ref[here, :], 3, chosen_ref[...])
    weighted[...] = (x_ref[...].astype(f32) * wide).astype(bf16)
    turned = b_ref[...].astype(f32).T.astype(bf16)
    turned_ref[...] = turned
    state[...] += jnp.dot(turned, weighted[...], preferred_element_type=f32)

    @pl.when(step == pl.num_programs(0) - 1)
    def _():
        wide = spread(meta_ref[length - 16 : length, :], 2, chosen_ref[...])[15:16, :]
        high = wide.astype(bf16).astype(f32)
        line = iota((16, width), 0)
        decay = jnp.where(line == 0, high, jnp.where(line == 1, wide - high, 0.0))
        core = scalars[1]
        for place, ref in ((0, mine_ref), (1, other_ref)):
            low = core == place
            ref[0:128, :] = jnp.where(low, state[:, :half], state[:, half:]).astype(bf16)
            ref[128:144, :] = jnp.where(low, decay[:, :half], decay[:, half:]).astype(bf16)


def states(scalars, x, b, rate, dt):
    length, width = x.shape
    heads = rate.shape[0]
    steps = 4
    rows = length // steps
    one = lambda i, s: (0, 0)
    return pl.pallas_call(
        states_kernel,
        grid_spec=pltpu.PrefetchScalarGridSpec(
            num_scalar_prefetch=1,
            grid=(steps,),
            in_specs=[
                pl.BlockSpec((rows, width), lambda i, s: (i, 0)),
                pl.BlockSpec((rows, 128), lambda i, s: (i, 0)),
                pl.BlockSpec((heads, length), one),
                pl.BlockSpec((heads, length), one),
            ],
            out_specs=[
                pl.BlockSpec((length, 128), one),
                pl.BlockSpec((32, length), one),
                pl.BlockSpec((128, rows), lambda i, s: (0, i)),
                pl.BlockSpec((256, width), one),
                pl.BlockSpec((144, width // 2), one),
                pl.BlockSpec((144, width // 2), one),
            ],
            scratch_shapes=[
                pltpu.VMEM((128, width), f32),
                pltpu.VMEM((2, 32 * (length // PART), PART), f32),
                pltpu.VMEM((rows, width), bf16),
            ],
        ),
        out_shape=[
            jax.ShapeDtypeStruct((length, 128), f32),
            jax.ShapeDtypeStruct((32, length), f32),
            jax.ShapeDtypeStruct((128, length), bf16),
            jax.ShapeDtypeStruct((256, width), bf16),
            jax.ShapeDtypeStruct((144, width // 2), bf16),
            jax.ShapeDtypeStruct((144, width // 2), bf16),
        ],
        compiler_params=pltpu.CompilerParams(dimension_semantics=("arbitrary",)),
        name="states",
    )(scalars, x, b, rate, dt)


def local_kernel(
    share, x_ref, b_ref, c_ref, turned_ref, meta_ref, row_ref, chosen_ref, skip_ref, from_ref,
    y_ref, state,
):
    width = x_ref.shape[1]
    pairs = width // 128
    lower = iota((PART, PART), 0) >= iota((PART, PART), 1)
    left = iota((PART, 128), 1) < 64

    @pl.when(pl.program_id(0) == 0)
    def _():
        state[...] = from_ref[...]

    for k in range(x_ref.shape[0] // PART):
        at = slice(k * PART, (k + 1) * PART)
        gram = lax.dot_general(
            c_ref[at, :], b_ref[at, :], (((1,), (1,)), ((), ())), preferred_element_type=f32
        )
        gram = jnp.where(lower, gram, 0.0)
        meta = meta_ref[at, :]
        grown = spread(jnp.exp2(meta), 0, chosen_ref[...])
        tail = spread(meta, 1, chosen_ref[...])
        held = jnp.dot(c_ref[at, :], state[...].astype(bf16), preferred_element_type=f32)
        fresh = []
        for q in range(pairs):
            cols = slice(q * 128, (q + 1) * 128)
            both = []
            for h in (2 * q, 2 * q + 1):
                power = jnp.minimum(meta[:, h : h + 1] - row_ref[h : h + 1, at], 100.0)
                both.append((gram * jnp.exp2(power)).astype(bf16))
            x = x_ref[at, cols]
            wide = x.astype(f32)
            none = jnp.zeros_like(x)
            stack = jnp.concatenate([jnp.where(left, x, none), jnp.where(left, none, x)], axis=0)
            inner = jnp.dot(jnp.concatenate(both, axis=1), stack, preferred_element_type=f32)
            y = inner + grown[:, cols] * held[:, cols] + skip_ref[0:1, cols] * wide
            y_ref[at, cols] = y.astype(bf16)
            fresh.append((wide * tail[:, cols]).astype(bf16))
        fresh = jnp.dot(
            turned_ref[:, at], jnp.concatenate(fresh, axis=1), preferred_element_type=f32
        )
        state[...] = state[...] * grown[PART - 1 : PART, :] + fresh


def local(x, b, c, turned, meta, row, chosen, skip, state, share, shares):
    length, width = x.shape
    tile = 256
    steps = length // tile // shares
    by_row = lambda i, s: (s[0] * steps + i, 0)
    by_column = lambda i, s: (0, s[0] * steps + i)
    one = lambda i, s: (0, 0)
    return pl.pallas_call(
        local_kernel,
        grid_spec=pltpu.PrefetchScalarGridSpec(
            num_scalar_prefetch=1,
            grid=(steps,),
            in_specs=[
            pl.BlockSpec((tile, width), by_row),
            pl.BlockSpec((tile, 128), by_row),
            pl.BlockSpec((tile, 128), by_row),
            pl.BlockSpec((128, tile), by_column),
            pl.BlockSpec((tile, 128), by_row),
            pl.BlockSpec((32, tile), by_column),
            pl.BlockSpec((256, width), one),
            pl.BlockSpec((1, width), one),
            pl.BlockSpec((128, width), one),
            ],
            out_specs=[
                pl.BlockSpec((tile, width), lambda i, s: (i, 0)),
                pl.BlockSpec((128, width), one),
            ],
        ),
        out_shape=[
            jax.ShapeDtypeStruct((length // shares, width), bf16),
            jax.ShapeDtypeStruct((128, width), f32),
        ],
        compiler_params=pltpu.CompilerParams(dimension_semantics=("arbitrary",)),
        name="local",
    )(jnp.full((1,), share, jnp.int32), x, b, c, turned, meta, row, chosen, skip, state)


def gate_kernel(
    scalars, block, first_ref, second_ref, g_ref, c_ref, meta_ref, chosen_ref, mine_ref, other_ref,
    gain_ref, matrix_ref, top_ref, low_ref, ss_ref, matrix, gated, sem,
):
    rows, width = g_ref.shape
    half = width // 2
    first = block * rows

    @pl.when(first >= scalars[0])
    def _():
        top_ref[...] = jnp.zeros_like(top_ref)
        low_ref[...] = jnp.zeros_like(low_ref)
        ss_ref[...] = jnp.zeros_like(ss_ref)

    @pl.when(first < scalars[0])
    def _():
        copy = pltpu.make_async_copy(matrix_ref, matrix, sem)
        copy.start()
        low = scalars[1] == 0
        early = block < 2
        held = []
        for place in (0, 1):
            picked = jnp.where(
                low == (place == 0), mine_ref[...].astype(f32), other_ref[...].astype(f32)
            )
            held.append(picked.astype(bf16))

        def piece(k, _):
            at = pl.ds(pl.multiple_of(k * PART, PART), PART)
            grown = spread(jnp.exp2(meta_ref[at, :]), 2, chosen_ref[...])
            live = (first + k * PART + iota((PART, 1), 0) < scalars[0]).astype(f32)
            squares = jnp.zeros((PART, 128), f32)
            for place in (0, 1):
                wide = jnp.dot(c_ref[at, :], held[place], preferred_element_type=f32)
                for j in range(half // 128):
                    cols = slice(place * half + j * 128, place * half + (j + 1) * 128)
                    y = jnp.where(early, first_ref[at, cols], second_ref[at, cols]).astype(f32)
                    y = y + grown[:, cols] * wide[:, j * 128 : (j + 1) * 128]
                    g = g_ref[at, cols].astype(f32)
                    v = y * live * (g / (1.0 + jnp.exp2(g * -LOG2E)))
                    squares = squares + v * v
                    gated[at, cols] = (v * gain_ref[0:1, cols]).astype(bf16)
            total = jnp.sum(squares, axis=1, keepdims=True)
            ss_ref[:, at] = jnp.broadcast_to(total, (PART, 128)).T[0:8, :]
            return 0

        lax.fori_loop(0, rows // PART, piece, 0)
        copy.wait()

        def columns(n, _):
            at = pl.ds(pl.multiple_of(n * 256, 256), 256)
            out = jnp.dot(gated[...], matrix[:, at], preferred_element_type=f32)
            top_ref[:, at] = out[: rows // 2].astype(bf16)
            low_ref[:, at] = out[rows // 2 :].astype(bf16)
            return 0

        lax.fori_loop(0, top_ref.shape[1] // 256, columns, 0)


def gate(scalars, ys, g, c, meta, chosen, mine, other, gain, matrix):
    width = g.shape[1]
    wide = matrix.shape[1]
    rows = 512

    def at(i, s):
        return (s[2], 0)

    def body(s, *refs):
        gate_kernel(s, s[2], *refs)

    one = lambda i, s: (0, 0)
    return pl.pallas_call(
        body,
        grid_spec=pltpu.PrefetchScalarGridSpec(
            num_scalar_prefetch=1,
            grid=(1,),
            in_specs=[
                pl.BlockSpec((rows, width), lambda i, s: (jnp.minimum(s[2], 1), 0)),
                pl.BlockSpec((rows, width), lambda i, s: (jnp.maximum(s[2] - 2, 0), 0)),
                pl.BlockSpec((rows, width), at),
                pl.BlockSpec((rows, 128), at),
                pl.BlockSpec((rows, 128), at),
                pl.BlockSpec((256, width), one),
                pl.BlockSpec((128, width // 2), one),
                pl.BlockSpec((128, width // 2), one),
                pl.BlockSpec((1, width), one),
                pl.BlockSpec(memory_space=pl.ANY),
            ],
            out_specs=[
                pl.BlockSpec((rows // 2, wide), one),
                pl.BlockSpec((rows // 2, wide), one),
                pl.BlockSpec((8, rows), one),
            ],
            scratch_shapes=[
                pltpu.VMEM((width, wide), bf16),
                pltpu.VMEM((rows, width), bf16),
                pltpu.SemaphoreType.DMA,
            ],
        ),
        out_shape=[
            jax.ShapeDtypeStruct((rows // 2, wide), bf16),
            jax.ShapeDtypeStruct((rows // 2, wide), bf16),
            jax.ShapeDtypeStruct((8, rows), f32),
        ],
        compiler_params=pltpu.CompilerParams(dimension_semantics=("arbitrary",)),
        name="gate",
    )(scalars, *ys, g, c, meta, chosen, mine, other, gain, matrix)


def finish_kernel(own_a, own_b, up_a, up_b, down_a, down_b, s0, s1, s2, s3, out_ref):
    rows = own_a.shape[0]
    total = s0[...] + s1[...] + s2[...] + s3[...]
    scale = lax.rsqrt(total * (1.0 / (HEADS * P_SIZE)) + 1e-05)
    for k, parts in enumerate(((own_a, up_a, down_a), (own_b, up_b, down_b))):
        for j in range(rows // PART):
            at = slice(j * PART, (j + 1) * PART)
            lanes = slice(k * rows + j * PART, k * rows + (j + 1) * PART)
            factor = jnp.broadcast_to(scale[0:1, lanes], (PART, PART)).T
            for n in range(out_ref.shape[1] // 128):
                cols = slice(n * 128, (n + 1) * 128)
                value = sum(part[at, cols].astype(f32) for part in parts)
                out_ref[lanes, cols] = (value * factor).astype(bf16)


def finish(pieces, squares):
    rows, wide = pieces[0].shape
    tile = 512
    return pl.pallas_call(
        finish_kernel,
        grid=(wide // tile,),
        in_specs=[pl.BlockSpec((rows, tile), lambda i: (0, i))] * 6
        + [pl.BlockSpec((8, 2 * rows), lambda i: (0, 0))] * 4,
        out_specs=pl.BlockSpec((2 * rows, tile), lambda i: (0, i)),
        out_shape=jax.ShapeDtypeStruct((2 * rows, wide), bf16),
        compiler_params=pltpu.CompilerParams(dimension_semantics=("arbitrary",)),
        name="finish",
    )(*pieces, *squares)


def unpack(message):
    decay = message[128].astype(f32) + message[129].astype(f32)
    return message[:128].astype(f32), decay


def pack(state, decay):
    high = decay.astype(bf16)
    low = (decay - high.astype(f32)).astype(bf16)
    rest = jnp.zeros((14, decay.shape[0]), bf16)
    return jnp.concatenate([state.astype(bf16), high[None], low[None], rest], axis=0)


def join(earlier, later):
    return (
        jnp.exp2(later[1])[None, :] * earlier[0] + later[0],
        earlier[1] + later[1],
    )


def shift(value, axis, by, wrap=True):
    count = lax.axis_size(axis)
    pairs = [(i, (i + by) % count) for i in range(count) if wrap or i + by < count]
    return lax.ppermute(value, axis, pairs)


def gather_ring(value, axis, wrap=True):
    count, place = lax.axis_size(axis), lax.axis_index(axis)
    got = [value] + [shift(value, axis, by, wrap) for by in range(1, count)]
    return [lax.select_n((place - k) % count, *got) for k in range(count)]


def before_in(pieces, place):
    zero = (jnp.zeros((128, pieces[0].shape[1]), f32), jnp.zeros((pieces[0].shape[1],), f32))
    inside, running = zero, zero
    for k, piece in enumerate(pieces):
        running = join(running, unpack(piece)) if k else unpack(piece)
        passed = k < place
        inside = jax.tree.map(lambda new, old: jnp.where(passed, new, old), running, inside)
    return inside, running


def incoming(mine, other, core, first_share, second_share):
    theirs = shift(other, "seq_2", 1)
    first = lax.select_n(core, mine, theirs)
    second = lax.select_n(core, theirs, mine)
    lone = unpack(first)
    chip = join(lone, unpack(second))
    pieces = gather_ring(pack(*chip), "seq_1")
    y1, state = first_share()
    inside_y, row = before_in(pieces, lax.axis_index("seq_1"))
    message, y1, state = lax.optimization_barrier((pack(*row), y1, state))
    pieces = gather_ring(message, "seq_0", wrap=False)
    y2 = second_share(state)
    inside_x, _ = before_in(pieces, lax.axis_index("seq_0"))
    start = join(inside_x, inside_y)
    middle = join(start, lone)
    own = lax.select_n(core, start[0], middle[0]).astype(bf16)
    away = lax.select_n(core, middle[0], start[0]).astype(bf16)
    return own, shift(away, "seq_2", 1), (y1, y2)


def body(
    values,
    gates,
    b_proj,
    c_proj,
    step_size,
    decay_rate,
    skip_gain,
    norm_gain,
    readout_matrix,
    span_counts,
    remaining_count,
):
    length, width = values.shape
    valid = (span_counts[0] - 1) * SPAN + remaining_count[0]
    core = lax.axis_index("seq_2")
    place = lax.axis_index("head")
    roles = [
        jnp.stack([valid, core, (place + role) % 4]).astype(jnp.int32) for role in range(4)
    ]
    scalars = roles[0]
    skip = jnp.repeat(skip_gain, P_SIZE)[None, :]
    meta, row, turned, chosen, mine, other = states(scalars, values, b_proj, decay_rate, step_size)
    zero = jnp.zeros((128, width), f32)

    def share(state, k):
        return local(
            values, b_proj, c_proj, turned, meta, row, chosen, skip, state, k, 2
        )

    own, theirs, ys = incoming(
        mine, other, core, lambda: share(zero, 0), lambda state: share(state, 1)[0]
    )
    gain = norm_gain[None, :]

    def part(role):
        return gate(
            roles[role], ys, gates, c_proj, meta, chosen, own, theirs, gain, readout_matrix
        )

    def reduced(blocks):
        def send(value, by, role):
            pairs = [(z, (z + by) % 4) for z in range(4) if (z + role) % 4 < blocks]
            return lax.ppermute(value, "head", pairs)

        def run():
            far_a, far_b, s2 = part(2)
            far_a, far_b = send(far_a, 1, 2), send(far_b, -1, 2)
            up_a, up_b, s1 = part(1)
            up_b = send(up_b, 1, 1)
            down_a, down_b, s3 = part(3)
            down_a = send(down_a, -1, 3)
            up_a = send((up_a.astype(f32) + far_a.astype(f32)).astype(bf16), 1, 1)
            down_b = send((down_b.astype(f32) + far_b.astype(f32)).astype(bf16), -1, 3)
            s2, s1, s3 = send(s2, 2, 2), send(s1, 1, 1), send(s3, -1, 3)
            own_a, own_b, s0 = part(0)
            return (own_a, own_b, up_a, up_b, down_a, down_b), (s0, s1, s2, s3)

        return run

    quarter = length // 4
    level = (valid > quarter).astype(jnp.int32) + (valid > 2 * quarter)
    return finish(*lax.switch(level, [reduced(n) for n in (1, 2, 4)]))


def solution(mesh):
    finer = Mesh(
        mesh.devices.reshape(4, 4, 2, mesh.shape["head"]), ("seq_0", "seq_1", "seq_2", "head")
    )
    return jax.shard_map(
        body,
        mesh=finer,
        in_specs=(
            P(SEQ, "head"),
            P(SEQ, "head"),
            P(SEQ, None),
            P(SEQ, None),
            P("head", SEQ),
            P("head", SEQ),
            P("head"),
            P("head"),
            P("head", None),
            P(SEQ),
            P(SEQ),
        ),
        out_specs=P(SEQ_HEAD, None),
        check_vma=False,
    )
```

```python
import jax
import jax.numpy as jnp
from jax import lax
from jax.experimental import pallas as pl
from jax.experimental.pallas import tpu as pltpu
from jax.sharding import Mesh
from jax.sharding import PartitionSpec as P

HEADS = 80
P_SIZE = 64
SPAN = 256
PART = 128
SEQ = ("seq_0", "seq_1", "seq_2")
SEQ_HEAD = ("seq_0", "seq_1", "seq_2", "head")
LOG2E = 1.4426950408889634
HIGHEST = lax.Precision.HIGHEST
f32 = jnp.float32
bf16 = jnp.bfloat16


def iota(shape, dim):
    return lax.broadcasted_iota(jnp.int32, shape, dim)


def selector(width):
    rows, cols = iota((256, width), 0), iota((256, width), 1)
    return ((rows % 32) == cols // P_SIZE).astype(f32).astype(bf16)


def spread(columns, group, chosen):
    lane = iota(columns.shape, 1)
    columns = jnp.where((lane >= 32 * group) & (lane < 32 * group + 32), columns, 0.0)
    high = columns.astype(bf16)
    low = (columns - high.astype(f32)).astype(bf16)
    return jnp.dot(
        jnp.concatenate([high, low], axis=1), chosen, preferred_element_type=f32
    )


def states_kernel(
    scalars, x_ref, b_ref, rate_ref, dt_ref,
    meta_ref, row_ref, turned_ref, chosen_ref, mine_ref, other_ref,
    state, raw, weighted,
):
    step = pl.program_id(0)
    heads, length = rate_ref.shape
    parts = length // PART
    rows, width = x_ref.shape
    half = width // 2

    @pl.when(step == 0)
    def _():
        state[...] = jnp.zeros_like(state)
        raw[...] = jnp.zeros_like(raw)
        chosen_ref[...] = selector(width)
        for k in range(parts):
            at = slice(k * PART, (k + 1) * PART)
            live = (k * PART + iota((1, PART), 1) < scalars[0]).astype(f32)
            raw[0, 32 * k : 32 * k + heads, :] = rate_ref[:, at] * (live * -LOG2E)
            raw[1, 32 * k : 32 * k + heads, :] = dt_ref[:, at] * live
        upper = (iota((PART, PART), 0) <= iota((PART, PART), 1)).astype(f32)
        running = jnp.dot(raw[0], upper, precision=HIGHEST, preferred_element_type=f32)
        ends = jnp.broadcast_to(running[:, PART - 1 : PART], running.shape)
        leads = [jnp.zeros((32, PART), f32)]
        for k in range(parts):
            leads.append(leads[-1] + ends[32 * k : 32 * k + 32])
        for k in range(parts):
            at = slice(k * PART, (k + 1) * PART)
            run = running[32 * k : 32 * k + 32]
            weight = raw[1, 32 * k : 32 * k + 32, :]
            total = leads[k] + run
            row_ref[:, at] = run - jnp.where(weight > 0, jnp.log(weight) * LOG2E, -1e30)
            tail = jnp.exp2(ends[32 * k : 32 * k + 32] - run) * weight
            last = jnp.exp2(leads[parts] - total) * weight
            meta_ref[at, :] = jnp.concatenate([run, tail, total, last], axis=0).T

    here = pl.ds(pl.multiple_of(step * rows, rows), rows)
    wide = spread(meta_ref[here, :], 3, chosen_ref[...])
    weighted[...] = (x_ref[...].astype(f32) * wide).astype(bf16)
    turned = b_ref[...].astype(f32).T.astype(bf16)
    turned_ref[...] = turned
    state[...] += jnp.dot(turned, weighted[...], preferred_element_type=f32)

    @pl.when(step == pl.num_programs(0) - 1)
    def _():
        wide = spread(meta_ref[length - 16 : length, :], 2, chosen_ref[...])[15:16, :]
        high = wide.astype(bf16).astype(f32)
        line = iota((16, width), 0)
        decay = jnp.where(line == 0, high, jnp.where(line == 1, wide - high, 0.0))
        core = scalars[1]
        for place, ref in ((0, mine_ref), (1, other_ref)):
            low = core == place
            ref[0:128, :] = jnp.where(low, state[:, :half], state[:, half:]).astype(bf16)
            ref[128:144, :] = jnp.where(low, decay[:, :half], decay[:, half:]).astype(bf16)


def states(scalars, x, b, rate, dt):
    length, width = x.shape
    heads = rate.shape[0]
    steps = 4
    rows = length // steps
    one = lambda i, s: (0, 0)
    return pl.pallas_call(
        states_kernel,
        grid_spec=pltpu.PrefetchScalarGridSpec(
            num_scalar_prefetch=1,
            grid=(steps,),
            in_specs=[
                pl.BlockSpec((rows, width), lambda i, s: (i, 0)),
                pl.BlockSpec((rows, 128), lambda i, s: (i, 0)),
                pl.BlockSpec((heads, length), one),
                pl.BlockSpec((heads, length), one),
            ],
            out_specs=[
                pl.BlockSpec((length, 128), one),
                pl.BlockSpec((32, length), one),
                pl.BlockSpec((128, rows), lambda i, s: (0, i)),
                pl.BlockSpec((256, width), one),
                pl.BlockSpec((144, width // 2), one),
                pl.BlockSpec((144, width // 2), one),
            ],
            scratch_shapes=[
                pltpu.VMEM((128, width), f32),
                pltpu.VMEM((2, 32 * (length // PART), PART), f32),
                pltpu.VMEM((rows, width), bf16),
            ],
        ),
        out_shape=[
            jax.ShapeDtypeStruct((length, 128), f32),
            jax.ShapeDtypeStruct((32, length), f32),
            jax.ShapeDtypeStruct((128, length), bf16),
            jax.ShapeDtypeStruct((256, width), bf16),
            jax.ShapeDtypeStruct((144, width // 2), bf16),
            jax.ShapeDtypeStruct((144, width // 2), bf16),
        ],
        compiler_params=pltpu.CompilerParams(dimension_semantics=("arbitrary",)),
        name="states",
    )(scalars, x, b, rate, dt)


def local_kernel(
    share, x_ref, b_ref, c_ref, turned_ref, meta_ref, row_ref, chosen_ref, skip_ref, *rest,
):
    y_ref, state = rest[-2:]
    width = x_ref.shape[1]
    pairs = width // 128
    lower = iota((PART, PART), 0) >= iota((PART, PART), 1)
    left = iota((PART, 128), 1) < 64

    @pl.when(pl.program_id(0) == 0)
    def _():
        state[...] = rest[0][...] if len(rest) == 4 else jnp.zeros_like(state)

    for k in range(x_ref.shape[0] // PART):
        at = slice(k * PART, (k + 1) * PART)
        gram = lax.dot_general(
            c_ref[at, :], b_ref[at, :], (((1,), (1,)), ((), ())), preferred_element_type=f32
        )
        gram = jnp.where(lower, gram, 0.0)
        meta = meta_ref[at, :]
        grown = spread(jnp.exp2(meta), 0, chosen_ref[...])
        tail = spread(meta, 1, chosen_ref[...])
        held = jnp.dot(c_ref[at, :], state[...].astype(bf16), preferred_element_type=f32)
        fresh = []
        for q in range(pairs):
            cols = slice(q * 128, (q + 1) * 128)
            both = []
            for h in (2 * q, 2 * q + 1):
                power = jnp.minimum(meta[:, h : h + 1] - row_ref[h : h + 1, at], 100.0)
                both.append((gram * jnp.exp2(power)).astype(bf16))
            x = x_ref[at, cols]
            wide = x.astype(f32)
            none = jnp.zeros_like(x)
            stack = jnp.concatenate([jnp.where(left, x, none), jnp.where(left, none, x)], axis=0)
            inner = jnp.dot(jnp.concatenate(both, axis=1), stack, preferred_element_type=f32)
            y = inner + grown[:, cols] * held[:, cols] + skip_ref[0:1, cols] * wide
            y_ref[at, cols] = y.astype(bf16)
            fresh.append((wide * tail[:, cols]).astype(bf16))
        fresh = jnp.dot(
            turned_ref[:, at], jnp.concatenate(fresh, axis=1), preferred_element_type=f32
        )
        state[...] = state[...] * grown[PART - 1 : PART, :] + fresh


def local(x, b, c, turned, meta, row, chosen, skip, share, shares, before=()):
    length, width = x.shape
    tile = 256
    steps = length // tile // shares
    by_row = lambda i, s: (share * steps + i, 0)
    by_column = lambda i, s: (0, share * steps + i)
    one = lambda i, s: (0, 0)
    return pl.pallas_call(
        local_kernel,
        grid_spec=pltpu.PrefetchScalarGridSpec(
            num_scalar_prefetch=1,
            grid=(steps,),
            in_specs=[
                pl.BlockSpec((tile, width), by_row),
                pl.BlockSpec((tile, 128), by_row),
                pl.BlockSpec((tile, 128), by_row),
                pl.BlockSpec((128, tile), by_column),
                pl.BlockSpec((tile, 128), by_row),
                pl.BlockSpec((32, tile), by_column),
                pl.BlockSpec((256, width), one),
                pl.BlockSpec((1, width), one),
            ]
            + [pl.BlockSpec((128, width), one), pl.BlockSpec(memory_space=pl.ANY)] * (len(before) // 2),
            out_specs=[
                pl.BlockSpec((tile, width), by_row),
                pl.BlockSpec((128, width), one),
            ],
        ),
        out_shape=[
            jax.ShapeDtypeStruct((length, width), bf16),
            jax.ShapeDtypeStruct((128, width), f32),
        ],
        input_output_aliases={10: 0} if before else {},
        compiler_params=pltpu.CompilerParams(dimension_semantics=("arbitrary",)),
        name="local",
    )(jnp.zeros((1,), jnp.int32), x, b, c, turned, meta, row, chosen, skip, *before)


def gate_kernel(
    scalars, block, y_ref, g_ref, c_ref, meta_ref, chosen_ref, mine_ref, other_ref,
    gain_ref, matrix_ref, top_ref, low_ref, ss_ref, matrix, gated, sem,
):
    rows, width = g_ref.shape
    half = width // 2
    first = block * rows

    @pl.when(first >= scalars[0])
    def _():
        top_ref[...] = jnp.zeros_like(top_ref)
        low_ref[...] = jnp.zeros_like(low_ref)
        ss_ref[...] = jnp.zeros_like(ss_ref)

    @pl.when(first < scalars[0])
    def _():
        copy = pltpu.make_async_copy(matrix_ref, matrix, sem)
        copy.start()
        low = scalars[1] == 0
        held = []
        for place in (0, 1):
            picked = jnp.where(
                low == (place == 0), mine_ref[...].astype(f32), other_ref[...].astype(f32)
            )
            held.append(picked.astype(bf16))

        def piece(k, _):
            at = pl.ds(pl.multiple_of(k * PART, PART), PART)
            grown = spread(jnp.exp2(meta_ref[at, :]), 2, chosen_ref[...])
            live = (first + k * PART + iota((PART, 1), 0) < scalars[0]).astype(f32)
            squares = jnp.zeros((PART, 128), f32)
            for place in (0, 1):
                wide = jnp.dot(c_ref[at, :], held[place], preferred_element_type=f32)
                for j in range(half // 128):
                    cols = slice(place * half + j * 128, place * half + (j + 1) * 128)
                    y = y_ref[at, cols].astype(f32)
                    y = y + grown[:, cols] * wide[:, j * 128 : (j + 1) * 128]
                    g = g_ref[at, cols].astype(f32)
                    v = y * live * (g / (1.0 + jnp.exp2(g * -LOG2E)))
                    squares = squares + v * v
                    gated[at, cols] = (v * gain_ref[0:1, cols]).astype(bf16)
            total = jnp.sum(squares, axis=1, keepdims=True)
            ss_ref[:, at] = jnp.broadcast_to(total, (PART, 128)).T[0:8, :]
            return 0

        lax.fori_loop(0, rows // PART, piece, 0)
        copy.wait()

        def columns(n, _):
            at = pl.ds(pl.multiple_of(n * 256, 256), 256)
            out = jnp.dot(gated[...], matrix[:, at], preferred_element_type=f32)
            top_ref[:, at] = out[: rows // 2].astype(bf16)
            low_ref[:, at] = out[rows // 2 :].astype(bf16)
            return 0

        lax.fori_loop(0, top_ref.shape[1] // 256, columns, 0)


def gate(scalars, y, g, c, meta, chosen, mine, other, gain, matrix):
    width = g.shape[1]
    wide = matrix.shape[1]
    rows = 512

    def at(i, s):
        return (s[2], 0)

    def body(s, *refs):
        gate_kernel(s, s[2], *refs)

    one = lambda i, s: (0, 0)
    return pl.pallas_call(
        body,
        grid_spec=pltpu.PrefetchScalarGridSpec(
            num_scalar_prefetch=1,
            grid=(1,),
            in_specs=[
                pl.BlockSpec((rows, width), at),
                pl.BlockSpec((rows, width), at),
                pl.BlockSpec((rows, 128), at),
                pl.BlockSpec((rows, 128), at),
                pl.BlockSpec((256, width), one),
                pl.BlockSpec((128, width // 2), one),
                pl.BlockSpec((128, width // 2), one),
                pl.BlockSpec((1, width), one),
                pl.BlockSpec(memory_space=pl.ANY),
            ],
            out_specs=[
                pl.BlockSpec((rows // 2, wide), one),
                pl.BlockSpec((rows // 2, wide), one),
                pl.BlockSpec((8, rows), one),
            ],
            scratch_shapes=[
                pltpu.VMEM((width, wide), bf16),
                pltpu.VMEM((rows, width), bf16),
                pltpu.SemaphoreType.DMA,
            ],
        ),
        out_shape=[
            jax.ShapeDtypeStruct((rows // 2, wide), bf16),
            jax.ShapeDtypeStruct((rows // 2, wide), bf16),
            jax.ShapeDtypeStruct((8, rows), f32),
        ],
        compiler_params=pltpu.CompilerParams(dimension_semantics=("arbitrary",)),
        name="gate",
    )(scalars, y, g, c, meta, chosen, mine, other, gain, matrix)


def finish_kernel(own_a, own_b, last_a, last_b, s0, s1, s2, s3, out_ref):
    rows = own_a.shape[0]
    total = s0[...] + s1[...] + s2[...] + s3[...]
    scale = lax.rsqrt(total * (1.0 / (HEADS * P_SIZE)) + 1e-05)
    for k, parts in enumerate(((own_a, last_a), (own_b, last_b))):
        for j in range(rows // PART):
            at = slice(j * PART, (j + 1) * PART)
            lanes = slice(k * rows + j * PART, k * rows + (j + 1) * PART)
            factor = jnp.broadcast_to(scale[0:1, lanes], (PART, PART)).T
            for n in range(out_ref.shape[1] // 128):
                cols = slice(n * 128, (n + 1) * 128)
                value = sum(part[at, cols].astype(f32) for part in parts)
                out_ref[lanes, cols] = (value * factor).astype(bf16)


def finish(pieces, squares):
    rows, wide = pieces[0].shape
    tile = 640
    return pl.pallas_call(
        finish_kernel,
        grid=(wide // tile,),
        in_specs=[pl.BlockSpec((rows, tile), lambda i: (0, i))] * 4
        + [pl.BlockSpec((8, 2 * rows), lambda i: (0, 0))] * 4,
        out_specs=pl.BlockSpec((2 * rows, tile), lambda i: (0, i)),
        out_shape=jax.ShapeDtypeStruct((2 * rows, wide), bf16),
        compiler_params=pltpu.CompilerParams(dimension_semantics=("arbitrary",)),
        name="finish",
    )(*pieces, *squares)


def unpack(ref):
    tail = ref[128:144, :].astype(f32)
    return ref[0:128, :].astype(f32), tail[0:1, :] + tail[1:2, :]


def pack(ref, state, decay):
    ref[0:128, :] = state.astype(bf16)
    high = decay.astype(bf16).astype(f32)
    line = iota((16, decay.shape[1]), 0)
    ref[128:144, :] = jnp.where(
        line == 0, high, jnp.where(line == 1, decay - high, 0.0)
    ).astype(bf16)


def join(earlier, later):
    return jnp.exp2(later[1]) * earlier[0] + later[0], earlier[1] + later[1]


def choose(test, one, two):
    return jax.tree.map(lambda x, y: jnp.where(test, x, y), one, two)


def scan_along(place, refs):
    pieces = [unpack(ref) for ref in refs]
    zero = jax.tree.map(jnp.zeros_like, pieces[0])
    inside = running = zero
    for k in range(4):
        at = lax.rem(place - k + 4, 4)
        piece = choose(
            at < 2, choose(at == 0, pieces[0], pieces[1]), choose(at == 2, pieces[2], pieces[3])
        )
        inside = choose(place == k, running, inside)
        running = join(running, piece)
    return inside, running


def chip_kernel(places, mine, theirs, out):
    first, second = unpack(mine), unpack(theirs)
    low = places[0] == 0
    pack(out, *join(choose(low, first, second), choose(low, second, first)))


def row_kernel(places, g0, g1, g2, g3, out, state, decay):
    inside, row = scan_along(places[1], (g0, g1, g2, g3))
    pack(out, *row)
    state[...] = inside[0]
    decay[...] = jnp.broadcast_to(inside[1], decay.shape)


def entry_kernel(places, g0, g1, g2, g3, state, decay, mine, theirs, own, away):
    before, _ = scan_along(places[2], (g0, g1, g2, g3))
    start = join(before, (state[...], decay[0:1, :]))
    first = choose(places[0] == 0, unpack(mine), unpack(theirs))
    middle = join(start, first)
    low = places[0] == 0
    own[...] = jnp.where(low, start[0], middle[0]).astype(bf16)
    away[...] = jnp.where(low, middle[0], start[0]).astype(bf16)


def small_call(kernel, name, out_shapes, places, *arrays):
    whole = lambda shape: pl.BlockSpec(shape, lambda i, s: (0, 0))
    return pl.pallas_call(
        kernel,
        grid_spec=pltpu.PrefetchScalarGridSpec(
            num_scalar_prefetch=1,
            grid=(1,),
            in_specs=[whole(a.shape) for a in arrays],
            out_specs=[whole(s.shape) for s in out_shapes],
        ),
        out_shape=out_shapes,
        name=name,
    )(places, *arrays)


def shift(value, axis, by, wrap=True):
    count = lax.axis_size(axis)
    pairs = [(i, (i + by) % count) for i in range(count) if wrap or i + by < count]
    return lax.ppermute(value, axis, pairs)


def gather_ring(value, axis):
    return [value] + [shift(value, axis, by) for by in (1, 2, 3)]


def incoming(mine, other, places, first_share, second_share):
    half = mine.shape[1]
    message = jax.ShapeDtypeStruct(mine.shape, bf16)
    state = jax.ShapeDtypeStruct((128, half), f32)
    decay = jax.ShapeDtypeStruct((8, half), f32)
    held = jax.ShapeDtypeStruct((128, half), bf16)
    theirs = shift(other, "seq_2", 1)
    (chip,) = small_call(chip_kernel, "chip", [message], places, mine, theirs)
    pieces = gather_ring(chip, "seq_1")
    shared = first_share()
    row, inside, faded = small_call(row_kernel, "row", [message, state, decay], places, *pieces)
    row, shared = lax.optimization_barrier((row, shared))
    pieces = gather_ring(row, "seq_0")
    y = second_share(*shared)
    pieces, y = lax.optimization_barrier((pieces, y))
    own, away = small_call(
        entry_kernel, "entry", [held, held], places, *pieces, inside, faded, mine, theirs
    )
    return own, shift(away, "seq_2", 1), y


def body(
    values,
    gates,
    b_proj,
    c_proj,
    step_size,
    decay_rate,
    skip_gain,
    norm_gain,
    readout_matrix,
    span_counts,
    remaining_count,
):
    length, width = values.shape
    valid = (span_counts[0] - 1) * SPAN + remaining_count[0]
    core = lax.axis_index("seq_2")
    place = lax.axis_index("head")
    roles = [
        jnp.stack([valid, core, (place + role) % 4]).astype(jnp.int32) for role in range(4)
    ]
    scalars = roles[0]
    skip = jnp.repeat(skip_gain, P_SIZE)[None, :]
    meta, row, turned, chosen, mine, other = states(scalars, values, b_proj, decay_rate, step_size)

    def share(k, before=()):
        return local(
            values, b_proj, c_proj, turned, meta, row, chosen, skip, k, 2, before
        )

    places = jnp.stack([core, lax.axis_index("seq_1"), lax.axis_index("seq_0")]).astype(jnp.int32)
    own, theirs, y = incoming(
        mine, other, places, lambda: share(0), lambda y, state: share(1, (state, y))[0]
    )
    gain = norm_gain[None, :]

    def part(role, block=None):
        return gate(
            roles[role] if block is None else block, y, gates, c_proj, meta, chosen, own, theirs, gain, readout_matrix
        )

    def reduced(blocks):
        def send(value, by, role):
            pairs = [(z, (z + by) % 4) for z in range(4) if (z + role) % 4 < blocks]
            return lax.ppermute(value, "head", pairs)

        def add(one, two):
            return (one.astype(f32) + two.astype(f32)).astype(bf16)

        def all_live():
            far_a, far_b, s2 = part(2)
            far_a, far_b = send(far_a, 1, 2), send(far_b, -1, 2)
            up_a, up_b, s1 = part(1)
            up_b = send(up_b, 1, 1)
            down_a, down_b, s3 = part(3)
            down_a = send(down_a, -1, 3)
            up_a, down_b, last = lax.optimization_barrier(
                (add(up_a, far_a), add(down_b, far_b), roles[0])
            )
            up_a, down_b = send(up_a, 1, 1), send(down_b, -1, 3)
            s2, s1, s3 = send(s2, 2, 2), send(s1, 1, 1), send(s3, -1, 3)
            own_a, own_b, s0 = part(0, last)
            return (add(own_a, down_a), add(own_b, up_b), up_a, down_b), (s0, s1, s2, s3)

        def few_live():
            down_a, down_b, s3 = part(3)
            a = send(down_a, 1, 3)
            up_a, up_b, s1 = part(1)
            b = send(up_b, -1, 1)
            far_a, far_b, s2 = part(2)
            a = send(add(far_a, a), 1, 2)
            b = send(add(far_b, b), -1, 2)
            a = send(add(up_a, a), 1, 1)
            b = send(add(down_b, b), -1, 3)
            s2, s1, s3 = send(s2, 2, 2), send(s1, 1, 1), send(s3, -1, 3)
            own_a, own_b, s0 = part(0)
            return (own_a, own_b, a, b), (s0, s1, s2, s3)

        return all_live if blocks == 4 else few_live

    quarter = length // 4
    level = (valid > quarter).astype(jnp.int32) + (valid > 2 * quarter)
    return finish(*lax.switch(level, [reduced(n) for n in (1, 2, 4)]))


def solution(mesh):
    finer = Mesh(
        mesh.devices.reshape(4, 4, 2, mesh.shape["head"]), ("seq_0", "seq_1", "seq_2", "head")
    )
    return jax.shard_map(
        body,
        mesh=finer,
        in_specs=(
            P(SEQ, "head"),
            P(SEQ, "head"),
            P(SEQ, None),
            P(SEQ, None),
            P("head", SEQ),
            P("head", SEQ),
            P("head"),
            P("head"),
            P("head", None),
            P(SEQ),
            P(SEQ),
        ),
        out_specs=P(SEQ_HEAD, None),
        check_vma=False,
    )
```

```python
import jax
import jax.numpy as jnp
from jax import lax
from jax.experimental import pallas as pl
from jax.experimental.pallas import tpu as pltpu
from jax.sharding import Mesh
from jax.sharding import PartitionSpec as P

HEADS = 80
P_SIZE = 64
SPAN = 256
PART = 128
SEQ = ("seq_0", "seq_1", "seq_2")
SEQ_HEAD = ("seq_0", "seq_1", "seq_2", "head")
LOG2E = 1.4426950408889634
HIGHEST = lax.Precision.HIGHEST
f32 = jnp.float32
bf16 = jnp.bfloat16


def iota(shape, dim):
    return lax.broadcasted_iota(jnp.int32, shape, dim)


def selector(width):
    rows, cols = iota((256, width), 0), iota((256, width), 1)
    return ((rows % 32) == cols // P_SIZE).astype(f32).astype(bf16)


def spread(columns, group, chosen):
    lane = iota(columns.shape, 1)
    columns = jnp.where((lane >= 32 * group) & (lane < 32 * group + 32), columns, 0.0)
    high = columns.astype(bf16)
    low = (columns - high.astype(f32)).astype(bf16)
    return jnp.dot(
        jnp.concatenate([high, low], axis=1), chosen, preferred_element_type=f32
    )


def states_kernel(
    scalars, x_ref, b_ref, rate_ref, dt_ref,
    meta_ref, row_ref, turned_ref, chosen_ref, mine_ref, other_ref,
    state, raw, weighted,
):
    step = pl.program_id(0)
    heads, length = rate_ref.shape
    parts = length // PART
    rows, width = x_ref.shape
    half = width // 2

    @pl.when(step == 0)
    def _():
        state[...] = jnp.zeros_like(state)
        raw[...] = jnp.zeros_like(raw)
        chosen_ref[...] = selector(width)
        for k in range(parts):
            at = slice(k * PART, (k + 1) * PART)
            live = (k * PART + iota((1, PART), 1) < scalars[0]).astype(f32)
            raw[0, 32 * k : 32 * k + heads, :] = rate_ref[:, at] * (live * -LOG2E)
            raw[1, 32 * k : 32 * k + heads, :] = dt_ref[:, at] * live
        upper = (iota((PART, PART), 0) <= iota((PART, PART), 1)).astype(f32)
        running = jnp.dot(raw[0], upper, precision=HIGHEST, preferred_element_type=f32)
        ends = jnp.broadcast_to(running[:, PART - 1 : PART], running.shape)
        leads = [jnp.zeros((32, PART), f32)]
        for k in range(parts):
            leads.append(leads[-1] + ends[32 * k : 32 * k + 32])
        for k in range(parts):
            at = slice(k * PART, (k + 1) * PART)
            run = running[32 * k : 32 * k + 32]
            weight = raw[1, 32 * k : 32 * k + 32, :]
            total = leads[k] + run
            row_ref[:, at] = run - jnp.where(weight > 0, jnp.log(weight) * LOG2E, -1e30)
            tail = jnp.exp2(ends[32 * k : 32 * k + 32] - run) * weight
            last = jnp.exp2(leads[parts] - total) * weight
            meta_ref[at, :] = jnp.concatenate([run, tail, total, last], axis=0).T

    here = pl.ds(pl.multiple_of(step * rows, rows), rows)
    wide = spread(meta_ref[here, :], 3, chosen_ref[...])
    weighted[...] = (x_ref[...].astype(f32) * wide).astype(bf16)
    turned = b_ref[...].astype(f32).T.astype(bf16)
    turned_ref[...] = turned
    state[...] += jnp.dot(turned, weighted[...], preferred_element_type=f32)

    @pl.when(step == pl.num_programs(0) - 1)
    def _():
        wide = spread(meta_ref[length - 16 : length, :], 2, chosen_ref[...])[15:16, :]
        high = wide.astype(bf16).astype(f32)
        line = iota((16, width), 0)
        decay = jnp.where(line == 0, high, jnp.where(line == 1, wide - high, 0.0))
        core = scalars[1]
        for place, ref in ((0, mine_ref), (1, other_ref)):
            low = core == place
            ref[0:128, :] = jnp.where(low, state[:, :half], state[:, half:]).astype(bf16)
            ref[128:144, :] = jnp.where(low, decay[:, :half], decay[:, half:]).astype(bf16)


def states(scalars, x, b, rate, dt):
    length, width = x.shape
    heads = rate.shape[0]
    steps = 4
    rows = length // steps
    one = lambda i, s: (0, 0)
    return pl.pallas_call(
        states_kernel,
        grid_spec=pltpu.PrefetchScalarGridSpec(
            num_scalar_prefetch=1,
            grid=(steps,),
            in_specs=[
                pl.BlockSpec((rows, width), lambda i, s: (i, 0)),
                pl.BlockSpec((rows, 128), lambda i, s: (i, 0)),
                pl.BlockSpec((heads, length), one),
                pl.BlockSpec((heads, length), one),
            ],
            out_specs=[
                pl.BlockSpec((length, 128), one),
                pl.BlockSpec((32, length), one),
                pl.BlockSpec((128, rows), lambda i, s: (0, i)),
                pl.BlockSpec((256, width), one),
                pl.BlockSpec((144, width // 2), one),
                pl.BlockSpec((144, width // 2), one),
            ],
            scratch_shapes=[
                pltpu.VMEM((128, width), f32),
                pltpu.VMEM((2, 32 * (length // PART), PART), f32),
                pltpu.VMEM((rows, width), bf16),
            ],
        ),
        out_shape=[
            jax.ShapeDtypeStruct((length, 128), f32),
            jax.ShapeDtypeStruct((32, length), f32),
            jax.ShapeDtypeStruct((128, length), bf16),
            jax.ShapeDtypeStruct((256, width), bf16),
            jax.ShapeDtypeStruct((144, width // 2), bf16),
            jax.ShapeDtypeStruct((144, width // 2), bf16),
        ],
        compiler_params=pltpu.CompilerParams(dimension_semantics=("arbitrary",)),
        name="states",
    )(scalars, x, b, rate, dt)


def local_kernel(
    share, x_ref, b_ref, c_ref, turned_ref, meta_ref, row_ref, chosen_ref, skip_ref, *rest,
):
    y_ref, state = rest[-2:]
    width = x_ref.shape[1]
    pairs = width // 128
    lower = iota((PART, PART), 0) >= iota((PART, PART), 1)
    left = iota((PART, 128), 1) < 64

    @pl.when(pl.program_id(0) == 0)
    def _():
        state[...] = rest[0][...] if len(rest) == 4 else jnp.zeros_like(state)

    for k in range(x_ref.shape[0] // PART):
        at = slice(k * PART, (k + 1) * PART)
        gram = lax.dot_general(
            c_ref[at, :], b_ref[at, :], (((1,), (1,)), ((), ())), preferred_element_type=f32
        )
        gram = jnp.where(lower, gram, 0.0)
        meta = meta_ref[at, :]
        grown = spread(jnp.exp2(meta), 0, chosen_ref[...])
        tail = spread(meta, 1, chosen_ref[...])
        held = jnp.dot(c_ref[at, :], state[...].astype(bf16), preferred_element_type=f32)
        fresh = []
        for q in range(pairs):
            cols = slice(q * 128, (q + 1) * 128)
            both = []
            for h in (2 * q, 2 * q + 1):
                power = jnp.minimum(meta[:, h : h + 1] - row_ref[h : h + 1, at], 100.0)
                both.append((gram * jnp.exp2(power)).astype(bf16))
            x = x_ref[at, cols]
            wide = x.astype(f32)
            none = jnp.zeros_like(x)
            stack = jnp.concatenate([jnp.where(left, x, none), jnp.where(left, none, x)], axis=0)
            inner = jnp.dot(jnp.concatenate(both, axis=1), stack, preferred_element_type=f32)
            y = inner + grown[:, cols] * held[:, cols] + skip_ref[0:1, cols] * wide
            y_ref[at, cols] = y.astype(bf16)
            fresh.append((wide * tail[:, cols]).astype(bf16))
        fresh = jnp.dot(
            turned_ref[:, at], jnp.concatenate(fresh, axis=1), preferred_element_type=f32
        )
        state[...] = state[...] * grown[PART - 1 : PART, :] + fresh


def local(x, b, c, turned, meta, row, chosen, skip, share, shares, before=()):
    length, width = x.shape
    tile = 256
    steps = length // tile // shares
    by_row = lambda i, s: (share * steps + i, 0)
    by_column = lambda i, s: (0, share * steps + i)
    one = lambda i, s: (0, 0)
    return pl.pallas_call(
        local_kernel,
        grid_spec=pltpu.PrefetchScalarGridSpec(
            num_scalar_prefetch=1,
            grid=(steps,),
            in_specs=[
                pl.BlockSpec((tile, width), by_row),
                pl.BlockSpec((tile, 128), by_row),
                pl.BlockSpec((tile, 128), by_row),
                pl.BlockSpec((128, tile), by_column),
                pl.BlockSpec((tile, 128), by_row),
                pl.BlockSpec((32, tile), by_column),
                pl.BlockSpec((256, width), one),
                pl.BlockSpec((1, width), one),
            ]
            + [pl.BlockSpec((128, width), one), pl.BlockSpec(memory_space=pl.ANY)] * (len(before) // 2),
            out_specs=[
                pl.BlockSpec((tile, width), by_row),
                pl.BlockSpec((128, width), one),
            ],
        ),
        out_shape=[
            jax.ShapeDtypeStruct((length, width), bf16),
            jax.ShapeDtypeStruct((128, width), f32),
        ],
        input_output_aliases={10: 0} if before else {},
        compiler_params=pltpu.CompilerParams(dimension_semantics=("arbitrary",)),
        name="local",
    )(jnp.zeros((1,), jnp.int32), x, b, c, turned, meta, row, chosen, skip, *before)


def gate_kernel(
    scalars, block, y_ref, g_ref, c_ref, meta_ref, chosen_ref, mine_ref, other_ref,
    gain_ref, matrix_ref, top_ref, low_ref, ss_ref, matrix, gated, sem,
):
    rows, width = g_ref.shape
    half = width // 2
    first = block * rows

    @pl.when(first >= scalars[0])
    def _():
        top_ref[...] = jnp.zeros_like(top_ref)
        low_ref[...] = jnp.zeros_like(low_ref)
        ss_ref[...] = jnp.zeros_like(ss_ref)

    @pl.when(first < scalars[0])
    def _():
        copy = pltpu.make_async_copy(matrix_ref, matrix, sem)
        copy.start()
        low = scalars[1] == 0
        held = []
        for place in (0, 1):
            picked = jnp.where(
                low == (place == 0), mine_ref[...].astype(f32), other_ref[...].astype(f32)
            )
            held.append(picked.astype(bf16))

        def piece(k, _):
            at = pl.ds(pl.multiple_of(k * PART, PART), PART)
            grown = spread(jnp.exp2(meta_ref[at, :]), 2, chosen_ref[...])
            live = (first + k * PART + iota((PART, 1), 0) < scalars[0]).astype(f32)
            squares = jnp.zeros((PART, 128), f32)
            for place in (0, 1):
                wide = jnp.dot(c_ref[at, :], held[place], preferred_element_type=f32)
                for j in range(half // 128):
                    cols = slice(place * half + j * 128, place * half + (j + 1) * 128)
                    y = y_ref[at, cols].astype(f32)
                    y = y + grown[:, cols] * wide[:, j * 128 : (j + 1) * 128]
                    g = g_ref[at, cols].astype(f32)
                    v = y * live * (g / (1.0 + jnp.exp2(g * -LOG2E)))
                    squares = squares + v * v
                    gated[at, cols] = (v * gain_ref[0:1, cols]).astype(bf16)
            total = jnp.sum(squares, axis=1, keepdims=True)
            ss_ref[:, at] = jnp.broadcast_to(total, (PART, 128)).T[0:8, :]
            return 0

        lax.fori_loop(0, rows // PART, piece, 0)
        copy.wait()

        def columns(n, _):
            at = pl.ds(pl.multiple_of(n * 256, 256), 256)
            out = jnp.dot(gated[...], matrix[:, at], preferred_element_type=f32)
            top_ref[:, at] = out[: rows // 2].astype(bf16)
            low_ref[:, at] = out[rows // 2 :].astype(bf16)
            return 0

        lax.fori_loop(0, top_ref.shape[1] // 256, columns, 0)


def gate(scalars, y, g, c, meta, chosen, mine, other, gain, matrix):
    width = g.shape[1]
    wide = matrix.shape[1]
    rows = 512

    def at(i, s):
        return (s[2], 0)

    def body(s, *refs):
        gate_kernel(s, s[2], *refs)

    one = lambda i, s: (0, 0)
    return pl.pallas_call(
        body,
        grid_spec=pltpu.PrefetchScalarGridSpec(
            num_scalar_prefetch=1,
            grid=(1,),
            in_specs=[
                pl.BlockSpec((rows, width), at),
                pl.BlockSpec((rows, width), at),
                pl.BlockSpec((rows, 128), at),
                pl.BlockSpec((rows, 128), at),
                pl.BlockSpec((256, width), one),
                pl.BlockSpec((128, width // 2), one),
                pl.BlockSpec((128, width // 2), one),
                pl.BlockSpec((1, width), one),
                pl.BlockSpec(memory_space=pl.ANY),
            ],
            out_specs=[
                pl.BlockSpec((rows // 2, wide), one),
                pl.BlockSpec((rows // 2, wide), one),
                pl.BlockSpec((8, rows), one),
            ],
            scratch_shapes=[
                pltpu.VMEM((width, wide), bf16),
                pltpu.VMEM((rows, width), bf16),
                pltpu.SemaphoreType.DMA,
            ],
        ),
        out_shape=[
            jax.ShapeDtypeStruct((rows // 2, wide), bf16),
            jax.ShapeDtypeStruct((rows // 2, wide), bf16),
            jax.ShapeDtypeStruct((8, rows), f32),
        ],
        compiler_params=pltpu.CompilerParams(dimension_semantics=("arbitrary",)),
        name="gate",
    )(scalars, y, g, c, meta, chosen, mine, other, gain, matrix)


def finish_kernel(own_a, own_b, last_a, last_b, s0, s1, s2, s3, out_ref):
    rows = own_a.shape[0]
    total = s0[...] + s1[...] + s2[...] + s3[...]
    scale = lax.rsqrt(total * (1.0 / (HEADS * P_SIZE)) + 1e-05)
    for k, parts in enumerate(((own_a, last_a), (own_b, last_b))):
        for j in range(rows // PART):
            at = slice(j * PART, (j + 1) * PART)
            lanes = slice(k * rows + j * PART, k * rows + (j + 1) * PART)
            factor = jnp.broadcast_to(scale[0:1, lanes], (PART, PART)).T
            for n in range(out_ref.shape[1] // 128):
                cols = slice(n * 128, (n + 1) * 128)
                value = sum(part[at, cols].astype(f32) for part in parts)
                out_ref[lanes, cols] = (value * factor).astype(bf16)


def finish(pieces, squares):
    rows, wide = pieces[0].shape
    tile = 640
    return pl.pallas_call(
        finish_kernel,
        grid=(wide // tile,),
        in_specs=[pl.BlockSpec((rows, tile), lambda i: (0, i))] * 4
        + [pl.BlockSpec((8, 2 * rows), lambda i: (0, 0))] * 4,
        out_specs=pl.BlockSpec((2 * rows, tile), lambda i: (0, i)),
        out_shape=jax.ShapeDtypeStruct((2 * rows, wide), bf16),
        compiler_params=pltpu.CompilerParams(dimension_semantics=("arbitrary",)),
        name="finish",
    )(*pieces, *squares)


def unpack(ref):
    tail = ref[128:144, :].astype(f32)
    return ref[0:128, :].astype(f32), tail[0:1, :] + tail[1:2, :]


def pack(ref, state, decay):
    ref[0:128, :] = state.astype(bf16)
    high = decay.astype(bf16).astype(f32)
    line = iota((16, decay.shape[1]), 0)
    ref[128:144, :] = jnp.where(
        line == 0, high, jnp.where(line == 1, decay - high, 0.0)
    ).astype(bf16)


def join(earlier, later):
    return jnp.exp2(later[1]) * earlier[0] + later[0], earlier[1] + later[1]


def choose(test, one, two):
    return jax.tree.map(lambda x, y: jnp.where(test, x, y), one, two)


def scan_along(place, refs):
    pieces = [unpack(ref) for ref in refs]
    zero = jax.tree.map(jnp.zeros_like, pieces[0])
    inside = running = zero
    for k in range(4):
        at = lax.rem(place - k + 4, 4)
        piece = choose(
            at < 2, choose(at == 0, pieces[0], pieces[1]), choose(at == 2, pieces[2], pieces[3])
        )
        inside = choose(place == k, running, inside)
        running = join(running, piece)
    return inside, running


def chip_kernel(places, mine, theirs, out):
    first, second = unpack(mine), unpack(theirs)
    low = places[0] == 0
    pack(out, *join(choose(low, first, second), choose(low, second, first)))


def row_kernel(places, g0, g1, g2, g3, out, state, decay):
    inside, row = scan_along(places[1], (g0, g1, g2, g3))
    pack(out, *row)
    state[...] = inside[0]
    decay[...] = jnp.broadcast_to(inside[1], decay.shape)


def entry_kernel(places, g0, g1, g2, g3, state, decay, mine, theirs, own, away):
    before, _ = scan_along(places[2], (g0, g1, g2, g3))
    start = join(before, (state[...], decay[0:1, :]))
    first = choose(places[0] == 0, unpack(mine), unpack(theirs))
    middle = join(start, first)
    low = places[0] == 0
    own[...] = jnp.where(low, start[0], middle[0]).astype(bf16)
    away[...] = jnp.where(low, middle[0], start[0]).astype(bf16)


def small_call(kernel, name, out_shapes, places, *arrays):
    whole = lambda shape: pl.BlockSpec(shape, lambda i, s: (0, 0))
    return pl.pallas_call(
        kernel,
        grid_spec=pltpu.PrefetchScalarGridSpec(
            num_scalar_prefetch=1,
            grid=(1,),
            in_specs=[whole(a.shape) for a in arrays],
            out_specs=[whole(s.shape) for s in out_shapes],
        ),
        out_shape=out_shapes,
        name=name,
    )(places, *arrays)


def shift(value, axis, by, wrap=True):
    count = lax.axis_size(axis)
    pairs = [(i, (i + by) % count) for i in range(count) if wrap or i + by < count]
    return lax.ppermute(value, axis, pairs)


def gather_ring(value, axis):
    return [value] + [shift(value, axis, by) for by in (1, 2, 3)]


def incoming(mine, other, places, first_share, second_share):
    half = mine.shape[1]
    message = jax.ShapeDtypeStruct(mine.shape, bf16)
    state = jax.ShapeDtypeStruct((128, half), f32)
    decay = jax.ShapeDtypeStruct((8, half), f32)
    held = jax.ShapeDtypeStruct((128, half), bf16)
    theirs = shift(other, "seq_2", 1)
    (chip,) = small_call(chip_kernel, "chip", [message], places, mine, theirs)
    pieces = gather_ring(chip, "seq_1")
    shared = first_share()
    row, inside, faded = small_call(row_kernel, "row", [message, state, decay], places, *pieces)
    row, shared = lax.optimization_barrier((row, shared))
    pieces = gather_ring(row, "seq_0")
    y = second_share(*shared)
    pieces, y = lax.optimization_barrier((pieces, y))
    own, away = small_call(
        entry_kernel, "entry", [held, held], places, *pieces, inside, faded, mine, theirs
    )
    return own, shift(away, "seq_2", 1), y


def body(
    values,
    gates,
    b_proj,
    c_proj,
    step_size,
    decay_rate,
    skip_gain,
    norm_gain,
    readout_matrix,
    span_counts,
    remaining_count,
):
    length, width = values.shape
    valid = (span_counts[0] - 1) * SPAN + remaining_count[0]
    core = lax.axis_index("seq_2")
    place = lax.axis_index("head")
    roles = [
        jnp.stack([valid, core, (place + role) % 4]).astype(jnp.int32) for role in range(4)
    ]
    scalars = roles[0]
    skip = jnp.repeat(skip_gain, P_SIZE)[None, :]
    meta, row, turned, chosen, mine, other = states(scalars, values, b_proj, decay_rate, step_size)

    def share(k, before=()):
        return local(
            values, b_proj, c_proj, turned, meta, row, chosen, skip, k, 2, before
        )

    places = jnp.stack([core, lax.axis_index("seq_1"), lax.axis_index("seq_0")]).astype(jnp.int32)
    own, theirs, y = incoming(
        mine, other, places, lambda: share(0), lambda y, state: share(1, (state, y))[0]
    )
    gain = norm_gain[None, :]

    def part(role, block=None):
        return gate(
            roles[role] if block is None else block, y, gates, c_proj, meta, chosen, own, theirs, gain, readout_matrix
        )

    def reduced(blocks):
        def send(value, by, role):
            pairs = [(z, (z + by) % 4) for z in range(4) if (z + role) % 4 < blocks]
            return lax.ppermute(value, "head", pairs)

        def add(one, two):
            return (one.astype(f32) + two.astype(f32)).astype(bf16)

        def all_live():
            far_a, far_b, s2 = part(2)
            far_a, far_b = send(far_a, 1, 2), send(far_b, -1, 2)
            up_a, up_b, s1 = part(1)
            up_b = send(up_b, 1, 1)
            down_a, down_b, s3 = part(3)
            down_a = send(down_a, -1, 3)
            up_a, down_b, last = lax.optimization_barrier(
                (add(up_a, far_a), add(down_b, far_b), roles[0])
            )
            up_a, down_b = send(up_a, 1, 1), send(down_b, -1, 3)
            s2, s1, s3 = send(s2, 2, 2), send(s1, 1, 1), send(s3, -1, 3)
            own_a, own_b, s0 = part(0, last)
            return (add(own_a, down_a), add(own_b, up_b), up_a, down_b), (s0, s1, s2, s3)

        def few_live():
            down_a, down_b, s3 = part(3)
            a = send(down_a, 1, 3)
            up_a, up_b, s1 = part(1)
            b = send(up_b, -1, 1)
            far_a, far_b, s2 = part(2)
            own_a, own_b, s0 = part(0)
            s2, s1, s3 = send(s2, 2, 2), send(s1, 1, 1), send(s3, -1, 3)
            a, b, s1, s2, s3, own_a = lax.optimization_barrier((a, b, s1, s2, s3, own_a))
            a = send(add(far_a, a), 1, 2)
            b = send(add(far_b, b), -1, 2)
            a = send(add(up_a, a), 1, 1)
            b = send(add(down_b, b), -1, 3)
            return (own_a, own_b, a, b), (s0, s1, s2, s3)

        return all_live if blocks == 4 else few_live

    quarter = length // 4
    level = (valid > quarter).astype(jnp.int32) + (valid > 2 * quarter)
    return finish(*lax.switch(level, [reduced(n) for n in (1, 2, 4)]))


def solution(mesh):
    finer = Mesh(
        mesh.devices.reshape(4, 4, 2, mesh.shape["head"]), ("seq_0", "seq_1", "seq_2", "head")
    )
    return jax.shard_map(
        body,
        mesh=finer,
        in_specs=(
            P(SEQ, "head"),
            P(SEQ, "head"),
            P(SEQ, None),
            P(SEQ, None),
            P("head", SEQ),
            P("head", SEQ),
            P("head"),
            P("head"),
            P("head", None),
            P(SEQ),
            P(SEQ),
        ),
        out_specs=P(SEQ_HEAD, None),
        check_vma=False,
    )
```

```python
import jax
import jax.numpy as jnp
from jax import lax
from jax.experimental import pallas as pl
from jax.experimental.pallas import tpu as pltpu
from jax.sharding import Mesh
from jax.sharding import PartitionSpec as P

HEADS = 80
P_SIZE = 64
SPAN = 256
PART = 128
SEQ = ("seq_0", "seq_1", "seq_2")
SEQ_HEAD = ("seq_0", "seq_1", "seq_2", "head")
LOG2E = 1.4426950408889634
HIGHEST = lax.Precision.HIGHEST
f32 = jnp.float32
bf16 = jnp.bfloat16


def iota(shape, dim):
    return lax.broadcasted_iota(jnp.int32, shape, dim)


def selector(width):
    rows, cols = iota((256, width), 0), iota((256, width), 1)
    return ((rows % 32) == cols // P_SIZE).astype(f32).astype(bf16)


def spread(columns, group, chosen):
    lane = iota(columns.shape, 1)
    columns = jnp.where((lane >= 32 * group) & (lane < 32 * group + 32), columns, 0.0)
    high = columns.astype(bf16)
    low = (columns - high.astype(f32)).astype(bf16)
    return jnp.dot(
        jnp.concatenate([high, low], axis=1), chosen, preferred_element_type=f32
    )


def states_kernel(
    scalars, x_ref, b_ref, rate_ref, dt_ref,
    meta_ref, row_ref, turned_ref, chosen_ref, mine_ref, other_ref,
    state, raw, weighted,
):
    step = pl.program_id(0)
    heads, length = rate_ref.shape
    parts = length // PART
    rows, width = x_ref.shape
    half = width // 2

    @pl.when(step == 0)
    def _():
        state[...] = jnp.zeros_like(state)
        raw[...] = jnp.zeros_like(raw)
        chosen_ref[...] = selector(width)
        for k in range(parts):
            at = slice(k * PART, (k + 1) * PART)
            live = (k * PART + iota((1, PART), 1) < scalars[0]).astype(f32)
            raw[0, 32 * k : 32 * k + heads, :] = rate_ref[:, at] * (live * -LOG2E)
            raw[1, 32 * k : 32 * k + heads, :] = dt_ref[:, at] * live
        upper = (iota((PART, PART), 0) <= iota((PART, PART), 1)).astype(f32)
        running = jnp.dot(raw[0], upper, precision=HIGHEST, preferred_element_type=f32)
        ends = jnp.broadcast_to(running[:, PART - 1 : PART], running.shape)
        leads = [jnp.zeros((32, PART), f32)]
        for k in range(parts):
            leads.append(leads[-1] + ends[32 * k : 32 * k + 32])
        for k in range(parts):
            at = slice(k * PART, (k + 1) * PART)
            run = running[32 * k : 32 * k + 32]
            weight = raw[1, 32 * k : 32 * k + 32, :]
            total = leads[k] + run
            row_ref[:, at] = run - jnp.where(weight > 0, jnp.log(weight) * LOG2E, -1e30)
            tail = jnp.exp2(ends[32 * k : 32 * k + 32] - run) * weight
            last = jnp.exp2(leads[parts] - total) * weight
            meta_ref[at, :] = jnp.concatenate([run, tail, total, last], axis=0).T

    here = pl.ds(pl.multiple_of(step * rows, rows), rows)
    wide = spread(meta_ref[here, :], 3, chosen_ref[...])
    weighted[...] = (x_ref[...].astype(f32) * wide).astype(bf16)
    turned = b_ref[...].astype(f32).T.astype(bf16)
    turned_ref[...] = turned
    state[...] += jnp.dot(turned, weighted[...], preferred_element_type=f32)

    @pl.when(step == pl.num_programs(0) - 1)
    def _():
        wide = spread(meta_ref[length - 16 : length, :], 2, chosen_ref[...])[15:16, :]
        high = wide.astype(bf16).astype(f32)
        line = iota((16, width), 0)
        decay = jnp.where(line == 0, high, jnp.where(line == 1, wide - high, 0.0))
        core = scalars[1]
        for place, ref in ((0, mine_ref), (1, other_ref)):
            low = core == place
            ref[0:128, :] = jnp.where(low, state[:, :half], state[:, half:]).astype(bf16)
            ref[128:144, :] = jnp.where(low, decay[:, :half], decay[:, half:]).astype(bf16)


def states(scalars, x, b, rate, dt):
    length, width = x.shape
    heads = rate.shape[0]
    steps = 4
    rows = length // steps
    one = lambda i, s: (0, 0)
    return pl.pallas_call(
        states_kernel,
        grid_spec=pltpu.PrefetchScalarGridSpec(
            num_scalar_prefetch=1,
            grid=(steps,),
            in_specs=[
                pl.BlockSpec((rows, width), lambda i, s: (i, 0)),
                pl.BlockSpec((rows, 128), lambda i, s: (i, 0)),
                pl.BlockSpec((heads, length), one),
                pl.BlockSpec((heads, length), one),
            ],
            out_specs=[
                pl.BlockSpec((length, 128), one),
                pl.BlockSpec((32, length), one),
                pl.BlockSpec((128, rows), lambda i, s: (0, i)),
                pl.BlockSpec((256, width), one),
                pl.BlockSpec((144, width // 2), one),
                pl.BlockSpec((144, width // 2), one),
            ],
            scratch_shapes=[
                pltpu.VMEM((128, width), f32),
                pltpu.VMEM((2, 32 * (length // PART), PART), f32),
                pltpu.VMEM((rows, width), bf16),
            ],
        ),
        out_shape=[
            jax.ShapeDtypeStruct((length, 128), f32),
            jax.ShapeDtypeStruct((32, length), f32),
            jax.ShapeDtypeStruct((128, length), bf16),
            jax.ShapeDtypeStruct((256, width), bf16),
            jax.ShapeDtypeStruct((144, width // 2), bf16),
            jax.ShapeDtypeStruct((144, width // 2), bf16),
        ],
        compiler_params=pltpu.CompilerParams(dimension_semantics=("arbitrary",)),
        name="states",
    )(scalars, x, b, rate, dt)


def local_kernel(
    share, x_ref, b_ref, c_ref, turned_ref, meta_ref, row_ref, chosen_ref, skip_ref, *rest,
):
    y_ref, state = rest[-2:]
    width = x_ref.shape[1]
    pairs = width // 128
    lower = iota((PART, PART), 0) >= iota((PART, PART), 1)
    left = iota((PART, 128), 1) < 64

    @pl.when(pl.program_id(0) == 0)
    def _():
        state[...] = rest[0][...] if len(rest) == 4 else jnp.zeros_like(state)

    for k in range(x_ref.shape[0] // PART):
        at = slice(k * PART, (k + 1) * PART)
        gram = lax.dot_general(
            c_ref[at, :], b_ref[at, :], (((1,), (1,)), ((), ())), preferred_element_type=f32
        )
        gram = jnp.where(lower, gram, 0.0)
        meta = meta_ref[at, :]
        grown = spread(jnp.exp2(meta), 0, chosen_ref[...])
        tail = spread(meta, 1, chosen_ref[...])
        held = jnp.dot(c_ref[at, :], state[...].astype(bf16), preferred_element_type=f32)
        fresh = []
        for q in range(pairs):
            cols = slice(q * 128, (q + 1) * 128)
            both = []
            for h in (2 * q, 2 * q + 1):
                power = jnp.minimum(meta[:, h : h + 1] - row_ref[h : h + 1, at], 100.0)
                both.append((gram * jnp.exp2(power)).astype(bf16))
            x = x_ref[at, cols]
            wide = x.astype(f32)
            none = jnp.zeros_like(x)
            stack = jnp.concatenate([jnp.where(left, x, none), jnp.where(left, none, x)], axis=0)
            inner = jnp.dot(jnp.concatenate(both, axis=1), stack, preferred_element_type=f32)
            y = inner + grown[:, cols] * held[:, cols] + skip_ref[0:1, cols] * wide
            y_ref[at, cols] = y.astype(bf16)
            fresh.append((wide * tail[:, cols]).astype(bf16))
        fresh = jnp.dot(
            turned_ref[:, at], jnp.concatenate(fresh, axis=1), preferred_element_type=f32
        )
        state[...] = state[...] * grown[PART - 1 : PART, :] + fresh


def local(x, b, c, turned, meta, row, chosen, skip, share, shares, before=()):
    length, width = x.shape
    tile = 256
    steps = length // tile // shares
    by_row = lambda i, s: (share * steps + i, 0)
    by_column = lambda i, s: (0, share * steps + i)
    one = lambda i, s: (0, 0)
    return pl.pallas_call(
        local_kernel,
        grid_spec=pltpu.PrefetchScalarGridSpec(
            num_scalar_prefetch=1,
            grid=(steps,),
            in_specs=[
                pl.BlockSpec((tile, width), by_row),
                pl.BlockSpec((tile, 128), by_row),
                pl.BlockSpec((tile, 128), by_row),
                pl.BlockSpec((128, tile), by_column),
                pl.BlockSpec((tile, 128), by_row),
                pl.BlockSpec((32, tile), by_column),
                pl.BlockSpec((256, width), one),
                pl.BlockSpec((1, width), one),
            ]
            + [pl.BlockSpec((128, width), one), pl.BlockSpec(memory_space=pl.ANY)] * (len(before) // 2),
            out_specs=[
                pl.BlockSpec((tile, width), by_row),
                pl.BlockSpec((128, width), one),
            ],
        ),
        out_shape=[
            jax.ShapeDtypeStruct((length, width), bf16),
            jax.ShapeDtypeStruct((128, width), f32),
        ],
        input_output_aliases={10: 0} if before else {},
        compiler_params=pltpu.CompilerParams(dimension_semantics=("arbitrary",)),
        name="local",
    )(jnp.zeros((1,), jnp.int32), x, b, c, turned, meta, row, chosen, skip, *before)


def gate_kernel(
    scalars, block, y_ref, g_ref, c_ref, meta_ref, chosen_ref, mine_ref, other_ref,
    gain_ref, matrix_ref, top_ref, low_ref, ss_ref, matrix, gated, sem,
):
    rows, width = g_ref.shape
    half = width // 2
    first = block * rows

    @pl.when(first >= scalars[0])
    def _():
        top_ref[...] = jnp.zeros_like(top_ref)
        low_ref[...] = jnp.zeros_like(low_ref)
        ss_ref[...] = jnp.zeros_like(ss_ref)

    @pl.when(first < scalars[0])
    def _():
        copy = pltpu.make_async_copy(matrix_ref, matrix, sem)
        copy.start()
        low = scalars[1] == 0
        held = []
        for place in (0, 1):
            picked = jnp.where(
                low == (place == 0), mine_ref[...].astype(f32), other_ref[...].astype(f32)
            )
            held.append(picked.astype(bf16))

        def piece(k, _):
            at = pl.ds(pl.multiple_of(k * PART, PART), PART)
            grown = spread(jnp.exp2(meta_ref[at, :]), 2, chosen_ref[...])
            live = (first + k * PART + iota((PART, 1), 0) < scalars[0]).astype(f32)
            squares = jnp.zeros((PART, 128), f32)
            for place in (0, 1):
                wide = jnp.dot(c_ref[at, :], held[place], preferred_element_type=f32)
                for j in range(half // 128):
                    cols = slice(place * half + j * 128, place * half + (j + 1) * 128)
                    y = y_ref[at, cols].astype(f32)
                    y = y + grown[:, cols] * wide[:, j * 128 : (j + 1) * 128]
                    g = g_ref[at, cols].astype(f32)
                    v = y * live * (g / (1.0 + jnp.exp2(g * -LOG2E)))
                    squares = squares + v * v
                    gated[at, cols] = (v * gain_ref[0:1, cols]).astype(bf16)
            total = jnp.sum(squares, axis=1, keepdims=True)
            ss_ref[:, at] = jnp.broadcast_to(total, (PART, 128)).T[0:8, :]
            return 0

        lax.fori_loop(0, rows // PART, piece, 0)
        copy.wait()

        def columns(n, _):
            at = pl.ds(pl.multiple_of(n * 256, 256), 256)
            out = jnp.dot(gated[...], matrix[:, at], preferred_element_type=f32)
            top_ref[:, at] = out[: rows // 2].astype(bf16)
            low_ref[:, at] = out[rows // 2 :].astype(bf16)
            return 0

        lax.fori_loop(0, top_ref.shape[1] // 256, columns, 0)


def gate(scalars, y, g, c, meta, chosen, mine, other, gain, matrix):
    width = g.shape[1]
    wide = matrix.shape[1]
    rows = 512

    def at(i, s):
        return (s[2], 0)

    def body(s, *refs):
        gate_kernel(s, s[2], *refs)

    one = lambda i, s: (0, 0)
    return pl.pallas_call(
        body,
        grid_spec=pltpu.PrefetchScalarGridSpec(
            num_scalar_prefetch=1,
            grid=(1,),
            in_specs=[
                pl.BlockSpec((rows, width), at),
                pl.BlockSpec((rows, width), at),
                pl.BlockSpec((rows, 128), at),
                pl.BlockSpec((rows, 128), at),
                pl.BlockSpec((256, width), one),
                pl.BlockSpec((128, width // 2), one),
                pl.BlockSpec((128, width // 2), one),
                pl.BlockSpec((1, width), one),
                pl.BlockSpec(memory_space=pl.ANY),
            ],
            out_specs=[
                pl.BlockSpec((rows // 2, wide), one),
                pl.BlockSpec((rows // 2, wide), one),
                pl.BlockSpec((8, rows), one),
            ],
            scratch_shapes=[
                pltpu.VMEM((width, wide), bf16),
                pltpu.VMEM((rows, width), bf16),
                pltpu.SemaphoreType.DMA,
            ],
        ),
        out_shape=[
            jax.ShapeDtypeStruct((rows // 2, wide), bf16),
            jax.ShapeDtypeStruct((rows // 2, wide), bf16),
            jax.ShapeDtypeStruct((8, rows), f32),
        ],
        compiler_params=pltpu.CompilerParams(dimension_semantics=("arbitrary",)),
        name="gate",
    )(scalars, y, g, c, meta, chosen, mine, other, gain, matrix)


def finish_kernel(own_a, own_b, last_a, last_b, s0, s1, s2, s3, out_ref):
    rows = own_a.shape[0]
    total = s0[...] + s1[...] + s2[...] + s3[...]
    scale = lax.rsqrt(total * (1.0 / (HEADS * P_SIZE)) + 1e-05)
    for k, parts in enumerate(((own_a, last_a), (own_b, last_b))):
        for j in range(rows // PART):
            at = slice(j * PART, (j + 1) * PART)
            lanes = slice(k * rows + j * PART, k * rows + (j + 1) * PART)
            factor = jnp.broadcast_to(scale[0:1, lanes], (PART, PART)).T
            for n in range(out_ref.shape[1] // 128):
                cols = slice(n * 128, (n + 1) * 128)
                value = sum(part[at, cols].astype(f32) for part in parts)
                out_ref[lanes, cols] = (value * factor).astype(bf16)


def finish(pieces, squares):
    rows, wide = pieces[0].shape
    tile = 640
    return pl.pallas_call(
        finish_kernel,
        grid=(wide // tile,),
        in_specs=[pl.BlockSpec((rows, tile), lambda i: (0, i))] * 4
        + [pl.BlockSpec((8, 2 * rows), lambda i: (0, 0))] * 4,
        out_specs=pl.BlockSpec((2 * rows, tile), lambda i: (0, i)),
        out_shape=jax.ShapeDtypeStruct((2 * rows, wide), bf16),
        compiler_params=pltpu.CompilerParams(dimension_semantics=("arbitrary",)),
        name="finish",
    )(*pieces, *squares)


def unpack(ref):
    tail = ref[128:144, :].astype(f32)
    return ref[0:128, :].astype(f32), tail[0:1, :] + tail[1:2, :]


def pack(ref, state, decay):
    ref[0:128, :] = state.astype(bf16)
    high = decay.astype(bf16).astype(f32)
    line = iota((16, decay.shape[1]), 0)
    ref[128:144, :] = jnp.where(
        line == 0, high, jnp.where(line == 1, decay - high, 0.0)
    ).astype(bf16)


def join(earlier, later):
    return jnp.exp2(later[1]) * earlier[0] + later[0], earlier[1] + later[1]


def choose(test, one, two):
    return jax.tree.map(lambda x, y: jnp.where(test, x, y), one, two)


def scan_along(place, refs):
    pieces = [unpack(ref) for ref in refs]
    zero = jax.tree.map(jnp.zeros_like, pieces[0])
    inside = running = zero
    for k in range(4):
        at = lax.rem(place - k + 4, 4)
        piece = choose(
            at < 2, choose(at == 0, pieces[0], pieces[1]), choose(at == 2, pieces[2], pieces[3])
        )
        inside = choose(place == k, running, inside)
        running = join(running, piece)
    return inside, running


def chip_kernel(places, mine, theirs, out):
    first, second = unpack(mine), unpack(theirs)
    low = places[0] == 0
    pack(out, *join(choose(low, first, second), choose(low, second, first)))


def row_kernel(places, g0, g1, g2, g3, out, state, decay):
    inside, row = scan_along(places[1], (g0, g1, g2, g3))
    pack(out, *row)
    state[...] = inside[0]
    decay[...] = jnp.broadcast_to(inside[1], decay.shape)


def entry_kernel(places, g0, g1, g2, g3, state, decay, mine, theirs, own, away):
    before, _ = scan_along(places[2], (g0, g1, g2, g3))
    start = join(before, (state[...], decay[0:1, :]))
    first = choose(places[0] == 0, unpack(mine), unpack(theirs))
    middle = join(start, first)
    low = places[0] == 0
    own[...] = jnp.where(low, start[0], middle[0]).astype(bf16)
    away[...] = jnp.where(low, middle[0], start[0]).astype(bf16)


def small_call(kernel, name, out_shapes, places, *arrays):
    whole = lambda shape: pl.BlockSpec(shape, lambda i, s: (0, 0))
    return pl.pallas_call(
        kernel,
        grid_spec=pltpu.PrefetchScalarGridSpec(
            num_scalar_prefetch=1,
            grid=(1,),
            in_specs=[whole(a.shape) for a in arrays],
            out_specs=[whole(s.shape) for s in out_shapes],
        ),
        out_shape=out_shapes,
        name=name,
    )(places, *arrays)


def shift(value, axis, by, wrap=True):
    count = lax.axis_size(axis)
    pairs = [(i, (i + by) % count) for i in range(count) if wrap or i + by < count]
    return lax.ppermute(value, axis, pairs)


def gather_ring(value, axis):
    return [value] + [shift(value, axis, by) for by in (1, 2, 3)]


def incoming(mine, other, places, first_share, second_share):
    half = mine.shape[1]
    message = jax.ShapeDtypeStruct(mine.shape, bf16)
    state = jax.ShapeDtypeStruct((128, half), f32)
    decay = jax.ShapeDtypeStruct((8, half), f32)
    held = jax.ShapeDtypeStruct((128, half), bf16)
    theirs = shift(other, "seq_2", 1)
    (chip,) = small_call(chip_kernel, "chip", [message], places, mine, theirs)
    pieces = gather_ring(chip, "seq_1")
    shared = first_share()
    row, inside, faded = small_call(row_kernel, "row", [message, state, decay], places, *pieces)
    row, shared = lax.optimization_barrier((row, shared))
    pieces = gather_ring(row, "seq_0")
    y = second_share(*shared)
    pieces, y = lax.optimization_barrier((pieces, y))
    own, away = small_call(
        entry_kernel, "entry", [held, held], places, *pieces, inside, faded, mine, theirs
    )
    return own, shift(away, "seq_2", 1), y


def body(
    values,
    gates,
    b_proj,
    c_proj,
    step_size,
    decay_rate,
    skip_gain,
    norm_gain,
    readout_matrix,
    span_counts,
    remaining_count,
):
    length, width = values.shape
    valid = (span_counts[0] - 1) * SPAN + remaining_count[0]
    core = lax.axis_index("seq_2")
    place = lax.axis_index("head")
    roles = [
        jnp.stack([valid, core, (place + role) % 4]).astype(jnp.int32) for role in range(4)
    ]
    scalars = roles[0]
    skip = jnp.repeat(skip_gain, P_SIZE)[None, :]
    meta, row, turned, chosen, mine, other = states(scalars, values, b_proj, decay_rate, step_size)

    def share(k, before=()):
        return local(
            values, b_proj, c_proj, turned, meta, row, chosen, skip, k, 2, before
        )

    places = jnp.stack([core, lax.axis_index("seq_1"), lax.axis_index("seq_0")]).astype(jnp.int32)
    own, theirs, y = incoming(
        mine, other, places, lambda: share(0), lambda y, state: share(1, (state, y))[0]
    )
    gain = norm_gain[None, :]

    def part(role, block=None):
        return gate(
            roles[role] if block is None else block, y, gates, c_proj, meta, chosen, own, theirs, gain, readout_matrix
        )

    def reduced(blocks):
        def send(value, by, role):
            pairs = [(z, (z + by) % 4) for z in range(4) if (z + role) % 4 < blocks]
            return lax.ppermute(value, "head", pairs)

        def add(one, two):
            return (one.astype(f32) + two.astype(f32)).astype(bf16)

        def all_live():
            far_a, far_b, s2 = part(2)
            far_a, far_b = send(far_a, 1, 2), send(far_b, -1, 2)
            up_a, up_b, s1 = part(1)
            up_b = send(up_b, 1, 1)
            down_a, down_b, s3 = part(3)
            down_a = send(down_a, -1, 3)
            up_a, down_b, last = lax.optimization_barrier(
                (add(up_a, far_a), add(down_b, far_b), roles[0])
            )
            up_a, down_b = send(up_a, 1, 1), send(down_b, -1, 3)
            s2, s1, s3 = send(s2, 2, 2), send(s1, 1, 1), send(s3, -1, 3)
            own_a, own_b, s0 = part(0, last)
            return (add(own_a, down_a), add(own_b, up_b), up_a, down_b), (s0, s1, s2, s3)

        def few_live():
            far_a, far_b, s2 = part(2)
            far_a, far_b = send(far_a, 1, 2), send(far_b, -1, 2)
            up_a, up_b, s1 = part(1)
            up_b = send(up_b, 1, 1)
            down_a, down_b, s3 = part(3)
            down_a = send(down_a, -1, 3)
            own_a, own_b, s0 = part(0)
            s2, s1, s3 = send(s2, 2, 2), send(s1, 1, 1), send(s3, -1, 3)
            far_a, far_b, s1, s2, s3, own_a = lax.optimization_barrier(
                (far_a, far_b, s1, s2, s3, own_a)
            )
            up_a = send(add(up_a, far_a), 1, 1)
            down_b = send(add(down_b, far_b), -1, 3)
            return (add(own_a, down_a), add(own_b, up_b), up_a, down_b), (s0, s1, s2, s3)

        return all_live if blocks == 4 else few_live

    quarter = length // 4
    level = (valid > quarter).astype(jnp.int32) + (valid > 2 * quarter)
    return finish(*lax.switch(level, [reduced(n) for n in (1, 2, 4)]))


def solution(mesh):
    finer = Mesh(
        mesh.devices.reshape(4, 4, 2, mesh.shape["head"]), ("seq_0", "seq_1", "seq_2", "head")
    )
    return jax.shard_map(
        body,
        mesh=finer,
        in_specs=(
            P(SEQ, "head"),
            P(SEQ, "head"),
            P(SEQ, None),
            P(SEQ, None),
            P("head", SEQ),
            P("head", SEQ),
            P("head"),
            P("head"),
            P("head", None),
            P(SEQ),
            P(SEQ),
        ),
        out_specs=P(SEQ_HEAD, None),
        check_vma=False,
    )
```

```python
import jax
import jax.numpy as jnp
from jax import lax
from jax.experimental import pallas as pl
from jax.experimental.pallas import tpu as pltpu
from jax.sharding import Mesh
from jax.sharding import PartitionSpec as P

HEADS = 80
P_SIZE = 64
SPAN = 256
PART = 128
SEQ = ("seq_0", "seq_1", "seq_2")
SEQ_HEAD = ("seq_0", "seq_1", "seq_2", "head")
LOG2E = 1.4426950408889634
HIGHEST = lax.Precision.HIGHEST
f32 = jnp.float32
bf16 = jnp.bfloat16


def iota(shape, dim):
    return lax.broadcasted_iota(jnp.int32, shape, dim)


def selector(width):
    rows, cols = iota((256, width), 0), iota((256, width), 1)
    return ((rows % 32) == cols // P_SIZE).astype(f32).astype(bf16)


def spread(columns, group, chosen):
    lane = iota(columns.shape, 1)
    columns = jnp.where((lane >= 32 * group) & (lane < 32 * group + 32), columns, 0.0)
    high = columns.astype(bf16)
    low = (columns - high.astype(f32)).astype(bf16)
    return jnp.dot(
        jnp.concatenate([high, low], axis=1), chosen, preferred_element_type=f32
    )


def states_kernel(
    scalars, x_ref, b_ref, rate_ref, dt_ref, skip_ref,
    meta_ref, row_ref, turned_ref, chosen_ref, wide_skip_ref, mine_ref, other_ref,
    state, raw, weighted, small,
):
    step = pl.program_id(0)
    heads, length = rate_ref.shape
    parts = length // PART
    rows, width = x_ref.shape
    half = width // 2

    @pl.when(step == 0)
    def _():
        state[...] = jnp.zeros_like(state)
        raw[...] = jnp.zeros_like(raw)
        chosen_ref[...] = selector(width)
        small[...] = jnp.zeros_like(small)
        small[0:1, 0:heads] = skip_ref[...]
        wide_skip_ref[...] = spread(small[...], 0, chosen_ref[...])
        for k in range(parts):
            at = slice(k * PART, (k + 1) * PART)
            live = (k * PART + iota((1, PART), 1) < scalars[0]).astype(f32)
            raw[0, 32 * k : 32 * k + heads, :] = rate_ref[:, at] * (live * -LOG2E)
            raw[1, 32 * k : 32 * k + heads, :] = dt_ref[:, at] * live
        upper = (iota((PART, PART), 0) <= iota((PART, PART), 1)).astype(f32)
        running = jnp.dot(raw[0], upper, precision=HIGHEST, preferred_element_type=f32)
        ends = jnp.broadcast_to(running[:, PART - 1 : PART], running.shape)
        leads = [jnp.zeros((32, PART), f32)]
        for k in range(parts):
            leads.append(leads[-1] + ends[32 * k : 32 * k + 32])
        for k in range(parts):
            at = slice(k * PART, (k + 1) * PART)
            run = running[32 * k : 32 * k + 32]
            weight = raw[1, 32 * k : 32 * k + 32, :]
            total = leads[k] + run
            row_ref[:, at] = run - jnp.where(weight > 0, jnp.log(weight) * LOG2E, -1e30)
            tail = jnp.exp2(ends[32 * k : 32 * k + 32] - run) * weight
            last = jnp.exp2(leads[parts] - total) * weight
            meta_ref[at, :] = jnp.concatenate([run, tail, total, last], axis=0).T

    here = pl.ds(pl.multiple_of(step * rows, rows), rows)
    wide = spread(meta_ref[here, :], 3, chosen_ref[...])
    weighted[...] = (x_ref[...].astype(f32) * wide).astype(bf16)
    turned = b_ref[...].astype(f32).T.astype(bf16)
    turned_ref[...] = turned
    state[...] += jnp.dot(turned, weighted[...], preferred_element_type=f32)

    @pl.when(step == pl.num_programs(0) - 1)
    def _():
        wide = spread(meta_ref[length - 16 : length, :], 2, chosen_ref[...])[15:16, :]
        high = wide.astype(bf16).astype(f32)
        line = iota((16, width), 0)
        decay = jnp.where(line == 0, high, jnp.where(line == 1, wide - high, 0.0))
        core = scalars[1]
        for place, ref in ((0, mine_ref), (1, other_ref)):
            low = core == place
            ref[0:128, :] = jnp.where(low, state[:, :half], state[:, half:]).astype(bf16)
            ref[128:144, :] = jnp.where(low, decay[:, :half], decay[:, half:]).astype(bf16)


def states(scalars, x, b, rate, dt, skip):
    length, width = x.shape
    heads = rate.shape[0]
    steps = 4
    rows = length // steps
    one = lambda i, s: (0, 0)
    return pl.pallas_call(
        states_kernel,
        grid_spec=pltpu.PrefetchScalarGridSpec(
            num_scalar_prefetch=1,
            grid=(steps,),
            in_specs=[
                pl.BlockSpec((rows, width), lambda i, s: (i, 0)),
                pl.BlockSpec((rows, 128), lambda i, s: (i, 0)),
                pl.BlockSpec((heads, length), one),
                pl.BlockSpec((heads, length), one),
                pl.BlockSpec((1, heads), one),
            ],
            out_specs=[
                pl.BlockSpec((length, 128), one),
                pl.BlockSpec((32, length), one),
                pl.BlockSpec((128, rows), lambda i, s: (0, i)),
                pl.BlockSpec((256, width), one),
                pl.BlockSpec((16, width), one),
                pl.BlockSpec((144, width // 2), one),
                pl.BlockSpec((144, width // 2), one),
            ],
            scratch_shapes=[
                pltpu.VMEM((128, width), f32),
                pltpu.VMEM((2, 32 * (length // PART), PART), f32),
                pltpu.VMEM((rows, width), bf16),
                pltpu.VMEM((16, 128), f32),
            ],
        ),
        out_shape=[
            jax.ShapeDtypeStruct((length, 128), f32),
            jax.ShapeDtypeStruct((32, length), f32),
            jax.ShapeDtypeStruct((128, length), bf16),
            jax.ShapeDtypeStruct((256, width), bf16),
            jax.ShapeDtypeStruct((16, width), f32),
            jax.ShapeDtypeStruct((144, width // 2), bf16),
            jax.ShapeDtypeStruct((144, width // 2), bf16),
        ],
        compiler_params=pltpu.CompilerParams(dimension_semantics=("arbitrary",)),
        name="states",
    )(scalars, x, b, rate, dt, skip)


def local_kernel(
    share, x_ref, b_ref, c_ref, turned_ref, meta_ref, row_ref, chosen_ref, skip_ref, *rest,
):
    y_ref, state = rest[-2:]
    width = x_ref.shape[1]
    pairs = width // 128
    lower = iota((PART, PART), 0) >= iota((PART, PART), 1)
    left = iota((PART, 128), 1) < 64

    @pl.when(pl.program_id(0) == 0)
    def _():
        state[...] = rest[0][...] if len(rest) == 4 else jnp.zeros_like(state)

    for k in range(x_ref.shape[0] // PART):
        at = slice(k * PART, (k + 1) * PART)
        gram = lax.dot_general(
            c_ref[at, :], b_ref[at, :], (((1,), (1,)), ((), ())), preferred_element_type=f32
        )
        gram = jnp.where(lower, gram, 0.0)
        meta = meta_ref[at, :]
        grown = spread(jnp.exp2(meta), 0, chosen_ref[...])
        tail = spread(meta, 1, chosen_ref[...])
        held = jnp.dot(c_ref[at, :], state[...].astype(bf16), preferred_element_type=f32)
        fresh = []
        for q in range(pairs):
            cols = slice(q * 128, (q + 1) * 128)
            both = []
            for h in (2 * q, 2 * q + 1):
                power = jnp.minimum(meta[:, h : h + 1] - row_ref[h : h + 1, at], 100.0)
                both.append((gram * jnp.exp2(power)).astype(bf16))
            x = x_ref[at, cols]
            wide = x.astype(f32)
            none = jnp.zeros_like(x)
            stack = jnp.concatenate([jnp.where(left, x, none), jnp.where(left, none, x)], axis=0)
            inner = jnp.dot(jnp.concatenate(both, axis=1), stack, preferred_element_type=f32)
            y = inner + grown[:, cols] * held[:, cols] + skip_ref[0:1, cols] * wide
            y_ref[at, cols] = y.astype(bf16)
            fresh.append((wide * tail[:, cols]).astype(bf16))
        fresh = jnp.dot(
            turned_ref[:, at], jnp.concatenate(fresh, axis=1), preferred_element_type=f32
        )
        state[...] = state[...] * grown[PART - 1 : PART, :] + fresh


def local(x, b, c, turned, meta, row, chosen, skip, share, shares, before=()):
    length, width = x.shape
    tile = 256
    steps = length // tile // shares
    by_row = lambda i, s: (share * steps + i, 0)
    by_column = lambda i, s: (0, share * steps + i)
    one = lambda i, s: (0, 0)
    return pl.pallas_call(
        local_kernel,
        grid_spec=pltpu.PrefetchScalarGridSpec(
            num_scalar_prefetch=1,
            grid=(steps,),
            in_specs=[
                pl.BlockSpec((tile, width), by_row),
                pl.BlockSpec((tile, 128), by_row),
                pl.BlockSpec((tile, 128), by_row),
                pl.BlockSpec((128, tile), by_column),
                pl.BlockSpec((tile, 128), by_row),
                pl.BlockSpec((32, tile), by_column),
                pl.BlockSpec((256, width), one),
                pl.BlockSpec((16, width), one),
            ]
            + [pl.BlockSpec((128, width), one), pl.BlockSpec(memory_space=pl.ANY)] * (len(before) // 2),
            out_specs=[
                pl.BlockSpec((tile, width), by_row),
                pl.BlockSpec((128, width), one),
            ],
        ),
        out_shape=[
            jax.ShapeDtypeStruct((length, width), bf16),
            jax.ShapeDtypeStruct((128, width), f32),
        ],
        input_output_aliases={10: 0} if before else {},
        compiler_params=pltpu.CompilerParams(
            dimension_semantics=("arbitrary",), vmem_limit_bytes=24 << 20
        ),
        name="local",
    )(jnp.zeros((1,), jnp.int32), x, b, c, turned, meta, row, chosen, skip, *before)


def gate_kernel(
    scalars, block, y_ref, g_ref, c_ref, meta_ref, chosen_ref, mine_ref, other_ref,
    gain_ref, matrix_ref, top_ref, low_ref, ss_ref, matrix, gated, sem,
):
    rows, width = g_ref.shape
    half = width // 2
    first = block * rows

    @pl.when(first >= scalars[0])
    def _():
        top_ref[...] = jnp.zeros_like(top_ref)
        low_ref[...] = jnp.zeros_like(low_ref)
        ss_ref[...] = jnp.zeros_like(ss_ref)

    @pl.when(first < scalars[0])
    def _():
        copy = pltpu.make_async_copy(matrix_ref, matrix, sem)
        copy.start()
        low = scalars[1] == 0
        held = []
        for place in (0, 1):
            picked = jnp.where(
                low == (place == 0), mine_ref[...].astype(f32), other_ref[...].astype(f32)
            )
            held.append(picked.astype(bf16))

        def piece(k, _):
            at = pl.ds(pl.multiple_of(k * PART, PART), PART)
            grown = spread(jnp.exp2(meta_ref[at, :]), 2, chosen_ref[...])
            live = (first + k * PART + iota((PART, 1), 0) < scalars[0]).astype(f32)
            squares = jnp.zeros((PART, 128), f32)
            for place in (0, 1):
                wide = jnp.dot(c_ref[at, :], held[place], preferred_element_type=f32)
                for j in range(half // 128):
                    cols = slice(place * half + j * 128, place * half + (j + 1) * 128)
                    y = y_ref[at, cols].astype(f32)
                    y = y + grown[:, cols] * wide[:, j * 128 : (j + 1) * 128]
                    g = g_ref[at, cols].astype(f32)
                    v = y * live * (g / (1.0 + jnp.exp2(g * -LOG2E)))
                    squares = squares + v * v
                    gated[at, cols] = (v * gain_ref[0:1, cols]).astype(bf16)
            total = jnp.sum(squares, axis=1, keepdims=True)
            ss_ref[:, at] = jnp.broadcast_to(total, (PART, 128)).T[0:8, :]
            return 0

        lax.fori_loop(0, rows // PART, piece, 0)
        copy.wait()

        def columns(n, _):
            at = pl.ds(pl.multiple_of(n * 256, 256), 256)
            out = jnp.dot(gated[...], matrix[:, at], preferred_element_type=f32)
            top_ref[:, at] = out[: rows // 2].astype(bf16)
            low_ref[:, at] = out[rows // 2 :].astype(bf16)
            return 0

        lax.fori_loop(0, top_ref.shape[1] // 256, columns, 0)


def gate(scalars, y, g, c, meta, chosen, mine, other, gain, matrix):
    width = g.shape[1]
    wide = matrix.shape[1]
    rows = 512

    def at(i, s):
        return (s[2], 0)

    def body(s, *refs):
        gate_kernel(s, s[2], *refs)

    one = lambda i, s: (0, 0)
    return pl.pallas_call(
        body,
        grid_spec=pltpu.PrefetchScalarGridSpec(
            num_scalar_prefetch=1,
            grid=(1,),
            in_specs=[
                pl.BlockSpec((rows, width), at),
                pl.BlockSpec((rows, width), at),
                pl.BlockSpec((rows, 128), at),
                pl.BlockSpec((rows, 128), at),
                pl.BlockSpec((256, width), one),
                pl.BlockSpec((128, width // 2), one),
                pl.BlockSpec((128, width // 2), one),
                pl.BlockSpec((1, width), one),
                pl.BlockSpec(memory_space=pl.ANY),
            ],
            out_specs=[
                pl.BlockSpec((rows // 2, wide), one),
                pl.BlockSpec((rows // 2, wide), one),
                pl.BlockSpec((8, rows), one),
            ],
            scratch_shapes=[
                pltpu.VMEM((width, wide), bf16),
                pltpu.VMEM((rows, width), bf16),
                pltpu.SemaphoreType.DMA,
            ],
        ),
        out_shape=[
            jax.ShapeDtypeStruct((rows // 2, wide), bf16),
            jax.ShapeDtypeStruct((rows // 2, wide), bf16),
            jax.ShapeDtypeStruct((8, rows), f32),
        ],
        compiler_params=pltpu.CompilerParams(
            dimension_semantics=("arbitrary",), vmem_limit_bytes=32 << 20
        ),
        name="gate",
    )(scalars, y, g, c, meta, chosen, mine, other, gain, matrix)


def finish_kernel(own_a, own_b, last_a, last_b, s0, s1, s2, s3, out_ref):
    rows = own_a.shape[0]
    total = s0[...] + s1[...] + s2[...] + s3[...]
    scale = lax.rsqrt(total * (1.0 / (HEADS * P_SIZE)) + 1e-05)
    for k, parts in enumerate(((own_a, last_a), (own_b, last_b))):
        for j in range(rows // PART):
            at = slice(j * PART, (j + 1) * PART)
            lanes = slice(k * rows + j * PART, k * rows + (j + 1) * PART)
            factor = jnp.broadcast_to(scale[0:1, lanes], (PART, PART)).T
            for n in range(out_ref.shape[1] // 128):
                cols = slice(n * 128, (n + 1) * 128)
                value = sum(part[at, cols].astype(f32) for part in parts)
                out_ref[lanes, cols] = (value * factor).astype(bf16)


def finish(pieces, squares):
    rows, wide = pieces[0].shape
    tile = 640
    return pl.pallas_call(
        finish_kernel,
        grid=(wide // tile,),
        in_specs=[pl.BlockSpec((rows, tile), lambda i: (0, i))] * 4
        + [pl.BlockSpec((8, 2 * rows), lambda i: (0, 0))] * 4,
        out_specs=pl.BlockSpec((2 * rows, tile), lambda i: (0, i)),
        out_shape=jax.ShapeDtypeStruct((2 * rows, wide), bf16),
        compiler_params=pltpu.CompilerParams(
            dimension_semantics=("arbitrary",), vmem_limit_bytes=16 << 20
        ),
        name="finish",
    )(*pieces, *squares)


def unpack(ref):
    tail = ref[128:144, :].astype(f32)
    return ref[0:128, :].astype(f32), tail[0:1, :] + tail[1:2, :]


def pack(ref, state, decay):
    ref[0:128, :] = state.astype(bf16)
    high = decay.astype(bf16).astype(f32)
    line = iota((16, decay.shape[1]), 0)
    ref[128:144, :] = jnp.where(
        line == 0, high, jnp.where(line == 1, decay - high, 0.0)
    ).astype(bf16)


def join(earlier, later):
    return jnp.exp2(later[1]) * earlier[0] + later[0], earlier[1] + later[1]


def choose(test, one, two):
    return jax.tree.map(lambda x, y: jnp.where(test, x, y), one, two)


def scan_along(place, refs):
    pieces = [unpack(ref) for ref in refs]
    zero = jax.tree.map(jnp.zeros_like, pieces[0])
    inside = running = zero
    for k in range(4):
        at = lax.rem(place - k + 4, 4)
        piece = choose(
            at < 2, choose(at == 0, pieces[0], pieces[1]), choose(at == 2, pieces[2], pieces[3])
        )
        inside = choose(place == k, running, inside)
        running = join(running, piece)
    return inside, running


def chip_kernel(places, mine, theirs, out):
    first, second = unpack(mine), unpack(theirs)
    low = places[0] == 0
    pack(out, *join(choose(low, first, second), choose(low, second, first)))


def row_kernel(places, g0, g1, g2, g3, out, state, decay):
    inside, row = scan_along(places[1], (g0, g1, g2, g3))
    pack(out, *row)
    state[...] = inside[0]
    decay[...] = jnp.broadcast_to(inside[1], decay.shape)


def entry_kernel(places, g0, g1, g2, g3, state, decay, mine, theirs, own, away):
    before, _ = scan_along(places[2], (g0, g1, g2, g3))
    start = join(before, (state[...], decay[0:1, :]))
    first = choose(places[0] == 0, unpack(mine), unpack(theirs))
    middle = join(start, first)
    low = places[0] == 0
    own[...] = jnp.where(low, start[0], middle[0]).astype(bf16)
    away[...] = jnp.where(low, middle[0], start[0]).astype(bf16)


def small_call(kernel, name, out_shapes, places, *arrays):
    near = pl.BlockSpec(memory_space=pltpu.VMEM)
    return pl.pallas_call(
        kernel,
        in_specs=[pl.BlockSpec(memory_space=pltpu.SMEM)] + [near] * len(arrays),
        out_specs=[near] * len(out_shapes),
        out_shape=out_shapes,
        compiler_params=pltpu.CompilerParams(vmem_limit_bytes=8 << 20),
        name=name,
    )(places, *arrays)


def shift(value, axis, by, wrap=True):
    count = lax.axis_size(axis)
    pairs = [(i, (i + by) % count) for i in range(count) if wrap or i + by < count]
    return lax.ppermute(value, axis, pairs)


def gather_ring(value, axis):
    return [value] + [shift(value, axis, by) for by in (1, 2, 3)]


def incoming(mine, other, places, first_share, second_share):
    half = mine.shape[1]
    message = jax.ShapeDtypeStruct(mine.shape, bf16)
    state = jax.ShapeDtypeStruct((128, half), f32)
    decay = jax.ShapeDtypeStruct((8, half), f32)
    held = jax.ShapeDtypeStruct((128, half), bf16)
    theirs = shift(other, "seq_2", 1)
    (chip,) = small_call(chip_kernel, "chip", [message], places, mine, theirs)
    pieces = gather_ring(chip, "seq_1")
    shared = first_share()
    row, inside, faded = small_call(row_kernel, "row", [message, state, decay], places, *pieces)
    row, shared = lax.optimization_barrier((row, shared))
    pieces = gather_ring(row, "seq_0")
    y = second_share(*shared)
    pieces, y = lax.optimization_barrier((pieces, y))
    own, away = small_call(
        entry_kernel, "entry", [held, held], places, *pieces, inside, faded, mine, theirs
    )
    return own, shift(away, "seq_2", 1), y


def body(
    values,
    gates,
    b_proj,
    c_proj,
    step_size,
    decay_rate,
    skip_gain,
    norm_gain,
    readout_matrix,
    span_counts,
    remaining_count,
):
    length, width = values.shape
    valid = (span_counts[0] - 1) * SPAN + remaining_count[0]
    core = lax.axis_index("seq_2")
    place = lax.axis_index("head")
    roles = [
        jnp.stack([valid, core, (place + role) % 4]).astype(jnp.int32) for role in range(4)
    ]
    scalars = roles[0]
    meta, row, turned, chosen, skip, mine, other = states(
        scalars, values, b_proj, decay_rate, step_size, skip_gain[None, :]
    )

    def share(k, before=()):
        return local(
            values, b_proj, c_proj, turned, meta, row, chosen, skip, k, 2, before
        )

    places = jnp.stack([core, lax.axis_index("seq_1"), lax.axis_index("seq_0")]).astype(jnp.int32)
    own, theirs, y = incoming(
        mine, other, places, lambda: share(0), lambda y, state: share(1, (state, y))[0]
    )
    gain = norm_gain[None, :]

    def part(role, block=None):
        return gate(
            roles[role] if block is None else block, y, gates, c_proj, meta, chosen, own, theirs, gain, readout_matrix
        )

    def reduced(blocks):
        def send(value, by, role):
            pairs = [(z, (z + by) % 4) for z in range(4) if (z + role) % 4 < blocks]
            return lax.ppermute(value, "head", pairs)

        def add(one, two):
            return (one.astype(f32) + two.astype(f32)).astype(bf16)

        def all_live():
            far_a, far_b, s2 = part(2)
            far_a, far_b = send(far_a, 1, 2), send(far_b, -1, 2)
            up_a, up_b, s1 = part(1)
            up_b = send(up_b, 1, 1)
            down_a, down_b, s3 = part(3)
            down_a = send(down_a, -1, 3)
            up_a, down_b, last = lax.optimization_barrier(
                (add(up_a, far_a), add(down_b, far_b), roles[0])
            )
            up_a, down_b = send(up_a, 1, 1), send(down_b, -1, 3)
            s2, s1, s3 = send(s2, 2, 2), send(s1, 1, 1), send(s3, -1, 3)
            own_a, own_b, s0 = part(0, last)
            return (add(own_a, down_a), add(own_b, up_b), up_a, down_b), (s0, s1, s2, s3)

        def few_live():
            far_a, far_b, s2 = part(2)
            far_a, far_b = send(far_a, 1, 2), send(far_b, -1, 2)
            up_a, up_b, s1 = part(1)
            up_b = send(up_b, 1, 1)
            down_a, down_b, s3 = part(3)
            down_a = send(down_a, -1, 3)
            own_a, own_b, s0 = part(0)
            s2, s1, s3 = send(s2, 2, 2), send(s1, 1, 1), send(s3, -1, 3)
            far_a, far_b, s1, s2, s3, own_a = lax.optimization_barrier(
                (far_a, far_b, s1, s2, s3, own_a)
            )
            up_a = send(add(up_a, far_a), 1, 1)
            down_b = send(add(down_b, far_b), -1, 3)
            return (add(own_a, down_a), add(own_b, up_b), up_a, down_b), (s0, s1, s2, s3)

        return all_live if blocks == 4 else few_live

    quarter = length // 4
    level = (valid > quarter).astype(jnp.int32) + (valid > 2 * quarter)
    return finish(*lax.switch(level, [reduced(n) for n in (1, 2, 4)]))


def solution(mesh):
    finer = Mesh(
        mesh.devices.reshape(4, 4, 2, mesh.shape["head"]), ("seq_0", "seq_1", "seq_2", "head")
    )
    return jax.shard_map(
        body,
        mesh=finer,
        in_specs=(
            P(SEQ, "head"),
            P(SEQ, "head"),
            P(SEQ, None),
            P(SEQ, None),
            P("head", SEQ),
            P("head", SEQ),
            P("head"),
            P("head"),
            P("head", None),
            P(SEQ),
            P(SEQ),
        ),
        out_specs=P(SEQ_HEAD, None),
        check_vma=False,
    )
```

```python
import jax
import jax.numpy as jnp
from jax import lax
from jax.experimental import pallas as pl
from jax.experimental.pallas import tpu as pltpu
from jax.sharding import Mesh
from jax.sharding import PartitionSpec as P

HEADS = 80
P_SIZE = 64
SPAN = 256
PART = 128
SEQ = ("seq_0", "seq_1", "seq_2")
SEQ_HEAD = ("seq_0", "seq_1", "seq_2", "head")
LOG2E = 1.4426950408889634
HIGHEST = lax.Precision.HIGHEST
f32 = jnp.float32
bf16 = jnp.bfloat16


def iota(shape, dim):
    return lax.broadcasted_iota(jnp.int32, shape, dim)


def selector(width):
    rows, cols = iota((256, width), 0), iota((256, width), 1)
    return ((rows % 32) == cols // P_SIZE).astype(f32).astype(bf16)


def spread(columns, group, chosen):
    lane = iota(columns.shape, 1)
    columns = jnp.where((lane >= 32 * group) & (lane < 32 * group + 32), columns, 0.0)
    high = columns.astype(bf16)
    low = (columns - high.astype(f32)).astype(bf16)
    return jnp.dot(
        jnp.concatenate([high, low], axis=1), chosen, preferred_element_type=f32
    )


def states_kernel(
    scalars, x_ref, b_ref, rate_ref, dt_ref, skip_ref,
    meta_ref, row_ref, turned_ref, chosen_ref, wide_skip_ref, mine_ref, other_ref,
    state, raw, weighted, small,
):
    step = pl.program_id(0)
    heads, length = rate_ref.shape
    parts = length // PART
    rows, width = x_ref.shape
    half = width // 2

    @pl.when(step == 0)
    def _():
        state[...] = jnp.zeros_like(state)
        raw[...] = jnp.zeros_like(raw)
        chosen_ref[...] = selector(width)
        small[...] = jnp.zeros_like(small)
        small[0:1, 0:heads] = skip_ref[...]
        wide_skip_ref[...] = spread(small[...], 0, chosen_ref[...])
        for k in range(parts):
            at = slice(k * PART, (k + 1) * PART)
            live = (k * PART + iota((1, PART), 1) < scalars[0]).astype(f32)
            raw[0, 32 * k : 32 * k + heads, :] = rate_ref[:, at] * (live * -LOG2E)
            raw[1, 32 * k : 32 * k + heads, :] = dt_ref[:, at] * live
        upper = (iota((PART, PART), 0) <= iota((PART, PART), 1)).astype(f32)
        running = jnp.dot(raw[0], upper, precision=HIGHEST, preferred_element_type=f32)
        ends = jnp.broadcast_to(running[:, PART - 1 : PART], running.shape)
        leads = [jnp.zeros((32, PART), f32)]
        for k in range(parts):
            leads.append(leads[-1] + ends[32 * k : 32 * k + 32])
        for k in range(parts):
            at = slice(k * PART, (k + 1) * PART)
            run = running[32 * k : 32 * k + 32]
            weight = raw[1, 32 * k : 32 * k + 32, :]
            total = leads[k] + run
            row_ref[:, at] = run - jnp.where(weight > 0, jnp.log(weight) * LOG2E, -1e30)
            tail = jnp.exp2(ends[32 * k : 32 * k + 32] - run) * weight
            last = jnp.exp2(leads[parts] - total) * weight
            meta_ref[at, :] = jnp.concatenate([run, tail, total, last], axis=0).T

    here = pl.ds(pl.multiple_of(step * rows, rows), rows)
    wide = spread(meta_ref[here, :], 3, chosen_ref[...])
    weighted[...] = (x_ref[...].astype(f32) * wide).astype(bf16)
    turned = b_ref[...].astype(f32).T.astype(bf16)
    turned_ref[...] = turned
    state[...] += jnp.dot(turned, weighted[...], preferred_element_type=f32)

    @pl.when(step == pl.num_programs(0) - 1)
    def _():
        wide = spread(meta_ref[length - 16 : length, :], 2, chosen_ref[...])[15:16, :]
        high = wide.astype(bf16).astype(f32)
        line = iota((16, width), 0)
        decay = jnp.where(line == 0, high, jnp.where(line == 1, wide - high, 0.0))
        core = scalars[1]
        for place, ref in ((0, mine_ref), (1, other_ref)):
            low = core == place
            ref[0:128, :] = jnp.where(low, state[:, :half], state[:, half:]).astype(bf16)
            ref[128:144, :] = jnp.where(low, decay[:, :half], decay[:, half:]).astype(bf16)


def states(scalars, x, b, rate, dt, skip):
    length, width = x.shape
    heads = rate.shape[0]
    steps = 4
    rows = length // steps
    one = lambda i, s: (0, 0)
    return pl.pallas_call(
        states_kernel,
        grid_spec=pltpu.PrefetchScalarGridSpec(
            num_scalar_prefetch=1,
            grid=(steps,),
            in_specs=[
                pl.BlockSpec((rows, width), lambda i, s: (i, 0)),
                pl.BlockSpec((rows, 128), lambda i, s: (i, 0)),
                pl.BlockSpec((heads, length), one),
                pl.BlockSpec((heads, length), one),
                pl.BlockSpec((1, heads), one),
            ],
            out_specs=[
                pl.BlockSpec((length, 128), one),
                pl.BlockSpec((32, length), one),
                pl.BlockSpec((128, rows), lambda i, s: (0, i)),
                pl.BlockSpec((256, width), one),
                pl.BlockSpec((16, width), one),
                pl.BlockSpec((144, width // 2), one),
                pl.BlockSpec((144, width // 2), one),
            ],
            scratch_shapes=[
                pltpu.VMEM((128, width), f32),
                pltpu.VMEM((2, 32 * (length // PART), PART), f32),
                pltpu.VMEM((rows, width), bf16),
                pltpu.VMEM((16, 128), f32),
            ],
        ),
        out_shape=[
            jax.ShapeDtypeStruct((length, 128), f32),
            jax.ShapeDtypeStruct((32, length), f32),
            jax.ShapeDtypeStruct((128, length), bf16),
            jax.ShapeDtypeStruct((256, width), bf16),
            jax.ShapeDtypeStruct((16, width), f32),
            jax.ShapeDtypeStruct((144, width // 2), bf16),
            jax.ShapeDtypeStruct((144, width // 2), bf16),
        ],
        compiler_params=pltpu.CompilerParams(
            dimension_semantics=("arbitrary",), vmem_limit_bytes=24 << 20
        ),
        name="states",
    )(scalars, x, b, rate, dt, skip)


def local_kernel(
    share, x_ref, b_ref, c_ref, turned_ref, meta_ref, row_ref, chosen_ref, skip_ref, *rest,
):
    y_ref, state = rest[-2:]
    width = x_ref.shape[1]
    pairs = width // 128
    lower = iota((PART, PART), 0) >= iota((PART, PART), 1)
    left = iota((PART, 128), 1) < 64

    @pl.when(pl.program_id(0) == 0)
    def _():
        state[...] = rest[0][...] if len(rest) == 4 else jnp.zeros_like(state)

    for k in range(x_ref.shape[0] // PART):
        at = slice(k * PART, (k + 1) * PART)
        gram = lax.dot_general(
            c_ref[at, :], b_ref[at, :], (((1,), (1,)), ((), ())), preferred_element_type=f32
        )
        gram = jnp.where(lower, gram, 0.0)
        meta = meta_ref[at, :]
        grown = spread(jnp.exp2(meta), 0, chosen_ref[...])
        tail = spread(meta, 1, chosen_ref[...])
        held = jnp.dot(c_ref[at, :], state[...].astype(bf16), preferred_element_type=f32)
        fresh = []
        for q in range(pairs):
            cols = slice(q * 128, (q + 1) * 128)
            both = []
            for h in (2 * q, 2 * q + 1):
                power = jnp.minimum(meta[:, h : h + 1] - row_ref[h : h + 1, at], 100.0)
                both.append((gram * jnp.exp2(power)).astype(bf16))
            x = x_ref[at, cols]
            wide = x.astype(f32)
            none = jnp.zeros_like(x)
            stack = jnp.concatenate([jnp.where(left, x, none), jnp.where(left, none, x)], axis=0)
            inner = jnp.dot(jnp.concatenate(both, axis=1), stack, preferred_element_type=f32)
            y = inner + grown[:, cols] * held[:, cols] + skip_ref[0:1, cols] * wide
            y_ref[at, cols] = y.astype(bf16)
            fresh.append((wide * tail[:, cols]).astype(bf16))
        fresh = jnp.dot(
            turned_ref[:, at], jnp.concatenate(fresh, axis=1), preferred_element_type=f32
        )
        state[...] = state[...] * grown[PART - 1 : PART, :] + fresh


def local(x, b, c, turned, meta, row, chosen, skip, share, shares, before=()):
    length, width = x.shape
    tile = 256
    steps = length // tile // shares
    by_row = lambda i, s: (share * steps + i, 0)
    by_column = lambda i, s: (0, share * steps + i)
    one = lambda i, s: (0, 0)
    return pl.pallas_call(
        local_kernel,
        grid_spec=pltpu.PrefetchScalarGridSpec(
            num_scalar_prefetch=1,
            grid=(steps,),
            in_specs=[
                pl.BlockSpec((tile, width), by_row),
                pl.BlockSpec((tile, 128), by_row),
                pl.BlockSpec((tile, 128), by_row),
                pl.BlockSpec((128, tile), by_column),
                pl.BlockSpec((tile, 128), by_row),
                pl.BlockSpec((32, tile), by_column),
                pl.BlockSpec((256, width), one),
                pl.BlockSpec((16, width), one),
            ]
            + [pl.BlockSpec((128, width), one), pl.BlockSpec(memory_space=pl.ANY)] * (len(before) // 2),
            out_specs=[
                pl.BlockSpec((tile, width), by_row),
                pl.BlockSpec((128, width), one),
            ],
        ),
        out_shape=[
            jax.ShapeDtypeStruct((length, width), bf16),
            jax.ShapeDtypeStruct((128, width), f32),
        ],
        input_output_aliases={10: 0} if before else {},
        compiler_params=pltpu.CompilerParams(
            dimension_semantics=("arbitrary",), vmem_limit_bytes=24 << 20
        ),
        name="local",
    )(jnp.zeros((1,), jnp.int32), x, b, c, turned, meta, row, chosen, skip, *before)


def gate_kernel(
    scalars, block, y_ref, g_ref, c_ref, meta_ref, chosen_ref, mine_ref, other_ref,
    gain_ref, matrix_ref, top_ref, low_ref, ss_ref, matrix, gated, sem,
):
    rows, width = g_ref.shape
    half = width // 2
    first = block * rows

    @pl.when(first >= scalars[0])
    def _():
        top_ref[...] = jnp.zeros_like(top_ref)
        low_ref[...] = jnp.zeros_like(low_ref)
        ss_ref[...] = jnp.zeros_like(ss_ref)

    @pl.when(first < scalars[0])
    def _():
        copy = pltpu.make_async_copy(matrix_ref, matrix, sem)
        copy.start()
        low = scalars[1] == 0
        held = []
        for place in (0, 1):
            picked = jnp.where(
                low == (place == 0), mine_ref[...].astype(f32), other_ref[...].astype(f32)
            )
            held.append(picked.astype(bf16))

        def piece(k, _):
            at = pl.ds(pl.multiple_of(k * PART, PART), PART)
            grown = spread(jnp.exp2(meta_ref[at, :]), 2, chosen_ref[...])
            live = (first + k * PART + iota((PART, 1), 0) < scalars[0]).astype(f32)
            squares = jnp.zeros((PART, 128), f32)
            for place in (0, 1):
                wide = jnp.dot(c_ref[at, :], held[place], preferred_element_type=f32)
                for j in range(half // 128):
                    cols = slice(place * half + j * 128, place * half + (j + 1) * 128)
                    y = y_ref[at, cols].astype(f32)
                    y = y + grown[:, cols] * wide[:, j * 128 : (j + 1) * 128]
                    g = g_ref[at, cols].astype(f32)
                    v = y * live * (g / (1.0 + jnp.exp2(g * -LOG2E)))
                    squares = squares + v * v
                    gated[at, cols] = (v * gain_ref[0:1, cols]).astype(bf16)
            total = jnp.sum(squares, axis=1, keepdims=True)
            ss_ref[:, at] = jnp.broadcast_to(total, (PART, 128)).T[0:8, :]
            return 0

        lax.fori_loop(0, rows // PART, piece, 0)
        copy.wait()

        def columns(n, _):
            at = pl.ds(pl.multiple_of(n * 256, 256), 256)
            out = jnp.dot(gated[...], matrix[:, at], preferred_element_type=f32)
            top_ref[:, at] = out[: rows // 2].astype(bf16)
            low_ref[:, at] = out[rows // 2 :].astype(bf16)
            return 0

        lax.fori_loop(0, top_ref.shape[1] // 256, columns, 0)


def gate(scalars, y, g, c, meta, chosen, mine, other, gain, matrix):
    width = g.shape[1]
    wide = matrix.shape[1]
    rows = 512

    def at(i, s):
        return (s[2], 0)

    def body(s, *refs):
        gate_kernel(s, s[2], *refs)

    one = lambda i, s: (0, 0)
    return pl.pallas_call(
        body,
        grid_spec=pltpu.PrefetchScalarGridSpec(
            num_scalar_prefetch=1,
            grid=(1,),
            in_specs=[
                pl.BlockSpec((rows, width), at),
                pl.BlockSpec((rows, width), at),
                pl.BlockSpec((rows, 128), at),
                pl.BlockSpec((rows, 128), at),
                pl.BlockSpec((256, width), one),
                pl.BlockSpec((128, width // 2), one),
                pl.BlockSpec((128, width // 2), one),
                pl.BlockSpec((1, width), one),
                pl.BlockSpec(memory_space=pl.ANY),
            ],
            out_specs=[
                pl.BlockSpec((rows // 2, wide), one),
                pl.BlockSpec((rows // 2, wide), one),
                pl.BlockSpec((8, rows), one),
            ],
            scratch_shapes=[
                pltpu.VMEM((width, wide), bf16),
                pltpu.VMEM((rows, width), bf16),
                pltpu.SemaphoreType.DMA,
            ],
        ),
        out_shape=[
            jax.ShapeDtypeStruct((rows // 2, wide), bf16),
            jax.ShapeDtypeStruct((rows // 2, wide), bf16),
            jax.ShapeDtypeStruct((8, rows), f32),
        ],
        compiler_params=pltpu.CompilerParams(
            dimension_semantics=("arbitrary",), vmem_limit_bytes=32 << 20
        ),
        name="gate",
    )(scalars, y, g, c, meta, chosen, mine, other, gain, matrix)


def finish_kernel(own_a, own_b, last_a, last_b, s0, s1, s2, s3, out_ref):
    rows = own_a.shape[0]
    total = s0[...] + s1[...] + s2[...] + s3[...]
    scale = lax.rsqrt(total * (1.0 / (HEADS * P_SIZE)) + 1e-05)
    for k, parts in enumerate(((own_a, last_a), (own_b, last_b))):
        for j in range(rows // PART):
            at = slice(j * PART, (j + 1) * PART)
            lanes = slice(k * rows + j * PART, k * rows + (j + 1) * PART)
            factor = jnp.broadcast_to(scale[0:1, lanes], (PART, PART)).T
            for n in range(out_ref.shape[1] // 128):
                cols = slice(n * 128, (n + 1) * 128)
                value = sum(part[at, cols].astype(f32) for part in parts)
                out_ref[lanes, cols] = (value * factor).astype(bf16)


def finish(pieces, squares):
    rows, wide = pieces[0].shape
    tile = 640
    return pl.pallas_call(
        finish_kernel,
        grid=(wide // tile,),
        in_specs=[pl.BlockSpec((rows, tile), lambda i: (0, i))] * 4
        + [pl.BlockSpec((8, 2 * rows), lambda i: (0, 0))] * 4,
        out_specs=pl.BlockSpec((2 * rows, tile), lambda i: (0, i)),
        out_shape=jax.ShapeDtypeStruct((2 * rows, wide), bf16),
        compiler_params=pltpu.CompilerParams(
            dimension_semantics=("arbitrary",), vmem_limit_bytes=16 << 20
        ),
        name="finish",
    )(*pieces, *squares)


def unpack(ref):
    tail = ref[128:144, :].astype(f32)
    return ref[0:128, :].astype(f32), tail[0:1, :] + tail[1:2, :]


def pack(ref, state, decay):
    ref[0:128, :] = state.astype(bf16)
    high = decay.astype(bf16).astype(f32)
    line = iota((16, decay.shape[1]), 0)
    ref[128:144, :] = jnp.where(
        line == 0, high, jnp.where(line == 1, decay - high, 0.0)
    ).astype(bf16)


def join(earlier, later):
    return jnp.exp2(later[1]) * earlier[0] + later[0], earlier[1] + later[1]


def choose(test, one, two):
    return jax.tree.map(lambda x, y: jnp.where(test, x, y), one, two)


def scan_along(place, refs):
    pieces = [unpack(ref) for ref in refs]
    zero = jax.tree.map(jnp.zeros_like, pieces[0])
    inside = running = zero
    for k in range(4):
        at = lax.rem(place - k + 4, 4)
        piece = choose(
            at < 2, choose(at == 0, pieces[0], pieces[1]), choose(at == 2, pieces[2], pieces[3])
        )
        inside = choose(place == k, running, inside)
        running = join(running, piece)
    return inside, running


def chip_kernel(places, mine, theirs, out):
    first, second = unpack(mine), unpack(theirs)
    low = places[0] == 0
    pack(out, *join(choose(low, first, second), choose(low, second, first)))


def row_kernel(places, g0, g1, g2, g3, out, state, decay):
    inside, row = scan_along(places[1], (g0, g1, g2, g3))
    pack(out, *row)
    state[...] = inside[0]
    decay[...] = jnp.broadcast_to(inside[1], decay.shape)


def entry_kernel(places, g0, g1, g2, g3, state, decay, mine, theirs, own, away):
    before, _ = scan_along(places[2], (g0, g1, g2, g3))
    start = join(before, (state[...], decay[0:1, :]))
    first = choose(places[0] == 0, unpack(mine), unpack(theirs))
    middle = join(start, first)
    low = places[0] == 0
    own[...] = jnp.where(low, start[0], middle[0]).astype(bf16)
    away[...] = jnp.where(low, middle[0], start[0]).astype(bf16)


def small_call(kernel, name, out_shapes, places, *arrays):
    near = pl.BlockSpec(memory_space=pltpu.VMEM)
    return pl.pallas_call(
        kernel,
        in_specs=[pl.BlockSpec(memory_space=pltpu.SMEM)] + [near] * len(arrays),
        out_specs=[near] * len(out_shapes),
        out_shape=out_shapes,
        compiler_params=pltpu.CompilerParams(vmem_limit_bytes=8 << 20),
        name=name,
    )(places, *arrays)


def shift(value, axis, by, wrap=True):
    count = lax.axis_size(axis)
    pairs = [(i, (i + by) % count) for i in range(count) if wrap or i + by < count]
    return lax.ppermute(value, axis, pairs)


def gather_ring(value, axis):
    return [value] + [shift(value, axis, by) for by in (1, 2, 3)]


def incoming(mine, other, places, first_share, second_share):
    half = mine.shape[1]
    message = jax.ShapeDtypeStruct(mine.shape, bf16)
    state = jax.ShapeDtypeStruct((128, half), f32)
    decay = jax.ShapeDtypeStruct((8, half), f32)
    held = jax.ShapeDtypeStruct((128, half), bf16)
    theirs = shift(other, "seq_2", 1)
    (chip,) = small_call(chip_kernel, "chip", [message], places, mine, theirs)
    pieces = gather_ring(chip, "seq_1")
    shared = first_share()
    row, inside, faded = small_call(row_kernel, "row", [message, state, decay], places, *pieces)
    row, shared = lax.optimization_barrier((row, shared))
    pieces = gather_ring(row, "seq_0")
    y = second_share(*shared)
    pieces, y = lax.optimization_barrier((pieces, y))
    own, away = small_call(
        entry_kernel, "entry", [held, held], places, *pieces, inside, faded, mine, theirs
    )
    return own, shift(away, "seq_2", 1), y


def body(
    values,
    gates,
    b_proj,
    c_proj,
    step_size,
    decay_rate,
    skip_gain,
    norm_gain,
    readout_matrix,
    span_counts,
    remaining_count,
):
    length, width = values.shape
    valid = (span_counts[0] - 1) * SPAN + remaining_count[0]
    core = lax.axis_index("seq_2")
    place = lax.axis_index("head")
    roles = [
        jnp.stack([valid, core, (place + role) % 4]).astype(jnp.int32) for role in range(4)
    ]
    scalars = roles[0]
    meta, row, turned, chosen, skip, mine, other = states(
        scalars, values, b_proj, decay_rate, step_size, skip_gain[None, :]
    )

    def share(k, before=()):
        return local(
            values, b_proj, c_proj, turned, meta, row, chosen, skip, k, 2, before
        )

    places = jnp.stack([core, lax.axis_index("seq_1"), lax.axis_index("seq_0")]).astype(jnp.int32)
    own, theirs, y = incoming(
        mine, other, places, lambda: share(0), lambda y, state: share(1, (state, y))[0]
    )
    gain = norm_gain[None, :]

    def part(role, block=None):
        return gate(
            roles[role] if block is None else block, y, gates, c_proj, meta, chosen, own, theirs, gain, readout_matrix
        )

    def reduced(blocks):
        def send(value, by, role):
            pairs = [(z, (z + by) % 4) for z in range(4) if (z + role) % 4 < blocks]
            return lax.ppermute(value, "head", pairs)

        def add(one, two):
            return (one.astype(f32) + two.astype(f32)).astype(bf16)

        def all_live():
            far_a, far_b, s2 = part(2)
            far_a, far_b = send(far_a, 1, 2), send(far_b, -1, 2)
            up_a, up_b, s1 = part(1)
            up_b = send(up_b, 1, 1)
            down_a, down_b, s3 = part(3)
            down_a = send(down_a, -1, 3)
            up_a, down_b, last = lax.optimization_barrier(
                (add(up_a, far_a), add(down_b, far_b), roles[0])
            )
            up_a, down_b = send(up_a, 1, 1), send(down_b, -1, 3)
            s2, s1, s3 = send(s2, 2, 2), send(s1, 1, 1), send(s3, -1, 3)
            own_a, own_b, s0 = part(0, last)
            return (add(own_a, down_a), add(own_b, up_b), up_a, down_b), (s0, s1, s2, s3)

        def few_live():
            far_a, far_b, s2 = part(2)
            far_a, far_b = send(far_a, 1, 2), send(far_b, -1, 2)
            up_a, up_b, s1 = part(1)
            up_b = send(up_b, 1, 1)
            down_a, down_b, s3 = part(3)
            down_a = send(down_a, -1, 3)
            own_a, own_b, s0 = part(0)
            s2, s1, s3 = send(s2, 2, 2), send(s1, 1, 1), send(s3, -1, 3)
            far_a, far_b, s1, s2, s3, own_a = lax.optimization_barrier(
                (far_a, far_b, s1, s2, s3, own_a)
            )
            up_a = send(add(up_a, far_a), 1, 1)
            down_b = send(add(down_b, far_b), -1, 3)
            return (add(own_a, down_a), add(own_b, up_b), up_a, down_b), (s0, s1, s2, s3)

        return all_live if blocks == 4 else few_live

    quarter = length // 4
    level = (valid > quarter).astype(jnp.int32) + (valid > 2 * quarter)
    return finish(*lax.switch(level, [reduced(n) for n in (1, 2, 4)]))


def solution(mesh):
    finer = Mesh(
        mesh.devices.reshape(4, 4, 2, mesh.shape["head"]), ("seq_0", "seq_1", "seq_2", "head")
    )
    return jax.shard_map(
        body,
        mesh=finer,
        in_specs=(
            P(SEQ, "head"),
            P(SEQ, "head"),
            P(SEQ, None),
            P(SEQ, None),
            P("head", SEQ),
            P("head", SEQ),
            P("head"),
            P("head"),
            P("head", None),
            P(SEQ),
            P(SEQ),
        ),
        out_specs=P(SEQ_HEAD, None),
        check_vma=False,
    )
```

```python
import jax
import jax.numpy as jnp
from jax import lax
from jax.experimental import pallas as pl
from jax.experimental.pallas import tpu as pltpu
from jax.sharding import Mesh
from jax.sharding import PartitionSpec as P

HEADS = 80
P_SIZE = 64
SPAN = 256
PART = 128
SEQ = ("seq_0", "seq_1", "seq_2")
SEQ_HEAD = ("seq_0", "seq_1", "seq_2", "head")
LOG2E = 1.4426950408889634
HIGHEST = lax.Precision.HIGHEST
f32 = jnp.float32
bf16 = jnp.bfloat16


def iota(shape, dim):
    return lax.broadcasted_iota(jnp.int32, shape, dim)


def selector(width):
    rows, cols = iota((256, width), 0), iota((256, width), 1)
    return ((rows % 32) == cols // P_SIZE).astype(f32).astype(bf16)


def spread(columns, group, chosen):
    lane = iota(columns.shape, 1)
    columns = jnp.where((lane >= 32 * group) & (lane < 32 * group + 32), columns, 0.0)
    high = columns.astype(bf16)
    low = (columns - high.astype(f32)).astype(bf16)
    return jnp.dot(
        jnp.concatenate([high, low], axis=1), chosen, preferred_element_type=f32
    )


def states_kernel(
    scalars, x_ref, b_ref, rate_ref, dt_ref, skip_ref,
    meta_ref, row_ref, turned_ref, chosen_ref, wide_skip_ref, mine_ref, other_ref,
    state, raw, weighted, small,
):
    step = pl.program_id(0)
    heads, length = rate_ref.shape
    parts = length // PART
    rows, width = x_ref.shape
    half = width // 2

    @pl.when(step == 0)
    def _():
        state[...] = jnp.zeros_like(state)
        raw[...] = jnp.zeros_like(raw)
        chosen_ref[...] = selector(width)
        small[...] = jnp.zeros_like(small)
        small[0:1, 0:heads] = skip_ref[...]
        wide_skip_ref[...] = spread(small[...], 0, chosen_ref[...])
        for k in range(parts):
            at = slice(k * PART, (k + 1) * PART)
            live = (k * PART + iota((1, PART), 1) < scalars[0]).astype(f32)
            raw[0, 32 * k : 32 * k + heads, :] = rate_ref[:, at] * (live * -LOG2E)
            raw[1, 32 * k : 32 * k + heads, :] = dt_ref[:, at] * live
        upper = (iota((PART, PART), 0) <= iota((PART, PART), 1)).astype(f32)
        running = jnp.dot(raw[0], upper, precision=HIGHEST, preferred_element_type=f32)
        ends = jnp.broadcast_to(running[:, PART - 1 : PART], running.shape)
        leads = [jnp.zeros((32, PART), f32)]
        for k in range(parts):
            leads.append(leads[-1] + ends[32 * k : 32 * k + 32])
        for k in range(parts):
            at = slice(k * PART, (k + 1) * PART)
            run = running[32 * k : 32 * k + 32]
            weight = raw[1, 32 * k : 32 * k + 32, :]
            total = leads[k] + run
            row_ref[:, at] = run - jnp.where(weight > 0, jnp.log(weight) * LOG2E, -1e30)
            tail = jnp.exp2(ends[32 * k : 32 * k + 32] - run) * weight
            last = jnp.exp2(leads[parts] - total) * weight
            meta_ref[at, :] = jnp.concatenate([run, tail, total, last], axis=0).T

    here = pl.ds(pl.multiple_of(step * rows, rows), rows)
    wide = spread(meta_ref[here, :], 3, chosen_ref[...])
    weighted[...] = (x_ref[...].astype(f32) * wide).astype(bf16)
    turned = b_ref[...].astype(f32).T.astype(bf16)
    turned_ref[...] = turned
    state[...] += jnp.dot(turned, weighted[...], preferred_element_type=f32)

    @pl.when(step == pl.num_programs(0) - 1)
    def _():
        wide = spread(meta_ref[length - 16 : length, :], 2, chosen_ref[...])[15:16, :]
        high = wide.astype(bf16).astype(f32)
        line = iota((16, width), 0)
        decay = jnp.where(line == 0, high, jnp.where(line == 1, wide - high, 0.0))
        core = scalars[1]
        for place, ref in ((0, mine_ref), (1, other_ref)):
            low = core == place
            ref[0:128, :] = jnp.where(low, state[:, :half], state[:, half:]).astype(bf16)
            ref[128:144, :] = jnp.where(low, decay[:, :half], decay[:, half:]).astype(bf16)


def states(scalars, x, b, rate, dt, skip):
    length, width = x.shape
    heads = rate.shape[0]
    steps = 4
    rows = length // steps
    one = lambda i, s: (0, 0)
    return pl.pallas_call(
        states_kernel,
        grid_spec=pltpu.PrefetchScalarGridSpec(
            num_scalar_prefetch=1,
            grid=(steps,),
            in_specs=[
                pl.BlockSpec((rows, width), lambda i, s: (i, 0)),
                pl.BlockSpec((rows, 128), lambda i, s: (i, 0)),
                pl.BlockSpec((heads, length), one),
                pl.BlockSpec((heads, length), one),
                pl.BlockSpec((1, heads), one),
            ],
            out_specs=[
                pl.BlockSpec((length, 128), one),
                pl.BlockSpec((32, length), one),
                pl.BlockSpec((128, rows), lambda i, s: (0, i)),
                pl.BlockSpec((256, width), one),
                pl.BlockSpec((16, width), one),
                pl.BlockSpec((144, width // 2), one),
                pl.BlockSpec((144, width // 2), one),
            ],
            scratch_shapes=[
                pltpu.VMEM((128, width), f32),
                pltpu.VMEM((2, 32 * (length // PART), PART), f32),
                pltpu.VMEM((rows, width), bf16),
                pltpu.VMEM((16, 128), f32),
            ],
        ),
        out_shape=[
            jax.ShapeDtypeStruct((length, 128), f32),
            jax.ShapeDtypeStruct((32, length), f32),
            jax.ShapeDtypeStruct((128, length), bf16),
            jax.ShapeDtypeStruct((256, width), bf16),
            jax.ShapeDtypeStruct((16, width), f32),
            jax.ShapeDtypeStruct((144, width // 2), bf16),
            jax.ShapeDtypeStruct((144, width // 2), bf16),
        ],
        compiler_params=pltpu.CompilerParams(
            dimension_semantics=("arbitrary",), vmem_limit_bytes=56 << 20
        ),
        name="states",
    )(scalars, x, b, rate, dt, skip)


def local_kernel(
    share, x_ref, b_ref, c_ref, turned_ref, meta_ref, row_ref, chosen_ref, skip_ref, *rest,
):
    y_ref, state = rest[-2:]
    width = x_ref.shape[1]
    pairs = width // 128
    lower = iota((PART, PART), 0) >= iota((PART, PART), 1)
    left = iota((PART, 128), 1) < 64

    @pl.when(pl.program_id(0) == 0)
    def _():
        state[...] = rest[0][...] if len(rest) == 4 else jnp.zeros_like(state)

    for k in range(x_ref.shape[0] // PART):
        at = slice(k * PART, (k + 1) * PART)
        gram = lax.dot_general(
            c_ref[at, :], b_ref[at, :], (((1,), (1,)), ((), ())), preferred_element_type=f32
        )
        gram = jnp.where(lower, gram, 0.0)
        meta = meta_ref[at, :]
        grown = spread(jnp.exp2(meta), 0, chosen_ref[...])
        tail = spread(meta, 1, chosen_ref[...])
        held = jnp.dot(c_ref[at, :], state[...].astype(bf16), preferred_element_type=f32)
        fresh = []
        for q in range(pairs):
            cols = slice(q * 128, (q + 1) * 128)
            both = []
            for h in (2 * q, 2 * q + 1):
                power = jnp.minimum(meta[:, h : h + 1] - row_ref[h : h + 1, at], 100.0)
                both.append((gram * jnp.exp2(power)).astype(bf16))
            x = x_ref[at, cols]
            wide = x.astype(f32)
            none = jnp.zeros_like(x)
            stack = jnp.concatenate([jnp.where(left, x, none), jnp.where(left, none, x)], axis=0)
            inner = jnp.dot(jnp.concatenate(both, axis=1), stack, preferred_element_type=f32)
            y = inner + grown[:, cols] * held[:, cols] + skip_ref[0:1, cols] * wide
            y_ref[at, cols] = y.astype(bf16)
            fresh.append((wide * tail[:, cols]).astype(bf16))
        fresh = jnp.dot(
            turned_ref[:, at], jnp.concatenate(fresh, axis=1), preferred_element_type=f32
        )
        state[...] = state[...] * grown[PART - 1 : PART, :] + fresh


def local(x, b, c, turned, meta, row, chosen, skip, share, shares, before=()):
    length, width = x.shape
    tile = 256
    steps = length // tile // shares
    by_row = lambda i, s: (share * steps + i, 0)
    by_column = lambda i, s: (0, share * steps + i)
    one = lambda i, s: (0, 0)
    return pl.pallas_call(
        local_kernel,
        grid_spec=pltpu.PrefetchScalarGridSpec(
            num_scalar_prefetch=1,
            grid=(steps,),
            in_specs=[
                pl.BlockSpec((tile, width), by_row),
                pl.BlockSpec((tile, 128), by_row),
                pl.BlockSpec((tile, 128), by_row),
                pl.BlockSpec((128, tile), by_column),
                pl.BlockSpec((tile, 128), by_row),
                pl.BlockSpec((32, tile), by_column),
                pl.BlockSpec((256, width), one),
                pl.BlockSpec((16, width), one),
            ]
            + [pl.BlockSpec((128, width), one), pl.BlockSpec(memory_space=pl.ANY)] * (len(before) // 2),
            out_specs=[
                pl.BlockSpec((tile, width), by_row),
                pl.BlockSpec((128, width), one),
            ],
        ),
        out_shape=[
            jax.ShapeDtypeStruct((length, width), bf16),
            jax.ShapeDtypeStruct((128, width), f32),
        ],
        input_output_aliases={10: 0} if before else {},
        compiler_params=pltpu.CompilerParams(
            dimension_semantics=("arbitrary",), vmem_limit_bytes=54 << 20
        ),
        name="local",
    )(jnp.zeros((1,), jnp.int32), x, b, c, turned, meta, row, chosen, skip, *before)


def gate_kernel(
    scalars, block, y_ref, g_ref, c_ref, meta_ref, chosen_ref, mine_ref, other_ref,
    gain_ref, matrix_ref, top_ref, low_ref, ss_ref, matrix, gated, sem,
):
    rows, width = g_ref.shape
    half = width // 2
    first = block * rows

    @pl.when(first >= scalars[0])
    def _():
        top_ref[...] = jnp.zeros_like(top_ref)
        low_ref[...] = jnp.zeros_like(low_ref)
        ss_ref[...] = jnp.zeros_like(ss_ref)

    @pl.when(first < scalars[0])
    def _():
        copy = pltpu.make_async_copy(matrix_ref, matrix, sem)
        copy.start()
        low = scalars[1] == 0
        held = []
        for place in (0, 1):
            picked = jnp.where(
                low == (place == 0), mine_ref[...].astype(f32), other_ref[...].astype(f32)
            )
            held.append(picked.astype(bf16))

        def piece(k, _):
            at = pl.ds(pl.multiple_of(k * PART, PART), PART)
            grown = spread(jnp.exp2(meta_ref[at, :]), 2, chosen_ref[...])
            live = (first + k * PART + iota((PART, 1), 0) < scalars[0]).astype(f32)
            squares = jnp.zeros((PART, 128), f32)
            for place in (0, 1):
                wide = jnp.dot(c_ref[at, :], held[place], preferred_element_type=f32)
                for j in range(half // 128):
                    cols = slice(place * half + j * 128, place * half + (j + 1) * 128)
                    y = y_ref[at, cols].astype(f32)
                    y = y + grown[:, cols] * wide[:, j * 128 : (j + 1) * 128]
                    g = g_ref[at, cols].astype(f32)
                    v = y * live * (g / (1.0 + jnp.exp2(g * -LOG2E)))
                    squares = squares + v * v
                    gated[at, cols] = (v * gain_ref[0:1, cols]).astype(bf16)
            total = jnp.sum(squares, axis=1, keepdims=True)
            ss_ref[:, at] = jnp.broadcast_to(total, (PART, 128)).T[0:8, :]
            return 0

        lax.fori_loop(0, rows // PART, piece, 0)
        copy.wait()

        def columns(n, _):
            at = pl.ds(pl.multiple_of(n * 256, 256), 256)
            out = jnp.dot(gated[...], matrix[:, at], preferred_element_type=f32)
            top_ref[:, at] = out[: rows // 2].astype(bf16)
            low_ref[:, at] = out[rows // 2 :].astype(bf16)
            return 0

        lax.fori_loop(0, top_ref.shape[1] // 256, columns, 0)


def gate(scalars, y, g, c, meta, chosen, mine, other, gain, matrix):
    width = g.shape[1]
    wide = matrix.shape[1]
    rows = 512

    def at(i, s):
        return (s[2], 0)

    def body(s, *refs):
        gate_kernel(s, s[2], *refs)

    one = lambda i, s: (0, 0)
    return pl.pallas_call(
        body,
        grid_spec=pltpu.PrefetchScalarGridSpec(
            num_scalar_prefetch=1,
            grid=(1,),
            in_specs=[
                pl.BlockSpec((rows, width), at),
                pl.BlockSpec((rows, width), at),
                pl.BlockSpec((rows, 128), at),
                pl.BlockSpec((rows, 128), at),
                pl.BlockSpec((256, width), one),
                pl.BlockSpec((128, width // 2), one),
                pl.BlockSpec((128, width // 2), one),
                pl.BlockSpec((1, width), one),
                pl.BlockSpec(memory_space=pl.ANY),
            ],
            out_specs=[
                pl.BlockSpec((rows // 2, wide), one),
                pl.BlockSpec((rows // 2, wide), one),
                pl.BlockSpec((8, rows), one),
            ],
            scratch_shapes=[
                pltpu.VMEM((width, wide), bf16),
                pltpu.VMEM((rows, width), bf16),
                pltpu.SemaphoreType.DMA,
            ],
        ),
        out_shape=[
            jax.ShapeDtypeStruct((rows // 2, wide), bf16),
            jax.ShapeDtypeStruct((rows // 2, wide), bf16),
            jax.ShapeDtypeStruct((8, rows), f32),
        ],
        compiler_params=pltpu.CompilerParams(
            dimension_semantics=("arbitrary",), vmem_limit_bytes=32 << 20
        ),
        name="gate",
    )(scalars, y, g, c, meta, chosen, mine, other, gain, matrix)


def finish_kernel(own_a, own_b, last_a, last_b, s0, s1, s2, s3, out_ref):
    rows = own_a.shape[0]
    total = s0[...] + s1[...] + s2[...] + s3[...]
    scale = lax.rsqrt(total * (1.0 / (HEADS * P_SIZE)) + 1e-05)
    for k, parts in enumerate(((own_a, last_a), (own_b, last_b))):
        for j in range(rows // PART):
            at = slice(j * PART, (j + 1) * PART)
            lanes = slice(k * rows + j * PART, k * rows + (j + 1) * PART)
            factor = jnp.broadcast_to(scale[0:1, lanes], (PART, PART)).T
            for n in range(out_ref.shape[1] // 128):
                cols = slice(n * 128, (n + 1) * 128)
                value = sum(part[at, cols].astype(f32) for part in parts)
                out_ref[lanes, cols] = (value * factor).astype(bf16)


def finish(pieces, squares):
    rows, wide = pieces[0].shape
    tile = 640
    return pl.pallas_call(
        finish_kernel,
        grid=(wide // tile,),
        in_specs=[pl.BlockSpec((rows, tile), lambda i: (0, i))] * 4
        + [pl.BlockSpec((8, 2 * rows), lambda i: (0, 0))] * 4,
        out_specs=pl.BlockSpec((2 * rows, tile), lambda i: (0, i)),
        out_shape=jax.ShapeDtypeStruct((2 * rows, wide), bf16),
        compiler_params=pltpu.CompilerParams(
            dimension_semantics=("arbitrary",), vmem_limit_bytes=16 << 20
        ),
        name="finish",
    )(*pieces, *squares)


def unpack(ref):
    tail = ref[128:144, :].astype(f32)
    return ref[0:128, :].astype(f32), tail[0:1, :] + tail[1:2, :]


def pack(ref, state, decay):
    ref[0:128, :] = state.astype(bf16)
    high = decay.astype(bf16).astype(f32)
    line = iota((16, decay.shape[1]), 0)
    ref[128:144, :] = jnp.where(
        line == 0, high, jnp.where(line == 1, decay - high, 0.0)
    ).astype(bf16)


def join(earlier, later):
    return jnp.exp2(later[1]) * earlier[0] + later[0], earlier[1] + later[1]


def choose(test, one, two):
    return jax.tree.map(lambda x, y: jnp.where(test, x, y), one, two)


def scan_along(place, refs):
    pieces = [unpack(ref) for ref in refs]
    zero = jax.tree.map(jnp.zeros_like, pieces[0])
    inside = running = zero
    for k in range(4):
        at = lax.rem(place - k + 4, 4)
        piece = choose(
            at < 2, choose(at == 0, pieces[0], pieces[1]), choose(at == 2, pieces[2], pieces[3])
        )
        inside = choose(place == k, running, inside)
        running = join(running, piece)
    return inside, running


def chip_kernel(places, mine, theirs, out):
    first, second = unpack(mine), unpack(theirs)
    low = places[0] == 0
    pack(out, *join(choose(low, first, second), choose(low, second, first)))


def row_kernel(places, g0, g1, g2, g3, out, state, decay):
    inside, row = scan_along(places[1], (g0, g1, g2, g3))
    pack(out, *row)
    state[...] = inside[0]
    decay[...] = jnp.broadcast_to(inside[1], decay.shape)


def entry_kernel(places, g0, g1, g2, g3, state, decay, mine, theirs, own, away):
    before, _ = scan_along(places[2], (g0, g1, g2, g3))
    start = join(before, (state[...], decay[0:1, :]))
    first = choose(places[0] == 0, unpack(mine), unpack(theirs))
    middle = join(start, first)
    low = places[0] == 0
    own[...] = jnp.where(low, start[0], middle[0]).astype(bf16)
    away[...] = jnp.where(low, middle[0], start[0]).astype(bf16)


def small_call(kernel, name, out_shapes, places, *arrays):
    near = pl.BlockSpec(memory_space=pltpu.VMEM)
    return pl.pallas_call(
        kernel,
        in_specs=[pl.BlockSpec(memory_space=pltpu.SMEM)] + [near] * len(arrays),
        out_specs=[near] * len(out_shapes),
        out_shape=out_shapes,
        compiler_params=pltpu.CompilerParams(vmem_limit_bytes=8 << 20),
        name=name,
    )(places, *arrays)


def shift(value, axis, by, wrap=True):
    count = lax.axis_size(axis)
    pairs = [(i, (i + by) % count) for i in range(count) if wrap or i + by < count]
    return lax.ppermute(value, axis, pairs)


def gather_ring(value, axis):
    return [value] + [shift(value, axis, by) for by in (1, 2, 3)]


def incoming(mine, other, places, first_share, second_share):
    half = mine.shape[1]
    message = jax.ShapeDtypeStruct(mine.shape, bf16)
    state = jax.ShapeDtypeStruct((128, half), f32)
    decay = jax.ShapeDtypeStruct((8, half), f32)
    held = jax.ShapeDtypeStruct((128, half), bf16)
    theirs = shift(other, "seq_2", 1)
    (chip,) = small_call(chip_kernel, "chip", [message], places, mine, theirs)
    pieces = gather_ring(chip, "seq_1")
    shared = first_share()
    row, inside, faded = small_call(row_kernel, "row", [message, state, decay], places, *pieces)
    row, shared = lax.optimization_barrier((row, shared))
    pieces = gather_ring(row, "seq_0")
    y = second_share(*shared)
    pieces, y = lax.optimization_barrier((pieces, y))
    own, away = small_call(
        entry_kernel, "entry", [held, held], places, *pieces, inside, faded, mine, theirs
    )
    return own, shift(away, "seq_2", 1), y


def body(
    values,
    gates,
    b_proj,
    c_proj,
    step_size,
    decay_rate,
    skip_gain,
    norm_gain,
    readout_matrix,
    span_counts,
    remaining_count,
):
    length, width = values.shape
    valid = (span_counts[0] - 1) * SPAN + remaining_count[0]
    core = lax.axis_index("seq_2")
    place = lax.axis_index("head")
    roles = [
        jnp.stack([valid, core, (place + role) % 4]).astype(jnp.int32) for role in range(4)
    ]
    scalars = roles[0]
    meta, row, turned, chosen, skip, mine, other = states(
        scalars, values, b_proj, decay_rate, step_size, skip_gain[None, :]
    )

    def share(k, before=()):
        return local(
            values, b_proj, c_proj, turned, meta, row, chosen, skip, k, 2, before
        )

    places = jnp.stack([core, lax.axis_index("seq_1"), lax.axis_index("seq_0")]).astype(jnp.int32)
    own, theirs, y = incoming(
        mine, other, places, lambda: share(0), lambda y, state: share(1, (state, y))[0]
    )
    gain = norm_gain[None, :]

    def part(role, block=None):
        return gate(
            roles[role] if block is None else block, y, gates, c_proj, meta, chosen, own, theirs, gain, readout_matrix
        )

    def reduced(blocks):
        def send(value, by, role):
            pairs = [(z, (z + by) % 4) for z in range(4) if (z + role) % 4 < blocks]
            return lax.ppermute(value, "head", pairs)

        def add(one, two):
            return (one.astype(f32) + two.astype(f32)).astype(bf16)

        def all_live():
            far_a, far_b, s2 = part(2)
            far_a, far_b = send(far_a, 1, 2), send(far_b, -1, 2)
            up_a, up_b, s1 = part(1)
            up_b = send(up_b, 1, 1)
            down_a, down_b, s3 = part(3)
            down_a = send(down_a, -1, 3)
            up_a, down_b, last = lax.optimization_barrier(
                (add(up_a, far_a), add(down_b, far_b), roles[0])
            )
            up_a, down_b = send(up_a, 1, 1), send(down_b, -1, 3)
            s2, s1, s3 = send(s2, 2, 2), send(s1, 1, 1), send(s3, -1, 3)
            own_a, own_b, s0 = part(0, last)
            return (add(own_a, down_a), add(own_b, up_b), up_a, down_b), (s0, s1, s2, s3)

        def few_live():
            far_a, far_b, s2 = part(2)
            far_a, far_b = send(far_a, 1, 2), send(far_b, -1, 2)
            up_a, up_b, s1 = part(1)
            up_b = send(up_b, 1, 1)
            down_a, down_b, s3 = part(3)
            down_a = send(down_a, -1, 3)
            own_a, own_b, s0 = part(0)
            s2, s1, s3 = send(s2, 2, 2), send(s1, 1, 1), send(s3, -1, 3)
            far_a, far_b, s1, s2, s3, own_a = lax.optimization_barrier(
                (far_a, far_b, s1, s2, s3, own_a)
            )
            up_a = send(add(up_a, far_a), 1, 1)
            down_b = send(add(down_b, far_b), -1, 3)
            return (add(own_a, down_a), add(own_b, up_b), up_a, down_b), (s0, s1, s2, s3)

        return all_live if blocks == 4 else few_live

    quarter = length // 4
    level = (valid > quarter).astype(jnp.int32) + (valid > 2 * quarter)
    return finish(*lax.switch(level, [reduced(n) for n in (1, 2, 4)]))


def solution(mesh):
    finer = Mesh(
        mesh.devices.reshape(4, 4, 2, mesh.shape["head"]), ("seq_0", "seq_1", "seq_2", "head")
    )
    return jax.shard_map(
        body,
        mesh=finer,
        in_specs=(
            P(SEQ, "head"),
            P(SEQ, "head"),
            P(SEQ, None),
            P(SEQ, None),
            P("head", SEQ),
            P("head", SEQ),
            P("head"),
            P("head"),
            P("head", None),
            P(SEQ),
            P(SEQ),
        ),
        out_specs=P(SEQ_HEAD, None),
        check_vma=False,
    )
```

```python
import jax
import jax.numpy as jnp
from jax import lax
from jax.experimental import pallas as pl
from jax.experimental.pallas import tpu as pltpu
from jax.sharding import Mesh
from jax.sharding import PartitionSpec as P

HEADS = 80
P_SIZE = 64
SPAN = 256
PART = 128
SEQ = ("seq_0", "seq_1", "seq_2")
SEQ_HEAD = ("seq_0", "seq_1", "seq_2", "head")
LOG2E = 1.4426950408889634
HIGHEST = lax.Precision.HIGHEST
f32 = jnp.float32
bf16 = jnp.bfloat16


def iota(shape, dim):
    return lax.broadcasted_iota(jnp.int32, shape, dim)


def selector(width):
    rows, cols = iota((256, width), 0), iota((256, width), 1)
    return ((rows % 32) == cols // P_SIZE).astype(f32).astype(bf16)


def spread(columns, group, chosen):
    lane = iota(columns.shape, 1)
    columns = jnp.where((lane >= 32 * group) & (lane < 32 * group + 32), columns, 0.0)
    high = columns.astype(bf16)
    low = (columns - high.astype(f32)).astype(bf16)
    return jnp.dot(
        jnp.concatenate([high, low], axis=1), chosen, preferred_element_type=f32
    )


def states_kernel(
    scalars, x_ref, b_ref, rate_ref, dt_ref, skip_ref,
    meta_ref, row_ref, turned_ref, chosen_ref, wide_skip_ref, mine_ref, other_ref,
    state, raw, weighted, small,
):
    step = pl.program_id(0)
    heads, length = rate_ref.shape
    parts = length // PART
    rows, width = x_ref.shape
    half = width // 2

    @pl.when(step == 0)
    def _():
        state[...] = jnp.zeros_like(state)
        raw[...] = jnp.zeros_like(raw)
        chosen_ref[...] = selector(width)
        small[...] = jnp.zeros_like(small)
        small[0:1, 0:heads] = skip_ref[...]
        wide_skip_ref[...] = spread(small[...], 0, chosen_ref[...])
        for k in range(parts):
            at = slice(k * PART, (k + 1) * PART)
            live = (k * PART + iota((1, PART), 1) < scalars[0]).astype(f32)
            raw[0, 32 * k : 32 * k + heads, :] = rate_ref[:, at] * (live * -LOG2E)
            raw[1, 32 * k : 32 * k + heads, :] = dt_ref[:, at] * live
        upper = (iota((PART, PART), 0) <= iota((PART, PART), 1)).astype(f32)
        running = jnp.dot(raw[0], upper, precision=HIGHEST, preferred_element_type=f32)
        ends = jnp.broadcast_to(running[:, PART - 1 : PART], running.shape)
        leads = [jnp.zeros((32, PART), f32)]
        for k in range(parts):
            leads.append(leads[-1] + ends[32 * k : 32 * k + 32])
        for k in range(parts):
            at = slice(k * PART, (k + 1) * PART)
            run = running[32 * k : 32 * k + 32]
            weight = raw[1, 32 * k : 32 * k + 32, :]
            total = leads[k] + run
            row_ref[:, at] = run - jnp.where(weight > 0, jnp.log(weight) * LOG2E, -1e30)
            tail = jnp.exp2(ends[32 * k : 32 * k + 32] - run) * weight
            last = jnp.exp2(leads[parts] - total) * weight
            meta_ref[at, :] = jnp.concatenate([run, tail, total, last], axis=0).T

    here = pl.ds(pl.multiple_of(step * rows, rows), rows)
    wide = spread(meta_ref[here, :], 3, chosen_ref[...])
    weighted[...] = (x_ref[...].astype(f32) * wide).astype(bf16)
    turned = b_ref[...].astype(f32).T.astype(bf16)
    turned_ref[...] = turned
    state[...] += jnp.dot(turned, weighted[...], preferred_element_type=f32)

    @pl.when(step == pl.num_programs(0) - 1)
    def _():
        wide = spread(meta_ref[length - 16 : length, :], 2, chosen_ref[...])[15:16, :]
        high = wide.astype(bf16).astype(f32)
        line = iota((16, width), 0)
        decay = jnp.where(line == 0, high, jnp.where(line == 1, wide - high, 0.0))
        core = scalars[1]
        for place, ref in ((0, mine_ref), (1, other_ref)):
            low = core == place
            ref[0:128, :] = jnp.where(low, state[:, :half], state[:, half:]).astype(bf16)
            ref[128:144, :] = jnp.where(low, decay[:, :half], decay[:, half:]).astype(bf16)


def states(scalars, x, b, rate, dt, skip):
    length, width = x.shape
    heads = rate.shape[0]
    steps = 4
    rows = length // steps
    one = lambda i, s: (0, 0)
    return pl.pallas_call(
        states_kernel,
        grid_spec=pltpu.PrefetchScalarGridSpec(
            num_scalar_prefetch=1,
            grid=(steps,),
            in_specs=[
                pl.BlockSpec((rows, width), lambda i, s: (i, 0)),
                pl.BlockSpec((rows, 128), lambda i, s: (i, 0)),
                pl.BlockSpec((heads, length), one),
                pl.BlockSpec((heads, length), one),
                pl.BlockSpec((1, heads), one),
            ],
            out_specs=[
                pl.BlockSpec((length, 128), one),
                pl.BlockSpec((32, length), one),
                pl.BlockSpec((128, rows), lambda i, s: (0, i)),
                pl.BlockSpec((256, width), one),
                pl.BlockSpec((16, width), one),
                pl.BlockSpec((144, width // 2), one),
                pl.BlockSpec((144, width // 2), one),
            ],
            scratch_shapes=[
                pltpu.VMEM((128, width), f32),
                pltpu.VMEM((2, 32 * (length // PART), PART), f32),
                pltpu.VMEM((rows, width), bf16),
                pltpu.VMEM((16, 128), f32),
            ],
        ),
        out_shape=[
            jax.ShapeDtypeStruct((length, 128), f32),
            jax.ShapeDtypeStruct((32, length), f32),
            jax.ShapeDtypeStruct((128, length), bf16),
            jax.ShapeDtypeStruct((256, width), bf16),
            jax.ShapeDtypeStruct((16, width), f32),
            jax.ShapeDtypeStruct((144, width // 2), bf16),
            jax.ShapeDtypeStruct((144, width // 2), bf16),
        ],
        compiler_params=pltpu.CompilerParams(
            dimension_semantics=("arbitrary",), vmem_limit_bytes=56 << 20
        ),
        name="states",
    )(scalars, x, b, rate, dt, skip)


def local_kernel(
    share, x_ref, b_ref, c_ref, turned_ref, meta_ref, row_ref, chosen_ref, skip_ref, *rest,
):
    y_ref, state = rest[-2:]
    width = x_ref.shape[1]
    pairs = width // 128
    lower = iota((PART, PART), 0) >= iota((PART, PART), 1)
    left = iota((PART, 128), 1) < 64

    @pl.when(pl.program_id(0) == 0)
    def _():
        state[...] = rest[0][...] if len(rest) == 4 else jnp.zeros_like(state)

    for k in range(x_ref.shape[0] // PART):
        at = slice(k * PART, (k + 1) * PART)
        gram = lax.dot_general(
            c_ref[at, :], b_ref[at, :], (((1,), (1,)), ((), ())), preferred_element_type=f32
        )
        gram = jnp.where(lower, gram, 0.0)
        meta = meta_ref[at, :]
        grown = spread(jnp.exp2(meta), 0, chosen_ref[...])
        tail = spread(meta, 1, chosen_ref[...])
        held = jnp.dot(c_ref[at, :], state[...].astype(bf16), preferred_element_type=f32)
        fresh = []
        for q in range(pairs):
            cols = slice(q * 128, (q + 1) * 128)
            both = []
            for h in (2 * q, 2 * q + 1):
                power = jnp.minimum(meta[:, h : h + 1] - row_ref[h : h + 1, at], 100.0)
                both.append((gram * jnp.exp2(power)).astype(bf16))
            x = x_ref[at, cols]
            wide = x.astype(f32)
            none = jnp.zeros_like(x)
            stack = jnp.concatenate([jnp.where(left, x, none), jnp.where(left, none, x)], axis=0)
            inner = jnp.dot(jnp.concatenate(both, axis=1), stack, preferred_element_type=f32)
            y = inner + grown[:, cols] * held[:, cols] + skip_ref[0:1, cols] * wide
            y_ref[at, cols] = y.astype(bf16)
            fresh.append((wide * tail[:, cols]).astype(bf16))
        fresh = jnp.dot(
            turned_ref[:, at], jnp.concatenate(fresh, axis=1), preferred_element_type=f32
        )
        state[...] = state[...] * grown[PART - 1 : PART, :] + fresh


def local(x, b, c, turned, meta, row, chosen, skip, share, shares, before=()):
    length, width = x.shape
    tile = 256
    steps = length // tile // shares
    by_row = lambda i, s: (share * steps + i, 0)
    by_column = lambda i, s: (0, share * steps + i)
    one = lambda i, s: (0, 0)
    return pl.pallas_call(
        local_kernel,
        grid_spec=pltpu.PrefetchScalarGridSpec(
            num_scalar_prefetch=1,
            grid=(steps,),
            in_specs=[
                pl.BlockSpec((tile, width), by_row),
                pl.BlockSpec((tile, 128), by_row),
                pl.BlockSpec((tile, 128), by_row),
                pl.BlockSpec((128, tile), by_column),
                pl.BlockSpec((tile, 128), by_row),
                pl.BlockSpec((32, tile), by_column),
                pl.BlockSpec((256, width), one),
                pl.BlockSpec((16, width), one),
            ]
            + [pl.BlockSpec((128, width), one), pl.BlockSpec(memory_space=pl.ANY)] * (len(before) // 2),
            out_specs=[
                pl.BlockSpec((tile, width), by_row),
                pl.BlockSpec((128, width), one),
            ],
        ),
        out_shape=[
            jax.ShapeDtypeStruct((length, width), bf16),
            jax.ShapeDtypeStruct((128, width), f32),
        ],
        input_output_aliases={10: 0} if before else {},
        compiler_params=pltpu.CompilerParams(
            dimension_semantics=("arbitrary",), vmem_limit_bytes=54 << 20
        ),
        name="local",
    )(jnp.zeros((1,), jnp.int32), x, b, c, turned, meta, row, chosen, skip, *before)


def gate_kernel(
    scalars, block, y_ref, g_ref, c_ref, meta_ref, chosen_ref, mine_ref, other_ref,
    gain_ref, matrix_ref, top_ref, low_ref, ss_ref, matrix, gated, sem,
):
    rows, width = g_ref.shape
    half = width // 2
    first = block * rows

    @pl.when(first >= scalars[0])
    def _():
        top_ref[...] = jnp.zeros_like(top_ref)
        low_ref[...] = jnp.zeros_like(low_ref)
        ss_ref[...] = jnp.zeros_like(ss_ref)

    @pl.when(first < scalars[0])
    def _():
        copy = pltpu.make_async_copy(matrix_ref, matrix, sem)
        copy.start()
        low = scalars[1] == 0
        held = []
        for place in (0, 1):
            picked = jnp.where(
                low == (place == 0), mine_ref[...].astype(f32), other_ref[...].astype(f32)
            )
            held.append(picked.astype(bf16))

        def piece(k, _):
            at = pl.ds(pl.multiple_of(k * PART, PART), PART)
            grown = spread(jnp.exp2(meta_ref[at, :]), 2, chosen_ref[...])
            live = (first + k * PART + iota((PART, 1), 0) < scalars[0]).astype(f32)
            squares = jnp.zeros((PART, 128), f32)
            for place in (0, 1):
                wide = jnp.dot(c_ref[at, :], held[place], preferred_element_type=f32)
                for j in range(half // 128):
                    cols = slice(place * half + j * 128, place * half + (j + 1) * 128)
                    y = y_ref[at, cols].astype(f32)
                    y = y + grown[:, cols] * wide[:, j * 128 : (j + 1) * 128]
                    g = g_ref[at, cols].astype(f32)
                    v = y * live * (g / (1.0 + jnp.exp2(g * -LOG2E)))
                    squares = squares + v * v
                    gated[at, cols] = (v * gain_ref[0:1, cols]).astype(bf16)
            total = jnp.sum(squares, axis=1, keepdims=True)
            ss_ref[:, at] = jnp.broadcast_to(total, (PART, 128)).T[0:8, :]
            return 0

        lax.fori_loop(0, rows // PART, piece, 0)
        copy.wait()

        def columns(n, _):
            at = pl.ds(pl.multiple_of(n * 256, 256), 256)
            out = jnp.dot(gated[...], matrix[:, at], preferred_element_type=f32)
            top_ref[:, at] = out[: rows // 2].astype(bf16)
            low_ref[:, at] = out[rows // 2 :].astype(bf16)
            return 0

        lax.fori_loop(0, top_ref.shape[1] // 256, columns, 0)


def gate(scalars, y, g, c, meta, chosen, mine, other, gain, matrix):
    width = g.shape[1]
    wide = matrix.shape[1]
    rows = 512

    def at(i, s):
        return (s[2], 0)

    def body(s, *refs):
        gate_kernel(s, s[2], *refs)

    one = lambda i, s: (0, 0)
    return pl.pallas_call(
        body,
        grid_spec=pltpu.PrefetchScalarGridSpec(
            num_scalar_prefetch=1,
            grid=(1,),
            in_specs=[
                pl.BlockSpec((rows, width), at),
                pl.BlockSpec((rows, width), at),
                pl.BlockSpec((rows, 128), at),
                pl.BlockSpec((rows, 128), at),
                pl.BlockSpec((256, width), one),
                pl.BlockSpec((128, width // 2), one),
                pl.BlockSpec((128, width // 2), one),
                pl.BlockSpec((1, width), one),
                pl.BlockSpec(memory_space=pl.ANY),
            ],
            out_specs=[
                pl.BlockSpec((rows // 2, wide), one),
                pl.BlockSpec((rows // 2, wide), one),
                pl.BlockSpec((8, rows), one),
            ],
            scratch_shapes=[
                pltpu.VMEM((width, wide), bf16),
                pltpu.VMEM((rows, width), bf16),
                pltpu.SemaphoreType.DMA,
            ],
        ),
        out_shape=[
            jax.ShapeDtypeStruct((rows // 2, wide), bf16),
            jax.ShapeDtypeStruct((rows // 2, wide), bf16),
            jax.ShapeDtypeStruct((8, rows), f32),
        ],
        compiler_params=pltpu.CompilerParams(
            dimension_semantics=("arbitrary",), vmem_limit_bytes=32 << 20
        ),
        name="gate",
    )(scalars, y, g, c, meta, chosen, mine, other, gain, matrix)


def finish_kernel(own_a, own_b, last_a, last_b, s0, s1, s2, s3, out_ref):
    rows = own_a.shape[0]
    total = s0[...] + s1[...] + s2[...] + s3[...]
    scale = lax.rsqrt(total * (1.0 / (HEADS * P_SIZE)) + 1e-05)
    for k, parts in enumerate(((own_a, last_a), (own_b, last_b))):
        for j in range(rows // PART):
            at = slice(j * PART, (j + 1) * PART)
            lanes = slice(k * rows + j * PART, k * rows + (j + 1) * PART)
            factor = jnp.broadcast_to(scale[0:1, lanes], (PART, PART)).T
            for n in range(out_ref.shape[1] // 128):
                cols = slice(n * 128, (n + 1) * 128)
                value = sum(part[at, cols].astype(f32) for part in parts)
                out_ref[lanes, cols] = (value * factor).astype(bf16)


def finish(pieces, squares):
    rows, wide = pieces[0].shape
    tile = 512
    return pl.pallas_call(
        finish_kernel,
        grid=(wide // tile,),
        in_specs=[pl.BlockSpec((rows, tile), lambda i: (0, i))] * 4
        + [pl.BlockSpec((8, 2 * rows), lambda i: (0, 0))] * 4,
        out_specs=pl.BlockSpec((2 * rows, tile), lambda i: (0, i)),
        out_shape=jax.ShapeDtypeStruct((2 * rows, wide), bf16),
        compiler_params=pltpu.CompilerParams(
            dimension_semantics=("arbitrary",), vmem_limit_bytes=16 << 20
        ),
        name="finish",
    )(*pieces, *squares)


def unpack(ref):
    tail = ref[128:144, :].astype(f32)
    return ref[0:128, :].astype(f32), tail[0:1, :] + tail[1:2, :]


def pack(ref, state, decay):
    ref[0:128, :] = state.astype(bf16)
    high = decay.astype(bf16).astype(f32)
    line = iota((16, decay.shape[1]), 0)
    ref[128:144, :] = jnp.where(
        line == 0, high, jnp.where(line == 1, decay - high, 0.0)
    ).astype(bf16)


def join(earlier, later):
    return jnp.exp2(later[1]) * earlier[0] + later[0], earlier[1] + later[1]


def choose(test, one, two):
    return jax.tree.map(lambda x, y: jnp.where(test, x, y), one, two)


def scan_along(place, refs):
    pieces = [unpack(ref) for ref in refs]
    zero = jax.tree.map(jnp.zeros_like, pieces[0])
    inside = running = zero
    for k in range(4):
        at = lax.rem(place - k + 4, 4)
        piece = choose(
            at < 2, choose(at == 0, pieces[0], pieces[1]), choose(at == 2, pieces[2], pieces[3])
        )
        inside = choose(place == k, running, inside)
        running = join(running, piece)
    return inside, running


def chip_kernel(places, mine, theirs, out):
    first, second = unpack(mine), unpack(theirs)
    low = places[0] == 0
    pack(out, *join(choose(low, first, second), choose(low, second, first)))


def row_kernel(places, g0, g1, g2, g3, out, state, decay):
    inside, row = scan_along(places[1], (g0, g1, g2, g3))
    pack(out, *row)
    state[...] = inside[0]
    decay[...] = jnp.broadcast_to(inside[1], decay.shape)


def entry_kernel(places, g0, g1, g2, g3, state, decay, mine, theirs, own, away):
    before, _ = scan_along(places[2], (g0, g1, g2, g3))
    start = join(before, (state[...], decay[0:1, :]))
    first = choose(places[0] == 0, unpack(mine), unpack(theirs))
    middle = join(start, first)
    low = places[0] == 0
    own[...] = jnp.where(low, start[0], middle[0]).astype(bf16)
    away[...] = jnp.where(low, middle[0], start[0]).astype(bf16)


def small_call(kernel, name, out_shapes, places, *arrays):
    near = pl.BlockSpec(memory_space=pltpu.VMEM)
    return pl.pallas_call(
        kernel,
        in_specs=[pl.BlockSpec(memory_space=pltpu.SMEM)] + [near] * len(arrays),
        out_specs=[near] * len(out_shapes),
        out_shape=out_shapes,
        compiler_params=pltpu.CompilerParams(vmem_limit_bytes=8 << 20),
        name=name,
    )(places, *arrays)


def shift(value, axis, by, wrap=True):
    count = lax.axis_size(axis)
    pairs = [(i, (i + by) % count) for i in range(count) if wrap or i + by < count]
    return lax.ppermute(value, axis, pairs)


def gather_ring(value, axis):
    return [value] + [shift(value, axis, by) for by in (1, 2, 3)]


def incoming(mine, other, places, first_share, second_share):
    half = mine.shape[1]
    message = jax.ShapeDtypeStruct(mine.shape, bf16)
    state = jax.ShapeDtypeStruct((128, half), f32)
    decay = jax.ShapeDtypeStruct((8, half), f32)
    held = jax.ShapeDtypeStruct((128, half), bf16)
    theirs = shift(other, "seq_2", 1)
    (chip,) = small_call(chip_kernel, "chip", [message], places, mine, theirs)
    pieces = gather_ring(chip, "seq_1")
    shared = first_share()
    row, inside, faded = small_call(row_kernel, "row", [message, state, decay], places, *pieces)
    row, shared = lax.optimization_barrier((row, shared))
    pieces = gather_ring(row, "seq_0")
    y = second_share(*shared)
    pieces, y = lax.optimization_barrier((pieces, y))
    own, away = small_call(
        entry_kernel, "entry", [held, held], places, *pieces, inside, faded, mine, theirs
    )
    return own, shift(away, "seq_2", 1), y


def body(
    values,
    gates,
    b_proj,
    c_proj,
    step_size,
    decay_rate,
    skip_gain,
    norm_gain,
    readout_matrix,
    span_counts,
    remaining_count,
):
    length, width = values.shape
    valid = (span_counts[0] - 1) * SPAN + remaining_count[0]
    core = lax.axis_index("seq_2")
    place = lax.axis_index("head")
    roles = [
        jnp.stack([valid, core, (place + role) % 4]).astype(jnp.int32) for role in range(4)
    ]
    scalars = roles[0]
    meta, row, turned, chosen, skip, mine, other = states(
        scalars, values, b_proj, decay_rate, step_size, skip_gain[None, :]
    )

    def share(k, before=()):
        return local(
            values, b_proj, c_proj, turned, meta, row, chosen, skip, k, 2, before
        )

    places = jnp.stack([core, lax.axis_index("seq_1"), lax.axis_index("seq_0")]).astype(jnp.int32)
    own, theirs, y = incoming(
        mine, other, places, lambda: share(0), lambda y, state: share(1, (state, y))[0]
    )
    gain = norm_gain[None, :]

    def part(role, block=None):
        return gate(
            roles[role] if block is None else block, y, gates, c_proj, meta, chosen, own, theirs, gain, readout_matrix
        )

    def reduced(blocks):
        def send(value, by, role):
            pairs = [(z, (z + by) % 4) for z in range(4) if (z + role) % 4 < blocks]
            return lax.ppermute(value, "head", pairs)

        def add(one, two):
            return (one.astype(f32) + two.astype(f32)).astype(bf16)

        def all_live():
            far_a, far_b, s2 = part(2)
            far_a, far_b = send(far_a, 1, 2), send(far_b, -1, 2)
            up_a, up_b, s1 = part(1)
            up_b = send(up_b, 1, 1)
            down_a, down_b, s3 = part(3)
            down_a = send(down_a, -1, 3)
            up_a, down_b, last = lax.optimization_barrier(
                (add(up_a, far_a), add(down_b, far_b), roles[0])
            )
            up_a, down_b = send(up_a, 1, 1), send(down_b, -1, 3)
            s2, s1, s3 = send(s2, 2, 2), send(s1, 1, 1), send(s3, -1, 3)
            own_a, own_b, s0 = part(0, last)
            return (add(own_a, down_a), add(own_b, up_b), up_a, down_b), (s0, s1, s2, s3)

        def few_live():
            far = [
                (z, (z + (1, -1)[(z + 2) % 2]) % 4) for z in range(4) if (z + 2) % 4 < blocks
            ]
            far_a, far_b, s2 = part(2)
            far_a, far_b = [lax.ppermute(v, "head", far) for v in (far_a, far_b)]
            up_a, up_b, s1 = part(1)
            down_a, down_b, s3 = part(3)
            own_a, own_b, s0 = part(0)
            s2, s1, s3 = send(s2, 2, 2), send(s1, 1, 1), send(s3, -1, 3)
            far_a, far_b, s1, s2, s3, own_a = lax.optimization_barrier(
                (far_a, far_b, s1, s2, s3, own_a)
            )
            up_a, up_b = [send(add(v, f), 1, 1) for v, f in ((up_a, far_a), (up_b, far_b))]
            down_a, down_b = [
                send(add(v, f), -1, 3) for v, f in ((down_a, far_a), (down_b, far_b))
            ]
            return (add(own_a, down_a), add(own_b, down_b), up_a, up_b), (s0, s1, s2, s3)

        def one_live():
            far_a, far_b, s2 = part(2)
            far_a, far_b = send(far_a, 1, 2), send(far_b, -1, 2)
            up_a, up_b, s1 = part(1)
            up_b = send(up_b, 1, 1)
            down_a, down_b, s3 = part(3)
            down_a = send(down_a, -1, 3)
            own_a, own_b, s0 = part(0)
            s2, s1, s3 = send(s2, 2, 2), send(s1, 1, 1), send(s3, -1, 3)
            far_a, far_b, s1, s2, s3, own_a = lax.optimization_barrier(
                (far_a, far_b, s1, s2, s3, own_a)
            )
            up_a = send(add(up_a, far_a), 1, 1)
            down_b = send(add(down_b, far_b), -1, 3)
            return (add(own_a, down_a), add(own_b, up_b), up_a, down_b), (s0, s1, s2, s3)

        return {1: one_live, 2: few_live, 4: all_live}[blocks]

    quarter = length // 4
    level = (valid > quarter).astype(jnp.int32) + (valid > 2 * quarter)
    return finish(*lax.switch(level, [reduced(n) for n in (1, 2, 4)]))


def solution(mesh):
    finer = Mesh(
        mesh.devices.reshape(4, 4, 2, mesh.shape["head"]), ("seq_0", "seq_1", "seq_2", "head")
    )
    return jax.shard_map(
        body,
        mesh=finer,
        in_specs=(
            P(SEQ, "head"),
            P(SEQ, "head"),
            P(SEQ, None),
            P(SEQ, None),
            P("head", SEQ),
            P("head", SEQ),
            P("head"),
            P("head"),
            P("head", None),
            P(SEQ),
            P(SEQ),
        ),
        out_specs=P(SEQ_HEAD, None),
        check_vma=False,
    )
```
